128 devices in a mesh: dp: 8 (over x, core), seq: 16 (over z, y).
Axes of the slice: x: 4, y: 4, z: 4, core: 2. Of those that a mesh axis runs over, the one named last changes fastest.
Arguments:
- text_rows: bfloat16 [16384, 8192], P(('dp', 'seq')), may hold values from -6 to 6
- image_rows: bfloat16 [32, 256, 8192], P('dp', 'seq'), may hold values from -6 to 6
- tile_group: int32 [32], replicated, may hold values from 0 to 7, as said below
- tile_offset: int32 [32], replicated, may hold values from 0 to 1792, as said below
- seq_len: int32 [8], P('dp'), may hold values from 1024 to 2048, as said below
- doc_ids: int32 [8, 2048], P('dp'), may hold values from 0 to 7, never falling along the last dimension, each value on 1 to 512 neighbouring positions
- norm_gain: float32 [8192], replicated, may hold values from 0.1 to 1.9
- q_weight: bfloat16 [8192, 8192], P(None, 'seq'), may hold values from -0.0625 to 0.0625
- k_weight: bfloat16 [8192, 1024], P(None, 'seq'), may hold values from -0.0625 to 0.0625
- v_weight: bfloat16 [8192, 1024], P(None, 'seq'), may hold values from -0.0625 to 0.0625
- q_bias: float32 [8192], P('seq'), may hold values from -3 to 3
- k_bias: float32 [1024], P('seq'), may hold values from -40 to 40
- v_bias: float32 [1024], P('seq'), may hold values from -3 to 3
Outputs:
- attention: bfloat16 [16384, 8192], P('dp', 'seq')
The draws below stay inside these ranges and needn't reach their ends.
Inputs may be any that keep to these rules, and one draw needn't show every extreme that they name: `tile_group`: the 4 tiles r * 4 to r * 4 + 3 of each r < 8 go to distinct packed sequences; one packed sequence takes exactly 7 tiles and none takes more. `tile_offset`: the tiles of one packed sequence lie back to back in increasing tile order and end at or before its seq_len. `seq_len`: some packed sequence uses all 2048 positions. `doc_ids`: document ids never fall along a sequence and no document is longer than 512 positions.
All inputs are finite; a program needn't handle non-finite values.
Results may differ from the reference program's by a relative error of at most 0.003.
The reference program's roundings to bfloat16 on the way count: a program that leaves them out, or rounds other values in their place, can miss the bound.
Values may be sent and summed in bfloat16 or wider, within the bound.
No kernel may reach another device: no remote copies, remote signals or barrier semaphores. Data moves between devices by JAX's collectives and lax.ppermute only.
A program may use at most 128 MiB of HBM per device.

```python
import math
import jax
import jax.numpy as jnp
import numpy as np
from jax import lax

D = 8192
HD = 128
TR = 256
DOCS = 8
HEADS = 64
KV_HEADS = 8
LENGTH = 2048
TOKENS = 16384
TILES = 32
N_DP = 8


def placement_tables(key):
    base_key = jax.random.fold_in(key, 101)
    key_list = jax.random.split(base_key, 6)
    half_rows = N_DP // 2
    others = N_DP - 1
    row_ids = jnp.arange(N_DP, dtype=jnp.int32)
    slot_ids = jnp.arange(half_rows, dtype=jnp.int32)
    opening = jax.random.randint(key_list[0], (), 0, others)
    leading = 1 + (opening + slot_ids) % others
    later_rows = jnp.where(slot_ids[None, :] == 0, 0, 1 + (row_ids[:, None] - 1 + slot_ids[None, :] - 1) % others)
    pattern = jnp.where(row_ids[:, None] == 0, leading[None, :], later_rows).astype(jnp.int32)
    relabel = jax.random.permutation(key_list[1], N_DP).astype(jnp.int32)
    reorder = jax.random.permutation(key_list[2], N_DP).astype(jnp.int32)
    scores = jax.random.randint(key_list[3], (N_DP, half_rows), 0, 1 << 20) * half_rows + slot_ids[None, :]
    shuffle = jnp.argsort(scores, axis=1)
    chosen = jnp.take_along_axis(pattern[reorder], shuffle, axis=1)
    tile_group = relabel[chosen].reshape(-1).astype(jnp.int32)
    counts = jnp.sum((tile_group[None, :] == row_ids[:, None]).astype(jnp.int32), axis=1)
    free_rows = LENGTH - counts * TR
    shortfall = jax.random.randint(key_list[4], (N_DP,), 0, free_rows // 2 + 1)
    is_full = row_ids == relabel[0]
    valid_len = jnp.where(is_full, LENGTH, LENGTH - shortfall).astype(jnp.int32)
    random_start = jax.random.randint(key_list[5], (N_DP,), 0, valid_len - counts * TR + 1)
    row_start = jnp.where(is_full, valid_len - counts * TR, random_start).astype(jnp.int32)
    tile_ids = jnp.arange(TILES, dtype=jnp.int32)
    earlier = jnp.sum(((tile_group[None, :] == tile_group[:, None]) & (tile_ids[None, :] < tile_ids[:, None])).astype(jnp.int32), axis=1)
    tile_offset = (row_start[tile_group] + TR * earlier).astype(jnp.int32)
    return (tile_group, tile_offset, valid_len)


def draw_tile_group(key, part):
    return placement_tables(key)[0]


def draw_tile_offset(key, part):
    return placement_tables(key)[1]


def draw_seq_len(key, part):
    return placement_tables(key)[2]


def draw_k_bias(key, part):
    bias_key = jax.random.fold_in(key, 202)
    values = 0.5 * jax.random.truncated_normal(bias_key, -6.0, 6.0, (KV_HEADS * HD,), jnp.float32)
    return values


def levels(rng, shape, cuts, low, top_value):
    gain, own = 1.0, jax.random.fold_in(rng, 6)
    for dim, shards_of in cuts:
        heights = jnp.exp(jax.random.uniform(jax.random.fold_in(own, dim), (shards_of,), jnp.float32, low / len(cuts), top_value / len(cuts)))
        gain = gain * jnp.repeat(heights, shape[dim] // shards_of).reshape([-1 if axis == dim else 1 for axis in range(len(shape))])
    return gain


def split_up(amount, total, limit, slope):
    weights = [(1 << 20) // math.isqrt(grade ** slope) + 1 for grade in range(2, amount + 1)]
    surplus, holding = total - limit - (amount - 1), [1] * (amount - 1)
    while surplus > 0:
        movable = [i for i in range(amount - 1) if holding[i] < limit]
        mass, left = sum([weights[i] for i in movable]), surplus
        for i in movable:
            extra = min(limit - holding[i], max(1, left * weights[i] // mass), surplus)
            holding[i] = holding[i] + extra
            surplus = surplus - extra
    return np.array([limit] + holding)


def uneven(key, amount, total, limit, slope):
    if amount == 2:
        one = jax.random.randint(key, (), max(1, total - limit), min(limit, total - 1) + 1)
        return jnp.stack([one, total - one])
    lengths = jnp.asarray(split_up(amount, total, limit, slope), jnp.int32)
    twos = (amount - 1) // 2
    giver, taker = lengths[1:1 + 2 * twos:2], lengths[2:2 + 2 * twos:2]
    margin = jnp.minimum(giver - 1, limit - taker)
    moved = jax.random.randint(jax.random.fold_in(key, 1), (twos,), 0, 1 << 20) % (margin + 1)
    lengths = lengths.at[1:1 + 2 * twos:2].set(giver - moved).at[2:2 + 2 * twos:2].set(taker + moved)
    return lengths[jax.random.permutation(jax.random.fold_in(key, 2), amount)]


def normal_values(own_key, dims, scale, reach, shards=(), held_as=jnp.bfloat16):
    drawn = jax.random.normal(own_key, dims, jnp.float32) * scale
    if len(shards) > 0:
        drawn = levels(own_key, dims, shards, -0.22, 0.18) * drawn
    return jnp.clip(drawn, min=-reach, max=reach).astype(held_as)


def setup_inputs(seed: int = 0) -> dict:
    splits = jax.random.split(jax.random.key(seed), 14)
    return {
        "text_rows": normal_values(splits[0], (TOKENS, D), 1.0, 6.0, ((0, 128),)),
        "image_rows": normal_values(splits[1], (TILES, TR, D), 1.0, 6.0, ((0, 8), (1, 16))),
        "tile_group": draw_tile_group(jax.random.fold_in(splits[13], 71), 0),
        "tile_offset": draw_tile_offset(jax.random.fold_in(splits[13], 71), 0),
        "seq_len": draw_seq_len(jax.random.fold_in(splits[13], 71), 0),
        "doc_ids": jax.vmap(lambda own: jnp.searchsorted(jnp.cumsum(uneven(own, DOCS, LENGTH, LENGTH // 4, 2)), jnp.arange(LENGTH), side="right"))(jax.random.split(splits[5], N_DP)).reshape((N_DP, LENGTH)).astype(jnp.int32),
        "norm_gain": jnp.clip(1.0 + 0.18 * jax.random.normal(splits[6], (D,), jnp.float32), 0.1, 1.9),
        "q_weight": normal_values(splits[7], (D, HEADS * HD), D ** -0.5, 0.0625, ((1, 16),)),
        "k_weight": normal_values(splits[8], (D, KV_HEADS * HD), D ** -0.5, 0.0625, ((1, 16),)),
        "v_weight": normal_values(splits[9], (D, KV_HEADS * HD), D ** -0.5, 0.0625, ((1, 16),)),
        "q_bias": normal_values(splits[10], (HEADS * HD,), 0.5, 3.0, ((0, 16),), jnp.float32),
        "k_bias": draw_k_bias(jax.random.fold_in(splits[13], 71), 0),
        "v_bias": normal_values(splits[12], (KV_HEADS * HD,), 0.5, 3.0, ((0, 16),), jnp.float32),
    }


THETA = 1000000.0
NEGATIVE = -1e+30
EPSILON = 1e-06

def rms_norm(row_block, norm_gain):
    float_rows = row_block.astype(jnp.float32)
    inv_rms = lax.rsqrt(lax.optimization_barrier(jnp.mean(float_rows * float_rows, axis=-1, keepdims=True)) + EPSILON)
    return (float_rows * inv_rms * norm_gain).astype(jnp.bfloat16)

def doc_positions(doc_row):
    indices = jnp.arange(doc_row.shape[0], dtype=jnp.int32)
    starts = jnp.concatenate([jnp.ones((1,), jnp.bool_), doc_row[1:] != doc_row[:-1]])
    first_index = lax.cummax(jnp.where(starts, indices, 0), axis=0)
    return indices - first_index

def rotary(values, position):
    head_dim = values.shape[-1]
    half_dim = head_dim // 2
    frequency = THETA ** (-(jnp.arange(half_dim, dtype=jnp.float32) * 2.0) / head_dim)
    angles = position.astype(jnp.float32)[:, None] * frequency[None, :]
    cosine = jnp.concatenate([jnp.cos(angles), jnp.cos(angles)], axis=-1)
    sine_part = jnp.concatenate([jnp.sin(angles), jnp.sin(angles)], axis=-1)
    if values.ndim == 3:
        cosine = cosine[:, None, :]
        sine_part = sine_part[:, None, :]
    rotated = jnp.concatenate([-values[..., half_dim:], values[..., :half_dim]], axis=-1)
    return values * cosine + rotated * sine_part

def reference(text_rows, image_rows, tile_group, tile_offset, seq_len, doc_ids, norm_gain, q_weight, k_weight, v_weight, q_bias, k_bias, v_bias):
    image_flat = image_rows.reshape(TILES * TR, D)
    positions = jnp.arange(LENGTH, dtype=jnp.int32)
    tile_ids = jnp.arange(TILES, dtype=jnp.int32)
    scale_factor = HD ** (-0.5)

    def one_sequence(inputs):
        my_group, text_part, doc_row, valid_len = inputs
        inside = (tile_group[None, :] == my_group) & (tile_offset[None, :] <= positions[:, None]) & (positions[:, None] < tile_offset[None, :] + TR)
        covered = jnp.any(inside, axis=1)
        tile_index = lax.optimization_barrier(jnp.sum(jnp.where(inside, tile_ids[None, :], 0), axis=1)).astype(jnp.int32)
        tile_start = lax.optimization_barrier(jnp.sum(jnp.where(inside, tile_offset[None, :], 0), axis=1)).astype(jnp.int32)
        source = (tile_index * TR + jnp.where(covered, positions - tile_start, 0)).astype(jnp.int32)
        merged = jnp.where(covered[:, None], jnp.take(image_flat, source, axis=0), text_part)
        normed = rms_norm(merged, norm_gain)
        query_raw = jnp.dot(normed, q_weight, preferred_element_type=jnp.float32) + q_bias
        key_raw = jnp.dot(normed, k_weight, preferred_element_type=jnp.float32) + k_bias
        value_all = (jnp.dot(normed, v_weight, preferred_element_type=jnp.float32) + v_bias).astype(jnp.bfloat16)
        in_doc = doc_positions(doc_row)
        queries = rotary(query_raw.reshape(LENGTH, HEADS, HD), in_doc).astype(jnp.bfloat16)
        key_all = rotary(key_raw.reshape(LENGTH, KV_HEADS, HD), in_doc).astype(jnp.bfloat16)
        value_all = value_all.reshape(LENGTH, KV_HEADS, HD)
        allowed = (doc_row[:, None] == doc_row[None, :]) & (positions[None, :] <= positions[:, None]) & (positions[None, :] < valid_len)

        def one_head(head_index):
            query_head = lax.dynamic_index_in_dim(queries, head_index, 1, keepdims=False)
            key_head = lax.dynamic_index_in_dim(key_all, head_index // 8, 1, keepdims=False)
            value_head = lax.dynamic_index_in_dim(value_all, head_index // 8, 1, keepdims=False)
            scores = jnp.dot(query_head, key_head.T, preferred_element_type=jnp.float32) * scale_factor
            scores = jnp.where(allowed, scores, NEGATIVE)
            row_peak = lax.optimization_barrier(jnp.max(scores, axis=-1, keepdims=True))
            exponent = jnp.exp(scores - row_peak)
            weights = (exponent / lax.optimization_barrier(jnp.sum(exponent, axis=-1, keepdims=True))).astype(jnp.bfloat16)
            mixed = jnp.dot(weights, value_head, preferred_element_type=jnp.float32)
            mixed = jnp.where((positions < valid_len)[:, None], mixed, 0.0)
            return mixed.astype(jnp.bfloat16)
        heads_out = lax.map(one_head, jnp.arange(HEADS, dtype=jnp.int32))
        return jnp.transpose(heads_out, (1, 0, 2)).reshape(LENGTH, HEADS * HD)
    result = lax.map(one_sequence, (jnp.arange(N_DP, dtype=jnp.int32), text_rows.reshape(N_DP, LENGTH, D), doc_ids, seq_len))
    return result.reshape(TOKENS, HEADS * HD)
```

```python
import math

import jax
import jax.numpy as jnp
from jax import lax
from jax.experimental import pallas as pl
from jax.experimental.pallas import tpu as pltpu
from jax.sharding import Mesh, PartitionSpec as P

TR = 256
UNIT = 16
HD = 128
LENGTH = 2048
CAPACITY = 36
ROWS = CAPACITY * UNIT
WINDOW = 512
THETA = 1000000.0
NEGATIVE = -1e30
EPSILON = 1e-06


def shifted(block, axis, step):
    count = lax.axis_size(axis)
    return lax.ppermute(block, axis, [(low, (low + step) % count) for low in range(count)])


def rms_norm(row_block, gain):
    float_rows = row_block.astype(jnp.float32)
    inv_rms = lax.rsqrt(jnp.mean(float_rows * float_rows, axis=-1, keepdims=True) + EPSILON)
    return (float_rows * inv_rms * gain).astype(jnp.bfloat16)


def norm_text_kernel(rows_ref, gain_ref, out_ref):
    out_ref[...] = rms_norm(rows_ref[...], gain_ref[...])


def norm_text(rows, gain):
    count, features = rows.shape
    step = 2 * UNIT
    return pl.pallas_call(
        norm_text_kernel,
        grid=(count // step,),
        in_specs=[
            pl.BlockSpec((step, features), lambda i: (i, 0)),
            pl.BlockSpec((1, features), lambda i: (0, 0)),
        ],
        out_specs=pl.BlockSpec((step, features), lambda i: (i, 0)),
        out_shape=jax.ShapeDtypeStruct(rows.shape, jnp.bfloat16),
        name="norm_text",
    )(rows, gain)


def norm_image_kernel(chosen_ref, rows_ref, gain_ref, out_ref):
    out_ref[0] = rms_norm(rows_ref[0], gain_ref[...])


def norm_image(pieces, gain, chosen):
    _, piece_rows, features = pieces.shape
    groups = chosen.shape[0]
    return pl.pallas_call(
        norm_image_kernel,
        grid_spec=pltpu.PrefetchScalarGridSpec(
            num_scalar_prefetch=1,
            grid=(groups,),
            in_specs=[
                pl.BlockSpec((1, piece_rows, features), lambda i, chosen: (chosen[i], 0, 0)),
                pl.BlockSpec((1, features), lambda i, chosen: (0, 0)),
            ],
            out_specs=pl.BlockSpec((1, piece_rows, features), lambda i, chosen: (i, 0, 0)),
        ),
        out_shape=jax.ShapeDtypeStruct((groups, piece_rows, features), jnp.bfloat16),
        name="norm_image",
    )(chosen, pieces, gain)


def project_kernel(
    place_ref,
    t0, t1, t2a, t2b, t3,
    i0, i1, i2a, i2b, i3,
    weight_ref, bias_ref, cos_ref, sin_ref,
    out_ref,
    rows_ref, sum_ref, pair_ref, sems,
):
    column = pl.program_id(0)
    part = pl.program_id(1)
    depth = weight_ref.shape[0]

    @pl.when((column == 0) & (part == 0))
    def _():
        total = place_ref[64]
        for unit in range(24, CAPACITY):
            @pl.when(unit >= total)
            def _(unit=unit):
                rows_ref[pl.ds(UNIT * unit, UNIT), :] = jnp.zeros(
                    (UNIT, rows_ref.shape[1]), jnp.bfloat16
                )

        def copy(index):
            delta, slot = index % 32 // 8, index % 8
            if index < 32:
                source = (t0, t1, t2a if slot < 4 else t2b, t3)[delta]
                slot = slot % 4 if delta == 2 else slot
                source = source.at[pl.ds(UNIT * slot, UNIT), :]
            else:
                source = (i0, i1, i2a if slot < 4 else i2b, i3)[delta]
                slot = slot % 4 if delta == 2 else slot
                source = source.at[slot]
            row = pl.multiple_of(UNIT * jnp.maximum(place_ref[index], 0), UNIT)
            return pltpu.make_async_copy(
                source, rows_ref.at[pl.ds(row, UNIT), :], sems.at[index]
            )

        for index in range(64):
            @pl.when(place_ref[index] >= 0)
            def _(index=index):
                copy(index).start()
        for index in range(64):
            @pl.when(place_ref[index] >= 0)
            def _(index=index):
                copy(index).wait()

    start = pl.multiple_of(part * depth, depth)
    product = jnp.dot(
        rows_ref[:, pl.ds(start, depth)], weight_ref[...], preferred_element_type=jnp.float32
    )

    @pl.when(part == 0)
    def _():
        sum_ref[...] = product

    @pl.when(part > 0)
    def _():
        sum_ref[...] += product

    @pl.when(part == pl.num_programs(1) - 1)
    def _():
        bias = bias_ref[pl.ds(column, 1), :]
        cosine = cos_ref[...]
        sine = sin_ref[...]

        def rotated(values):
            return values * cosine + pltpu.roll(values, HD // 2, 1) * sine

        heads = weight_ref.shape[1] // HD - 1
        for head in range(heads):
            lanes = slice(head * HD, (head + 1) * HD)
            out_ref[column, :, lanes] = rotated(sum_ref[:, lanes] + bias[:, lanes]).astype(
                jnp.bfloat16
            )
        last = heads * HD
        halves = sum_ref[:, last:] + bias[:, last:]

        @pl.when(column % 2 == 0)
        def _():
            pair_ref[...] = halves

        @pl.when(column % 2 == 1)
        def _():
            lower = pair_ref[...]
            in_low = lax.broadcasted_iota(jnp.int32, lower.shape, 1) < HD // 2
            key = jnp.where(in_low, lower, pltpu.roll(halves, HD // 2, 1))
            value = jnp.where(in_low, pltpu.roll(lower, HD // 2, 1), halves).astype(jnp.bfloat16)
            key = rotated(key).astype(jnp.bfloat16)
            for target in (column - 1, column):
                out_ref[target, :, last:last + HD] = key
                out_ref[target, :, last + HD:] = value


def project(place, texts, images, weights, bias, cosine, sine):
    columns = bias.shape[0]
    width = bias.shape[1]
    features = texts[0].shape[1]
    parts = 8
    depth = features // parts
    any_spec = pl.BlockSpec(memory_space=pl.ANY)
    whole = lambda shape: pl.BlockSpec(shape, lambda i, k, place: (0,) * len(shape))
    return pl.pallas_call(
        project_kernel,
        grid_spec=pltpu.PrefetchScalarGridSpec(
            num_scalar_prefetch=1,
            grid=(columns, parts),
            in_specs=[any_spec] * 10
            + [
                pl.BlockSpec((depth, width), lambda i, k, place: (k * columns + i, 0)),
                whole((columns, width)),
                whole((ROWS, HD)),
                whole((ROWS, HD)),
            ],
            out_specs=whole((columns, ROWS, width + HD)),
            scratch_shapes=[
                pltpu.VMEM((ROWS, features), jnp.bfloat16),
                pltpu.VMEM((ROWS, width), jnp.float32),
                pltpu.VMEM((ROWS, HD), jnp.float32),
                pltpu.SemaphoreType.DMA((64,)),
            ],
        ),
        out_shape=jax.ShapeDtypeStruct((columns, ROWS, width + HD), jnp.bfloat16),
        compiler_params=pltpu.CompilerParams(vmem_limit_bytes=48 << 20),
        cost_estimate=pl.CostEstimate(
            flops=2 * ROWS * features * width * columns,
            transcendentals=0,
            bytes_accessed=2 * features * width * columns,
        ),
        name="project",
    )(place, *texts, *images, weights, bias, cosine, sine)


def attend_kernel(info_ref, text_ref, parts_ref, out_ref, merged_ref, run_ref, mask_ref):
    step = pl.program_id(0)
    block = out_ref.shape[0]
    width = parts_ref.shape[2]
    run_start = info_ref[8]
    run_end = info_ref[9]
    used = info_ref[10]
    first_unit = (run_start + UNIT - 1) // UNIT
    lag = first_unit * UNIT - run_start

    @pl.when(step == 0)
    def _():
        merged_ref[0:WINDOW, :] = jnp.zeros((WINDOW, width), jnp.bfloat16)
        run_ref[0:128, :] = jnp.zeros((128, width), jnp.bfloat16)
        run_ref[128 + 7 * TR:, :] = jnp.zeros((run_ref.shape[0] - 128 - 7 * TR, width), jnp.bfloat16)

        def tile_step(tile, carry):
            for piece in range(16):
                source = pl.multiple_of(tile * 64 + piece // 4 * UNIT, UNIT)
                target = pl.multiple_of(128 + tile * TR + piece * UNIT, UNIT)
                run_ref[pl.ds(target, UNIT), :] = parts_ref[piece % 4, pl.ds(source, UNIT), :]
            return carry

        lax.fori_loop(0, (run_end - run_start) // TR, tile_step, 0)

        def clear_step(tile, carry):
            target = pl.multiple_of(128 + tile * TR, TR // 2)
            run_ref[pl.ds(target, TR), :] = jnp.zeros((TR, width), jnp.bfloat16)
            return carry

        lax.fori_loop((run_end - run_start) // TR, 7, clear_step, 0)

        def block_step(row, carry):
            for member in range(4):
                number = row * 4 + member
                begin = number * 128
                for unit in range(8):
                    source = pl.multiple_of(text_ref[number * 8 + unit] * UNIT, UNIT)
                    target = pl.multiple_of(WINDOW + begin + unit * UNIT, UNIT)
                    merged_ref[pl.ds(target, UNIT), :] = parts_ref[member, pl.ds(source, UNIT), :]

                @pl.when((begin < run_end) & (begin + 128 > run_start))
                def _():
                    origin = pl.multiple_of(128 + UNIT * (8 * number - first_unit), UNIT)
                    window = run_ref[pl.ds(origin, 256), :]
                    place = lax.broadcasted_iota(jnp.int32, (128, 256), 0)
                    taken = lax.broadcasted_iota(jnp.int32, (128, 256), 1)
                    pick = jnp.where(taken == place + lag, 1.0, 0.0).astype(jnp.bfloat16)
                    moved = jnp.dot(pick, window, preferred_element_type=jnp.float32)
                    here = pl.ds(pl.multiple_of(WINDOW + begin, 128), 128)
                    old = merged_ref[here, :].astype(jnp.float32)
                    position = begin + lax.broadcasted_iota(jnp.int32, old.shape, 0)
                    covered = (position >= run_start) & (position < run_end)
                    merged_ref[here, :] = jnp.where(covered, moved, old).astype(jnp.bfloat16)
            return carry

        lax.fori_loop(0, 4, block_step, 0)

    base = pl.multiple_of(step * block, block)
    span = block + WINDOW
    position = base + lax.broadcasted_iota(jnp.int32, (block, 1), 0)
    doc_start = jnp.zeros((block, 1), jnp.int32)
    for doc in range(1, 8):
        doc_start = jnp.where(position >= info_ref[doc], info_ref[doc], doc_start)
    other = base - WINDOW + lax.broadcasted_iota(jnp.int32, (block, span), 1)
    allowed = (other >= doc_start) & (other <= position) & (other < used)
    mask_ref[...] = jnp.where(allowed, 0.0, NEGATIVE)
    queries = pl.ds(pl.multiple_of(WINDOW + base, block), block)
    keys = merged_ref[pl.ds(base, span), 4 * HD:5 * HD]
    values = merged_ref[pl.ds(base, span), 5 * HD:6 * HD]
    factor = HD ** (-0.5) * math.log2(math.e)
    for head in range(4):
        lanes = slice(head * HD, (head + 1) * HD)
        scores = lax.dot_general(
            merged_ref[queries, lanes], keys, (((1,), (1,)), ((), ())),
            preferred_element_type=jnp.float32,
        ) + mask_ref[...]
        peak = jnp.max(scores, axis=-1, keepdims=True)
        exponent = jnp.exp2((scores - peak) * factor)
        inverse = 1.0 / jnp.sum(exponent, axis=-1, keepdims=True)
        probs = (exponent * inverse).astype(jnp.bfloat16)
        mixed = jnp.dot(probs, values, preferred_element_type=jnp.float32)
        out_ref[:, lanes] = jnp.where(position < used, mixed, 0.0).astype(jnp.bfloat16)


def attend(info, text_index, parts):
    block = 256
    width = parts.shape[2]
    return pl.pallas_call(
        attend_kernel,
        grid_spec=pltpu.PrefetchScalarGridSpec(
            num_scalar_prefetch=2,
            grid=(LENGTH // block,),
            in_specs=[pl.BlockSpec(parts.shape, lambda i, a, b: (0, 0, 0))],
            out_specs=pl.BlockSpec((block, 4 * HD), lambda i, a, b: (i, 0)),
            scratch_shapes=[
                pltpu.VMEM((WINDOW + LENGTH, width), jnp.bfloat16),
                pltpu.VMEM((128 + 7 * TR + 384, width), jnp.bfloat16),
                pltpu.VMEM((block, block + WINDOW), jnp.float32),
            ],
        ),
        out_shape=jax.ShapeDtypeStruct((LENGTH, 4 * HD), jnp.bfloat16),
        compiler_params=pltpu.CompilerParams(vmem_limit_bytes=48 << 20),
        name="attend",
    )(info, text_index, parts)


def tables(tile_group, tile_offset, seq_len, doc_ids, group, z, y):
    mine = tile_group == group
    present = jnp.any(mine.reshape(8, 4), axis=1)
    count = jnp.sum(mine.astype(jnp.int32))
    run_start = jnp.where(count > 0, jnp.min(jnp.where(mine, tile_offset, LENGTH)), 0)
    run_end = run_start + TR * count
    low_unit = (run_start + UNIT - 1) // UNIT
    high_unit = run_end // UNIT
    eight = jnp.arange(8, dtype=jnp.int32)
    rank = jnp.sum((present[None, :] & (eight[None, :] < eight[:, None])).astype(jnp.int32), axis=1)
    order = jnp.arange(32, dtype=jnp.int32)
    four = jnp.arange(4, dtype=jnp.int32)
    unit_of = 8 * (4 * (order[None, :] // 8) + four[:, None]) + order[None, :] % 8
    before = jnp.sum((unit_of < low_unit).astype(jnp.int32), axis=1)
    hidden = jnp.sum((unit_of < high_unit).astype(jnp.int32), axis=1) - before
    held = (unit_of < low_unit) | (unit_of >= high_unit)
    compact = 4 * count + order[None, :] - jnp.where(unit_of >= high_unit, hidden[:, None], 0)
    compact = jnp.where(held, compact, -1)
    text_index = jnp.maximum(compact, 0).reshape(4, 4, 8).transpose(1, 0, 2).reshape(-1)
    my_before = lax.dynamic_index_in_dim(before, y, 0, keepdims=False)
    my_hidden = lax.dynamic_index_in_dim(hidden, y, 0, keepdims=False)
    member = (z + four) % 4
    my_compact = lax.dynamic_index_in_dim(compact, y, 0, keepdims=False).reshape(4, 8)
    text_place = jnp.take(my_compact, member, axis=0).reshape(-1)
    image_place = jnp.where(present[None, :], 4 * rank[None, :] + member[:, None], -1).reshape(-1)
    total = 4 * count + 32 - my_hidden
    place = jnp.concatenate([text_place, image_place, total[None]]).astype(jnp.int32)
    number = jnp.arange(ROWS, dtype=jnp.int32) // UNIT
    inner = jnp.arange(ROWS, dtype=jnp.int32) % UNIT
    image_at = run_start + TR * (number // 4) + UNIT * (4 * (number % 4) + y)
    text_number = number - 4 * count
    text_number = jnp.clip(text_number + jnp.where(text_number >= my_before, my_hidden, 0), 0, 31)
    text_at = 128 * (4 * (text_number // 8) + y) + UNIT * (text_number % 8)
    position = jnp.where(number < 4 * count, image_at, text_at) + inner
    starts = jnp.sum((doc_ids[0][None, :] < eight[:, None]).astype(jnp.int32), axis=1)
    doc_start = jnp.max(
        jnp.where(starts[None, :] <= position[:, None], starts[None, :], 0), axis=1
    )
    in_doc = position - doc_start
    info = jnp.concatenate([starts, run_start[None], run_end[None], seq_len]).astype(jnp.int32)
    return place, text_index, info, in_doc


def per_device(
    text_rows, image_rows, tile_group, tile_offset, seq_len, doc_ids, norm_gain,
    q_weight, k_weight, v_weight, q_bias, k_bias, v_bias,
):
    group = lax.axis_index("x") * 2 + lax.axis_index("c")
    z = lax.axis_index("z")
    y = lax.axis_index("y")
    depth = q_weight.shape[0] // 8
    gain = norm_gain.reshape(1, -1)

    def own_part(weight):
        return lax.dynamic_slice_in_dim(weight, group * depth, depth, 0)

    weight_part = jnp.concatenate(
        [own_part(q_weight), own_part(k_weight), own_part(v_weight)], axis=1
    )
    weights = lax.all_gather(weight_part, ("x", "c", "y"), axis=0, tiled=True)

    t0 = norm_text(text_rows, gain)
    t3 = shifted(t0, "z", 1)
    t1 = shifted(t0, "z", -1)
    t2a = shifted(t3[:64], "z", 1)
    t2b = shifted(t1[64:], "z", -1)

    row_groups = lax.dynamic_slice_in_dim(tile_group, group * 4, 4)
    matches = row_groups[None, :] == jnp.arange(8, dtype=jnp.int32)[:, None]
    chosen = jnp.sum(jnp.where(matches, jnp.arange(4, dtype=jnp.int32)[None, :], 0), axis=1)
    outgoing = norm_image(image_rows, gain, chosen.astype(jnp.int32))
    i0 = lax.all_to_all(outgoing, ("x", "c"), split_axis=0, concat_axis=0, tiled=True)
    i3 = shifted(i0, "z", 1)
    i1 = shifted(i0, "z", -1)
    i2a = shifted(i3[:4], "z", 1)
    i2b = shifted(i1[4:], "z", -1)

    bias = lax.all_gather(jnp.concatenate([q_bias, k_bias, v_bias]), "y", axis=0, tiled=False)
    place, text_index, info, in_doc = tables(
        tile_group, tile_offset, seq_len, doc_ids, group, z, y
    )
    frequency = THETA ** (-(jnp.arange(HD // 2, dtype=jnp.float32) * 2.0) / HD)
    angles = in_doc.astype(jnp.float32)[:, None] * frequency[None, :]
    cosine = jnp.concatenate([jnp.cos(angles), jnp.cos(angles)], axis=-1)
    sine = jnp.concatenate([-jnp.sin(angles), jnp.sin(angles)], axis=-1)

    outward = project(
        place, (t0, t1, t2a, t2b, t3), (i0, i1, i2a, i2b, i3), weights, bias, cosine, sine
    )
    parts = lax.all_to_all(outward, "y", split_axis=0, concat_axis=0, tiled=True)
    return attend(info, text_index, parts)


def solution(mesh):
    fine = Mesh(mesh.devices.reshape(4, 2, 4, 4), ("x", "c", "z", "y"))
    dp, seq = ("x", "c"), ("z", "y")
    return jax.shard_map(
        per_device,
        mesh=fine,
        in_specs=(
            P(dp + seq, None),
            P(dp, seq, None),
            P(),
            P(),
            P(dp),
            P(dp, None),
            P(),
            P(None, seq),
            P(None, seq),
            P(None, seq),
            P(seq),
            P(seq),
            P(seq),
        ),
        out_specs=P(dp, seq),
        check_vma=False,
    )
```

```python
import math

import jax
import jax.numpy as jnp
from jax import lax
from jax.experimental import pallas as pl
from jax.experimental.pallas import tpu as pltpu
from jax.sharding import Mesh, PartitionSpec as P

TR = 256
UNIT = 16
HD = 128
LENGTH = 2048
CAPACITY = 36
ROWS = CAPACITY * UNIT
WINDOW = 512
THETA = 1000000.0
NEGATIVE = -1e30
EPSILON = 1e-06


def shifted(block, axis, step):
    count = lax.axis_size(axis)
    return lax.ppermute(block, axis, [(low, (low + step) % count) for low in range(count)])


def rms_norm(row_block, gain):
    float_rows = row_block.astype(jnp.float32)
    inv_rms = lax.rsqrt(jnp.mean(float_rows * float_rows, axis=-1, keepdims=True) + EPSILON)
    return (float_rows * inv_rms * gain).astype(jnp.bfloat16)


def norm_text_kernel(rows_ref, gain_ref, out_ref):
    out_ref[...] = rms_norm(rows_ref[...], gain_ref[...])


def norm_text(rows, gain):
    count, features = rows.shape
    step = 2 * UNIT
    return pl.pallas_call(
        norm_text_kernel,
        grid=(count // step,),
        in_specs=[
            pl.BlockSpec((step, features), lambda i: (i, 0)),
            pl.BlockSpec((1, features), lambda i: (0, 0)),
        ],
        out_specs=pl.BlockSpec((step, features), lambda i: (i, 0)),
        out_shape=jax.ShapeDtypeStruct(rows.shape, jnp.bfloat16),
        name="norm_text",
    )(rows, gain)


def norm_image_kernel(chosen_ref, rows_ref, gain_ref, out_ref):
    out_ref[0] = rms_norm(rows_ref[0], gain_ref[...])


def norm_image(pieces, gain, chosen):
    _, piece_rows, features = pieces.shape
    groups = chosen.shape[0]
    return pl.pallas_call(
        norm_image_kernel,
        grid_spec=pltpu.PrefetchScalarGridSpec(
            num_scalar_prefetch=1,
            grid=(groups,),
            in_specs=[
                pl.BlockSpec((1, piece_rows, features), lambda i, chosen: (chosen[i], 0, 0)),
                pl.BlockSpec((1, features), lambda i, chosen: (0, 0)),
            ],
            out_specs=pl.BlockSpec((1, piece_rows, features), lambda i, chosen: (i, 0, 0)),
        ),
        out_shape=jax.ShapeDtypeStruct((groups, piece_rows, features), jnp.bfloat16),
        name="norm_image",
    )(chosen, pieces, gain)


def pick_kernel(chosen_ref, rows_ref, out_ref):
    out_ref[...] = rows_ref[...]


def pick_slots(pieces, chosen):
    _, piece_rows, features = pieces.shape
    count = chosen.shape[0]
    return pl.pallas_call(
        pick_kernel,
        grid_spec=pltpu.PrefetchScalarGridSpec(
            num_scalar_prefetch=1,
            grid=(count,),
            in_specs=[pl.BlockSpec((1, piece_rows, features), lambda i, chosen: (chosen[i], 0, 0))],
            out_specs=pl.BlockSpec((1, piece_rows, features), lambda i, chosen: (i, 0, 0)),
        ),
        out_shape=jax.ShapeDtypeStruct((count, piece_rows, features), jnp.bfloat16),
        name="pick_slots",
    )(chosen, pieces)


def rotated(values, cosine, sine):
    return values * cosine + pltpu.roll(values, HD // 2, 1) * sine


def project_first_kernel(
    place_ref,
    t0, t1, t2a, t2b, t3,
    i0, i1, i2a, i2b, i3,
    weight_ref, kv_bias_ref, q_bias_ref, cos_ref, sin_ref,
    out_ref, kv_ref, compact_ref,
    rows_ref, weight_buf, sum_ref, sems, weight_sems, copy_sem,
):
    slots = weight_buf.shape[0]
    chunks = 8
    depth = weight_buf.shape[1]
    width = weight_buf.shape[2]
    target = place_ref[65]

    def weight_copies(step, slot):
        kv = [
            pltpu.make_async_copy(
                weight_ref.at[pl.ds((step * 4 + y) * depth, depth), pl.ds(width, HD)],
                weight_buf.at[slot, :, pl.ds(y * HD, HD)],
                weight_sems.at[slot, y],
            )
            for y in range(4)
        ]
        query = pltpu.make_async_copy(
            weight_ref.at[pl.ds(((step - chunks) * 4 + target) * depth, depth), pl.ds(0, width)],
            weight_buf.at[slot],
            weight_sems.at[slot, 0],
        )
        return kv, query

    def start(step):
        slot = step % slots

        @pl.when(step < chunks)
        def _():
            for copy in weight_copies(step, slot)[0]:
                copy.start()

        @pl.when((step >= chunks) & (step < 2 * chunks))
        def _():
            weight_copies(step, slot)[1].start()

    for step in range(slots - 1):
        start(jnp.int32(step))

    total = place_ref[64]
    for unit in range(24, CAPACITY):
        @pl.when(unit >= total)
        def _(unit=unit):
            rows_ref[pl.ds(UNIT * unit, UNIT), :] = jnp.zeros(
                (UNIT, rows_ref.shape[1]), jnp.bfloat16
            )

    def unit_copy(index):
        delta, slot = index % 32 // 8, index % 8
        if index < 32:
            source = (t0, t1, t2a if slot < 4 else t2b, t3)[delta]
            slot = slot % 4 if delta == 2 else slot
            source = source.at[pl.ds(UNIT * slot, UNIT), :]
        else:
            source = (i0, i1, i2a if slot < 4 else i2b, i3)[delta]
            slot = slot % 4 if delta == 2 else slot
            source = source.at[slot]
        row = pl.multiple_of(UNIT * jnp.maximum(place_ref[index], 0), UNIT)
        return pltpu.make_async_copy(source, rows_ref.at[pl.ds(row, UNIT), :], sems.at[index])

    used = [index for index in range(64) if index < 32 or index % 8 < 7]
    for index in used:
        @pl.when(place_ref[index] >= 0)
        def _(index=index):
            unit_copy(index).start()
    for index in used:
        @pl.when(place_ref[index] >= 0)
        def _(index=index):
            unit_copy(index).wait()
    copy_out = pltpu.make_async_copy(rows_ref, compact_ref, copy_sem)
    copy_out.start()

    def product(step, part):
        slot = step % slots
        lanes = pl.ds(pl.multiple_of(part * depth, depth), depth)
        value = jnp.dot(
            rows_ref[:, lanes], weight_buf[slot], preferred_element_type=jnp.float32
        )

        @pl.when(part == 0)
        def _():
            sum_ref[...] = value

        @pl.when(part > 0)
        def _():
            sum_ref[...] += value

    def kv_step(step, carry):
        start(step + slots - 1)
        for copy in weight_copies(step, step % slots)[0]:
            copy.wait()
        product(step, step)
        return carry

    lax.fori_loop(0, chunks, kv_step, 0)
    cosine = cos_ref[...]
    sine = sin_ref[...]
    in_low = lax.broadcasted_iota(jnp.int32, cosine.shape, 1) < HD // 2
    half = HD // 2
    for head in range(2):
        low_lanes = slice(2 * head * HD, (2 * head + 1) * HD)
        high_lanes = slice((2 * head + 1) * HD, (2 * head + 2) * HD)
        low = sum_ref[:, low_lanes] + kv_bias_ref[:, low_lanes]
        high = sum_ref[:, high_lanes] + kv_bias_ref[:, high_lanes]
        key = jnp.where(in_low, low, pltpu.roll(high, half, 1))
        value = jnp.where(in_low, pltpu.roll(low, half, 1), high)
        kv_ref[head, :, :HD] = rotated(key, cosine, sine).astype(jnp.bfloat16)
        kv_ref[head, :, HD:] = value.astype(jnp.bfloat16)

    def query_step(step, carry):
        start(step + slots - 1)
        weight_copies(step, step % slots)[1].wait()
        product(step, step - chunks)
        return carry

    lax.fori_loop(chunks, 2 * chunks, query_step, 0)
    for head in range(width // HD):
        lanes = slice(head * HD, (head + 1) * HD)
        out_ref[:, lanes] = rotated(
            sum_ref[:, lanes] + q_bias_ref[:, lanes], cos_ref[...], sin_ref[...]
        ).astype(jnp.bfloat16)
    out_ref[:, width:] = kv_ref[target // 2]
    copy_out.wait()


def cost(width, features):
    return pl.CostEstimate(
        flops=2 * ROWS * features * width,
        transcendentals=0,
        bytes_accessed=2 * features * (width + ROWS),
    )


def project_first(place, texts, images, weights, kv_bias, q_bias, cosine, sine):
    width = q_bias.shape[1]
    features = texts[0].shape[1]
    depth = features // 8
    any_spec = pl.BlockSpec(memory_space=pltpu.HBM)
    whole = lambda shape: pl.BlockSpec(shape, lambda i, place: (0,) * len(shape))
    return pl.pallas_call(
        project_first_kernel,
        grid_spec=pltpu.PrefetchScalarGridSpec(
            num_scalar_prefetch=1,
            grid=(1,),
            in_specs=[any_spec] * 11
            + [whole((1, width)), whole((1, width)), whole((ROWS, HD)), whole((ROWS, HD))],
            out_specs=(
                whole((ROWS, width + 2 * HD)),
                whole((2, ROWS, 2 * HD)),
                any_spec,
            ),
            scratch_shapes=[
                pltpu.VMEM((ROWS, features), jnp.bfloat16),
                pltpu.VMEM((4, depth, width), jnp.bfloat16),
                pltpu.VMEM((ROWS, width), jnp.float32),
                pltpu.SemaphoreType.DMA((64,)),
                pltpu.SemaphoreType.DMA((4, 4)),
                pltpu.SemaphoreType.DMA,
            ],
        ),
        out_shape=(
            jax.ShapeDtypeStruct((ROWS, width + 2 * HD), jnp.bfloat16),
            jax.ShapeDtypeStruct((2, ROWS, 2 * HD), jnp.bfloat16),
            jax.ShapeDtypeStruct((ROWS, features), jnp.bfloat16),
        ),
        compiler_params=pltpu.CompilerParams(vmem_limit_bytes=40 << 20),
        cost_estimate=cost(2 * width, features),
        name="project_first",
    )(place, *texts, *images, weights, kv_bias, q_bias, cosine, sine)


def project_next_kernel(
    target_ref, rows_ref, weight_ref, kv_ref, bias_ref, cos_ref, sin_ref, out_ref, sum_ref
):
    part = pl.program_id(0)
    width = weight_ref.shape[1]
    value = jnp.dot(rows_ref[...], weight_ref[...], preferred_element_type=jnp.float32)

    @pl.when(part == 0)
    def _():
        sum_ref[...] = value

    @pl.when(part > 0)
    def _():
        sum_ref[...] += value

    @pl.when(part == pl.num_programs(0) - 1)
    def _():
        for head in range(width // HD):
            lanes = slice(head * HD, (head + 1) * HD)
            out_ref[:, lanes] = rotated(
                sum_ref[:, lanes] + bias_ref[:, lanes], cos_ref[...], sin_ref[...]
            ).astype(jnp.bfloat16)
        out_ref[:, width:] = kv_ref[0]


def project_next(target, compact, weights, kv, q_bias, cosine, sine):
    width = q_bias.shape[1]
    features = compact.shape[1]
    parts = 8
    depth = features // parts
    whole = lambda shape: pl.BlockSpec(shape, lambda k, target: (0,) * len(shape))
    return pl.pallas_call(
        project_next_kernel,
        grid_spec=pltpu.PrefetchScalarGridSpec(
            num_scalar_prefetch=1,
            grid=(parts,),
            in_specs=[
                pl.BlockSpec((ROWS, depth), lambda k, target: (0, k)),
                pl.BlockSpec((depth, width), lambda k, target: (k * 4 + target[0], 0)),
                pl.BlockSpec((1, ROWS, 2 * HD), lambda k, target: (target[0] // 2, 0, 0)),
                whole((1, width)),
                whole((ROWS, HD)),
                whole((ROWS, HD)),
            ],
            out_specs=whole((ROWS, width + 2 * HD)),
            scratch_shapes=[pltpu.VMEM((ROWS, width), jnp.float32)],
        ),
        out_shape=jax.ShapeDtypeStruct((ROWS, width + 2 * HD), jnp.bfloat16),
        compiler_params=pltpu.CompilerParams(vmem_limit_bytes=32 << 20),
        cost_estimate=cost(width, features),
        name="project_next",
    )(
        target, pltpu.with_memory_space_constraint(compact, pltpu.HBM), weights, kv, q_bias,
        cosine, sine,
    )


def attend_kernel(
    info_ref, text_ref, part0, part1, part2, part3, out_ref, merged_ref, run_ref, mask_ref
):
    parts = (part0, part1, part2, part3)
    step = pl.program_id(0)
    block = out_ref.shape[0]
    width = part0.shape[1]
    mine = info_ref[11]
    run_start = info_ref[8]
    run_end = info_ref[9]
    used = info_ref[10]
    first_unit = (run_start + UNIT - 1) // UNIT
    lag = first_unit * UNIT - run_start

    @pl.when(step == 0)
    def _():
        merged_ref[0:WINDOW, :] = jnp.zeros((WINDOW, width), jnp.bfloat16)
        run_ref[0:128, :] = jnp.zeros((128, width), jnp.bfloat16)
        run_ref[128 + 7 * TR:, :] = jnp.zeros((run_ref.shape[0] - 128 - 7 * TR, width), jnp.bfloat16)

        def tile_step(tile, carry):
            for piece in range(16):
                level, delta = piece // 4, piece % 4
                member = (mine + delta) % 4
                source = pl.multiple_of(tile * 64 + level * UNIT, UNIT)
                target = pl.multiple_of(128 + tile * TR + (4 * level + member) * UNIT, UNIT)
                run_ref[pl.ds(target, UNIT), :] = parts[delta][pl.ds(source, UNIT), :]
            return carry

        lax.fori_loop(0, (run_end - run_start) // TR, tile_step, 0)

        def clear_step(tile, carry):
            target = pl.multiple_of(128 + tile * TR, TR // 2)
            run_ref[pl.ds(target, TR), :] = jnp.zeros((TR, width), jnp.bfloat16)
            return carry

        lax.fori_loop((run_end - run_start) // TR, 7, clear_step, 0)

        def block_step(row, carry):
            for delta in range(4):
                number = row * 4 + (mine + delta) % 4
                begin = number * 128
                for unit in range(8):
                    source = pl.multiple_of(text_ref[number * 8 + unit] * UNIT, UNIT)
                    target = pl.multiple_of(WINDOW + begin + unit * UNIT, UNIT)
                    merged_ref[pl.ds(target, UNIT), :] = parts[delta][pl.ds(source, UNIT), :]

                @pl.when((begin < run_end) & (begin + 128 > run_start))
                def _():
                    origin = pl.multiple_of(128 + UNIT * (8 * number - first_unit), UNIT)
                    window = run_ref[pl.ds(origin, 256), :]
                    place = lax.broadcasted_iota(jnp.int32, (128, 256), 0)
                    taken = lax.broadcasted_iota(jnp.int32, (128, 256), 1)
                    pick = jnp.where(taken == place + lag, 1.0, 0.0).astype(jnp.bfloat16)
                    moved = jnp.dot(pick, window, preferred_element_type=jnp.float32)
                    here = pl.ds(pl.multiple_of(WINDOW + begin, 128), 128)
                    old = merged_ref[here, :].astype(jnp.float32)
                    position = begin + lax.broadcasted_iota(jnp.int32, old.shape, 0)
                    covered = (position >= run_start) & (position < run_end)
                    merged_ref[here, :] = jnp.where(covered, moved, old).astype(jnp.bfloat16)
            return carry

        lax.fori_loop(0, 4, block_step, 0)

    base = pl.multiple_of(step * block, block)
    span = block + WINDOW
    position = base + lax.broadcasted_iota(jnp.int32, (block, 1), 0)
    doc_start = jnp.zeros((block, 1), jnp.int32)
    for doc in range(1, 8):
        doc_start = jnp.where(position >= info_ref[doc], info_ref[doc], doc_start)
    other = base - WINDOW + lax.broadcasted_iota(jnp.int32, (block, span), 1)
    allowed = (other >= doc_start) & (other <= position) & (other < used)
    mask_ref[...] = jnp.where(allowed, 0.0, NEGATIVE)
    queries = pl.ds(pl.multiple_of(WINDOW + base, block), block)
    keys = merged_ref[pl.ds(base, span), 4 * HD:5 * HD]
    values = merged_ref[pl.ds(base, span), 5 * HD:6 * HD]
    factor = HD ** (-0.5) * math.log2(math.e)
    for head in range(4):
        lanes = slice(head * HD, (head + 1) * HD)
        scores = lax.dot_general(
            merged_ref[queries, lanes], keys, (((1,), (1,)), ((), ())),
            preferred_element_type=jnp.float32,
        ) + mask_ref[...]
        peak = jnp.max(scores, axis=-1, keepdims=True)
        exponent = jnp.exp2((scores - peak) * factor)
        inverse = 1.0 / jnp.sum(exponent, axis=-1, keepdims=True)
        probs = (exponent * inverse).astype(jnp.bfloat16)
        mixed = jnp.dot(probs, values, preferred_element_type=jnp.float32)
        out_ref[:, lanes] = jnp.where(position < used, mixed, 0.0).astype(jnp.bfloat16)


def attend(info, text_index, parts):
    block = 256
    shape = parts[0].shape
    width = shape[1]
    return pl.pallas_call(
        attend_kernel,
        grid_spec=pltpu.PrefetchScalarGridSpec(
            num_scalar_prefetch=2,
            grid=(LENGTH // block,),
            in_specs=[pl.BlockSpec(shape, lambda i, a, b: (0, 0))] * 4,
            out_specs=pl.BlockSpec((block, 4 * HD), lambda i, a, b: (i, 0)),
            scratch_shapes=[
                pltpu.VMEM((WINDOW + LENGTH, width), jnp.bfloat16),
                pltpu.VMEM((128 + 7 * TR + 384, width), jnp.bfloat16),
                pltpu.VMEM((block, block + WINDOW), jnp.float32),
            ],
        ),
        out_shape=jax.ShapeDtypeStruct((LENGTH, 4 * HD), jnp.bfloat16),
        compiler_params=pltpu.CompilerParams(vmem_limit_bytes=48 << 20),
        name="attend",
    )(info, text_index, *parts)


def tables(tile_group, tile_offset, seq_len, doc_ids, group, z, y):
    mine = tile_group == group
    present = jnp.any(mine.reshape(8, 4), axis=1)
    count = jnp.sum(mine.astype(jnp.int32))
    run_start = jnp.where(count > 0, jnp.min(jnp.where(mine, tile_offset, LENGTH)), 0)
    run_end = run_start + TR * count
    low_unit = (run_start + UNIT - 1) // UNIT
    high_unit = run_end // UNIT
    eight = jnp.arange(8, dtype=jnp.int32)
    rank = jnp.sum((present[None, :] & (eight[None, :] < eight[:, None])).astype(jnp.int32), axis=1)
    order = jnp.arange(32, dtype=jnp.int32)
    four = jnp.arange(4, dtype=jnp.int32)
    unit_of = 8 * (4 * (order[None, :] // 8) + four[:, None]) + order[None, :] % 8
    before = jnp.sum((unit_of < low_unit).astype(jnp.int32), axis=1)
    hidden = jnp.sum((unit_of < high_unit).astype(jnp.int32), axis=1) - before
    held = (unit_of < low_unit) | (unit_of >= high_unit)
    compact = 4 * count + order[None, :] - jnp.where(unit_of >= high_unit, hidden[:, None], 0)
    compact = jnp.where(held, compact, -1)
    text_index = jnp.maximum(compact, 0).reshape(4, 4, 8).transpose(1, 0, 2).reshape(-1)
    my_before = lax.dynamic_index_in_dim(before, y, 0, keepdims=False)
    my_hidden = lax.dynamic_index_in_dim(hidden, y, 0, keepdims=False)
    member = (z + four) % 4
    my_compact = lax.dynamic_index_in_dim(compact, y, 0, keepdims=False).reshape(4, 8)
    text_place = jnp.take(my_compact, member, axis=0).reshape(-1)
    image_place = jnp.where(eight[None, :] < count, 4 * eight[None, :] + member[:, None], -1)
    image_place = image_place.reshape(-1)
    total = 4 * count + 32 - my_hidden
    place = jnp.concatenate([text_place, image_place, total[None], (y[None] + 2) % 4])
    place = place.astype(jnp.int32)
    is_slot = present[None, :] & (rank[None, :] == eight[:7, None])
    slots = jnp.sum(jnp.where(is_slot, eight[None, :], 0), axis=1).astype(jnp.int32)
    number = jnp.arange(ROWS, dtype=jnp.int32) // UNIT
    inner = jnp.arange(ROWS, dtype=jnp.int32) % UNIT
    image_at = run_start + TR * (number // 4) + UNIT * (4 * (number % 4) + y)
    text_number = number - 4 * count
    text_number = jnp.clip(text_number + jnp.where(text_number >= my_before, my_hidden, 0), 0, 31)
    text_at = 128 * (4 * (text_number // 8) + y) + UNIT * (text_number % 8)
    position = jnp.where(number < 4 * count, image_at, text_at) + inner
    starts = jnp.sum((doc_ids[0][None, :] < eight[:, None]).astype(jnp.int32), axis=1)
    doc_start = jnp.max(
        jnp.where(starts[None, :] <= position[:, None], starts[None, :], 0), axis=1
    )
    in_doc = position - doc_start
    info = jnp.concatenate([starts, run_start[None], run_end[None], seq_len, y[None]])
    return place, slots, text_index, info.astype(jnp.int32), in_doc


def one_device(
    text_rows, image_rows, tile_group, tile_offset, seq_len, doc_ids, norm_gain,
    q_weight, k_weight, v_weight, q_bias, k_bias, v_bias,
):
    group = lax.axis_index("x") * 2 + lax.axis_index("c")
    z = lax.axis_index("z")
    y = lax.axis_index("y")
    depth = q_weight.shape[0] // 8
    gain = norm_gain.reshape(1, -1)

    def own_part(weight):
        return lax.dynamic_slice_in_dim(weight, group * depth, depth, 0)

    weight_part = jnp.concatenate(
        [own_part(q_weight), own_part(k_weight), own_part(v_weight)], axis=1
    )
    weights = lax.all_gather(weight_part, ("x", "c", "y"), axis=0, tiled=True)

    t0 = norm_text(text_rows, gain)
    t3 = shifted(t0, "z", 1)
    t1 = shifted(t0, "z", -1)

    place, slots, text_index, info, in_doc = tables(
        tile_group, tile_offset, seq_len, doc_ids, group, z, y
    )
    row_groups = lax.dynamic_slice_in_dim(tile_group, group * 4, 4)
    matches = row_groups[None, :] == jnp.arange(8, dtype=jnp.int32)[:, None]
    chosen = jnp.sum(jnp.where(matches, jnp.arange(4, dtype=jnp.int32)[None, :], 0), axis=1)
    image_rows, t0 = lax.optimization_barrier((image_rows, t0))
    outgoing = norm_image(image_rows, gain, chosen.astype(jnp.int32))
    arrived = lax.all_to_all(outgoing, ("x", "c"), split_axis=0, concat_axis=0, tiled=True)
    i0 = pick_slots(arrived, slots)
    i3 = shifted(i0, "z", 1)
    i1 = shifted(i0, "z", -1)
    t2a = shifted(t3[:64], "z", 1)
    t2b = shifted(t1[64:], "z", -1)
    i2a = shifted(i3[:4], "z", 1)
    i2b = shifted(i1[4:], "z", -1)

    bias = jnp.concatenate([q_bias, k_bias, v_bias])
    biases = [bias, shifted(bias, "y", -1), shifted(bias, "y", 2), shifted(bias, "y", 1)]
    q_biases = [value[None, :4 * HD] for value in biases]
    kv_bias = jnp.stack([value[4 * HD:] for value in biases])
    member = jnp.arange(4, dtype=jnp.int32)[:, None, None]
    delta = jnp.arange(4, dtype=jnp.int32)[None, :, None]
    kv_bias = jnp.sum(jnp.where((y + delta) % 4 == member, kv_bias[None], 0.0), axis=1)
    kv_bias = kv_bias.reshape(1, -1)
    frequency = THETA ** (-(jnp.arange(HD // 2, dtype=jnp.float32) * 2.0) / HD)
    angles = in_doc.astype(jnp.float32)[:, None] * frequency[None, :]
    cosine = jnp.concatenate([jnp.cos(angles), jnp.cos(angles)], axis=-1)
    sine = jnp.concatenate([-jnp.sin(angles), jnp.sin(angles)], axis=-1)

    out2, kv, compact = project_first(
        place, (t0, t1, t2a, t2b, t3), (i0, i1, i2a, i2b, i3),
        weights, kv_bias, q_biases[2], cosine, sine,
    )
    part2 = shifted(out2, "y", 2)
    outs = {}
    after = kv
    for step in (1, 3, 0):
        target = (y[None] + step) % 4
        outs[step] = project_next(
            target.astype(jnp.int32), compact, weights, after, q_biases[step], cosine, sine
        )
        after, outs[step] = lax.optimization_barrier((after, outs[step]))
    part3 = shifted(outs[1], "y", 1)
    part1 = shifted(outs[3], "y", -1)
    return attend(info, text_index, (outs[0], part1, part2, part3))


def solution(mesh):
    fine = Mesh(mesh.devices.reshape(4, 2, 4, 4), ("x", "c", "z", "y"))
    dp, seq = ("x", "c"), ("z", "y")
    return jax.shard_map(
        one_device,
        mesh=fine,
        in_specs=(
            P(dp + seq, None),
            P(dp, seq, None),
            P(),
            P(),
            P(dp),
            P(dp, None),
            P(),
            P(None, seq),
            P(None, seq),
            P(None, seq),
            P(seq),
            P(seq),
            P(seq),
        ),
        out_specs=P(dp, seq),
        check_vma=False,
    )
```

```python
import math

import jax
import jax.numpy as jnp
from jax import lax
from jax.experimental import pallas as pl
from jax.experimental.pallas import tpu as pltpu
from jax.sharding import Mesh, PartitionSpec as P

TR = 256
UNIT = 16
HD = 128
LENGTH = 2048
CAPACITY = 36
ROWS = CAPACITY * UNIT
WINDOW = 512
THETA = 1000000.0
NEGATIVE = -1e30
EPSILON = 1e-06


def shifted(block, axis, step):
    count = lax.axis_size(axis)
    return lax.ppermute(block, axis, [(low, (low + step) % count) for low in range(count)])


def rms_norm(row_block, gain):
    float_rows = row_block.astype(jnp.float32)
    inv_rms = lax.rsqrt(jnp.mean(float_rows * float_rows, axis=-1, keepdims=True) + EPSILON)
    return (float_rows * inv_rms * gain).astype(jnp.bfloat16)


def norm_text_kernel(rows_ref, gain_ref, out_ref):
    out_ref[...] = rms_norm(rows_ref[...], gain_ref[...])


def norm_text(rows, gain):
    count, features = rows.shape
    step = 2 * UNIT
    return pl.pallas_call(
        norm_text_kernel,
        grid=(count // step,),
        in_specs=[
            pl.BlockSpec((step, features), lambda i: (i, 0)),
            pl.BlockSpec((1, features), lambda i: (0, 0)),
        ],
        out_specs=pl.BlockSpec((step, features), lambda i: (i, 0)),
        out_shape=jax.ShapeDtypeStruct(rows.shape, jnp.bfloat16),
        name="norm_text",
    )(rows, gain)


def norm_image_kernel(chosen_ref, rows_ref, gain_ref, out_ref):
    out_ref[0] = rms_norm(rows_ref[0], gain_ref[...])


def norm_image(pieces, gain, chosen):
    _, piece_rows, features = pieces.shape
    groups = chosen.shape[0]
    return pl.pallas_call(
        norm_image_kernel,
        grid_spec=pltpu.PrefetchScalarGridSpec(
            num_scalar_prefetch=1,
            grid=(groups,),
            in_specs=[
                pl.BlockSpec((1, piece_rows, features), lambda i, chosen: (chosen[i], 0, 0)),
                pl.BlockSpec((1, features), lambda i, chosen: (0, 0)),
            ],
            out_specs=pl.BlockSpec((1, piece_rows, features), lambda i, chosen: (i, 0, 0)),
        ),
        out_shape=jax.ShapeDtypeStruct((groups, piece_rows, features), jnp.bfloat16),
        name="norm_image",
    )(chosen, pieces, gain)


def pick_kernel(chosen_ref, rows_ref, out_ref):
    out_ref[...] = rows_ref[...]


def pick_slots(pieces, chosen):
    _, piece_rows, features = pieces.shape
    count = chosen.shape[0]
    return pl.pallas_call(
        pick_kernel,
        grid_spec=pltpu.PrefetchScalarGridSpec(
            num_scalar_prefetch=1,
            grid=(count,),
            in_specs=[pl.BlockSpec((1, piece_rows, features), lambda i, chosen: (chosen[i], 0, 0))],
            out_specs=pl.BlockSpec((1, piece_rows, features), lambda i, chosen: (i, 0, 0)),
        ),
        out_shape=jax.ShapeDtypeStruct((count, piece_rows, features), jnp.bfloat16),
        name="pick_slots",
    )(chosen, pieces)


def rotated(values, cosine, sine):
    return values * cosine + pltpu.roll(values, HD // 2, 1) * sine


COLUMNS = 256
PIECE = 1024


def weight_tile(own_q, own_kv, pieces, place_ref, weight_buf, sems):
    def copies(tile, slot):
        found = []
        lane = 0
        for delta, first, count in tile:
            lanes = pl.ds(lane, count)
            lane += count
            if delta == 0:
                source = own_kv if first == 512 else own_q.at[:, pl.ds(first, count)]
                found.append((source, weight_buf.at[slot, :, lanes]))
            else:
                for index, piece in enumerate(pieces[delta]):
                    row = pl.multiple_of(place_ref[66 + index // 2] + index % 2 * PIECE, PIECE)
                    found.append(
                        (
                            piece.at[:, pl.ds(first, count)],
                            weight_buf.at[slot, pl.ds(row, PIECE), lanes],
                        )
                    )
        return [
            pltpu.make_async_copy(source, target, sems.at[slot, index])
            for index, (source, target) in enumerate(found)
        ]

    return copies


def run_tiles(tiles, copies, rows_ref, weight_buf, sum_ref, finish, before):
    slots = weight_buf.shape[0]
    for index in range(min(slots, len(tiles))):
        for copy in copies(tiles[index], index):
            copy.start()
    before()

    def step(number, carry):
        slot = number % slots
        for index, tile in enumerate(tiles):
            @pl.when(number == index)
            def _(index=index, tile=tile):
                for copy in copies(tile, index % slots):
                    copy.wait()

        sum_ref[slot] = jnp.dot(
            rows_ref[...], weight_buf[slot], preferred_element_type=jnp.float32
        )
        for index in range(len(tiles)):
            @pl.when(number == index)
            def _(index=index):
                if index + slots < len(tiles):
                    for copy in copies(tiles[index + slots], index % slots):
                        copy.start()
                finish(index, sum_ref.at[index % slots])

        return carry

    lax.fori_loop(0, len(tiles), step, 0)


def project_first_kernel(*refs):
    place_ref = refs[0]
    t0, t1, t2a, t2b, t3, i0, i1, i2a, i2b, i3 = refs[1:11]
    own_q, own_kv = refs[11:13]
    pieces = {1: refs[13:21], 2: refs[21:29], 3: refs[29:37]}
    kv_bias_ref, q_bias_ref, cos_ref, sin_ref, out_ref, kv_ref, compact_ref = refs[37:44]
    rows_ref, weight_buf, sum_ref, sems, weight_sems, copy_sem = refs[44:]
    copies = weight_tile(own_q, own_kv, pieces, place_ref, weight_buf, weight_sems)
    width = q_bias_ref.shape[1]
    copy_out = pltpu.make_async_copy(rows_ref, compact_ref, copy_sem)

    def unit_copy(index):
        delta, slot = index % 32 // 8, index % 8
        if index < 32:
            source = (t0, t1, t2a if slot < 4 else t2b, t3)[delta]
            slot = slot % 4 if delta == 2 else slot
            source = source.at[pl.ds(UNIT * slot, UNIT), :]
        else:
            source = (i0, i1, i2a if slot < 4 else i2b, i3)[delta]
            slot = slot % 4 if delta == 2 else slot
            source = source.at[slot]
        row = pl.multiple_of(UNIT * jnp.maximum(place_ref[index], 0), UNIT)
        return pltpu.make_async_copy(source, rows_ref.at[pl.ds(row, UNIT), :], sems.at[index])

    def assemble():
        total = place_ref[64]
        for unit in range(24, CAPACITY):
            @pl.when(unit >= total)
            def _(unit=unit):
                rows_ref[pl.ds(UNIT * unit, UNIT), :] = jnp.zeros(
                    (UNIT, rows_ref.shape[1]), jnp.bfloat16
                )

        used = [index for index in range(64) if index < 32 or index % 8 < 7]
        for index in used:
            @pl.when(place_ref[index] >= 0)
            def _(index=index):
                unit_copy(index).start()
        for index in used:
            @pl.when(place_ref[index] >= 0)
            def _(index=index):
                unit_copy(index).wait()
        copy_out.start()

    def finish(index, product):
        if index == 1:
            odd = place_ref[65] == 1
            halves = [
                sum_ref[delta // 2, :, pl.ds(delta % 2 * HD, HD)]
                + kv_bias_ref[:, pl.ds(delta * HD, HD)]
                for delta in range(4)
            ]
            in_low = lax.broadcasted_iota(jnp.int32, halves[0].shape, 1) < HD // 2
            ends = (
                (jnp.where(odd, halves[3], halves[0]), jnp.where(odd, halves[0], halves[1])),
                (jnp.where(odd, halves[1], halves[2]), jnp.where(odd, halves[2], halves[3])),
            )
            for head, (low, high) in enumerate(ends):
                key = jnp.where(in_low, low, pltpu.roll(high, HD // 2, 1))
                value = jnp.where(in_low, pltpu.roll(low, HD // 2, 1), high)
                kv_ref[head, :, :HD] = rotated(key, cos_ref[...], sin_ref[...]).astype(
                    jnp.bfloat16
                )
                kv_ref[head, :, HD:] = value.astype(jnp.bfloat16)
            out_ref[:, width:] = kv_ref[1]
        if index >= 2:
            store_heads(out_ref, index - 2, product, q_bias_ref, cos_ref, sin_ref)

    tiles = [
        [(0, 512, HD), (1, 512, HD)], [(2, 512, HD), (3, 512, HD)],
        [(2, 0, COLUMNS)], [(2, COLUMNS, COLUMNS)],
    ]
    run_tiles(tiles, copies, rows_ref, weight_buf, sum_ref, finish, assemble)
    copy_out.wait()


def store_heads(out_ref, part, product, bias_ref, cos_ref, sin_ref):
    for head in range(COLUMNS // HD):
        lanes = slice(part * COLUMNS + head * HD, part * COLUMNS + (head + 1) * HD)
        values = product[:, head * HD:(head + 1) * HD] + bias_ref[:, lanes]
        out_ref[:, lanes] = rotated(values, cos_ref[...], sin_ref[...]).astype(jnp.bfloat16)


def cost(width, features):
    return pl.CostEstimate(
        flops=2 * ROWS * features * width,
        transcendentals=0,
        bytes_accessed=2 * features * (width + ROWS),
    )


def far(values):
    return [pltpu.with_memory_space_constraint(value, pltpu.HBM) for value in values]


def whole(shape):
    return pl.BlockSpec(shape, lambda i, place: (0,) * len(shape))


def project_first(place, texts, images, own, pieces, kv_bias, q_bias, cosine, sine):
    width = q_bias.shape[1]
    features = texts[0].shape[1]
    far_spec = pl.BlockSpec(memory_space=pltpu.HBM)
    flat = [piece for delta in (1, 2, 3) for piece in pieces[delta]]
    return pl.pallas_call(
        project_first_kernel,
        grid_spec=pltpu.PrefetchScalarGridSpec(
            num_scalar_prefetch=1,
            grid=(1,),
            in_specs=[far_spec] * (12 + len(flat))
            + [whole((1, width)), whole((1, width)), whole((ROWS, HD)), whole((ROWS, HD))],
            out_specs=(whole((ROWS, width + 2 * HD)), whole((2, ROWS, 2 * HD)), far_spec),
            scratch_shapes=[
                pltpu.VMEM((ROWS, features), jnp.bfloat16),
                pltpu.VMEM((2, features, COLUMNS), jnp.bfloat16),
                pltpu.VMEM((2, ROWS, COLUMNS), jnp.float32),
                pltpu.SemaphoreType.DMA((64,)),
                pltpu.SemaphoreType.DMA((2, 16)),
                pltpu.SemaphoreType.DMA,
            ],
        ),
        out_shape=(
            jax.ShapeDtypeStruct((ROWS, width + 2 * HD), jnp.bfloat16),
            jax.ShapeDtypeStruct((2, ROWS, 2 * HD), jnp.bfloat16),
            pltpu.HBM((ROWS, features), jnp.bfloat16),
        ),
        compiler_params=pltpu.CompilerParams(vmem_limit_bytes=40 << 20),
        cost_estimate=cost(2 * width, features),
        name="project_first",
    )(place, *far([*texts, *images, *own, *flat]), kv_bias, q_bias, cosine, sine)


def project_near_kernel(*refs):
    place_ref, compact_ref = refs[:2]
    pieces = {1: refs[2:10], 3: refs[10:18]}
    kv_ref, bias1_ref, bias3_ref, cos_ref, sin_ref, out1_ref, out3_ref = refs[18:25]
    rows_ref, weight_buf, sum_ref, row_sem, weight_sems = refs[25:]
    copies = weight_tile(None, None, pieces, place_ref, weight_buf, weight_sems)
    copy_in = pltpu.make_async_copy(compact_ref, rows_ref, row_sem)
    copy_in.start()
    width = bias1_ref.shape[1]
    odd = place_ref[65]
    out1_ref[:, width:] = kv_ref[odd]
    out3_ref[:, width:] = kv_ref[1 - odd]

    def finish(index, product):
        out_ref, bias_ref = ((out1_ref, bias1_ref), (out3_ref, bias3_ref))[index // 2]
        store_heads(out_ref, index % 2, product, bias_ref, cos_ref, sin_ref)

    tiles = [[(delta, first, COLUMNS)] for delta in (1, 3) for first in (0, COLUMNS)]
    run_tiles(tiles, copies, rows_ref, weight_buf, sum_ref, finish, copy_in.wait)


def project_near(place, compact, pieces, kv, bias1, bias3, cosine, sine):
    width = bias1.shape[1]
    features = compact.shape[1]
    far_spec = pl.BlockSpec(memory_space=pltpu.HBM)
    flat = [piece for delta in (1, 3) for piece in pieces[delta]]
    shape = (ROWS, width + 2 * HD)
    return pl.pallas_call(
        project_near_kernel,
        grid_spec=pltpu.PrefetchScalarGridSpec(
            num_scalar_prefetch=1,
            grid=(1,),
            in_specs=[far_spec] * (1 + len(flat))
            + [
                whole((2, ROWS, 2 * HD)), whole((1, width)), whole((1, width)),
                whole((ROWS, HD)), whole((ROWS, HD)),
            ],
            out_specs=(whole(shape), whole(shape)),
            scratch_shapes=[
                pltpu.VMEM((ROWS, features), jnp.bfloat16),
                pltpu.VMEM((2, features, COLUMNS), jnp.bfloat16),
                pltpu.VMEM((2, ROWS, COLUMNS), jnp.float32),
                pltpu.SemaphoreType.DMA,
                pltpu.SemaphoreType.DMA((2, 16)),
            ],
        ),
        out_shape=(jax.ShapeDtypeStruct(shape, jnp.bfloat16),) * 2,
        compiler_params=pltpu.CompilerParams(vmem_limit_bytes=40 << 20),
        cost_estimate=cost(2 * width, features),
        name="project_near",
    )(place, *far([compact, *flat]), kv, bias1, bias3, cosine, sine)


def project_own_kernel(
    place_ref, compact_ref, own_q, kv_ref, bias_ref, cos_ref, sin_ref, out_ref,
    rows_ref, weight_buf, sum_ref, row_sem, weight_sems,
):
    copies = weight_tile(own_q, None, {}, place_ref, weight_buf, weight_sems)
    copy_in = pltpu.make_async_copy(compact_ref, rows_ref, row_sem)
    copy_in.start()
    out_ref[:, bias_ref.shape[1]:] = kv_ref[0]

    def finish(index, product):
        store_heads(out_ref, index, product, bias_ref, cos_ref, sin_ref)

    tiles = [[(0, 0, COLUMNS)], [(0, COLUMNS, COLUMNS)]]
    run_tiles(tiles, copies, rows_ref, weight_buf, sum_ref, finish, copy_in.wait)


def project_own(place, compact, own_q, kv, bias, cosine, sine):
    width = bias.shape[1]
    features = compact.shape[1]
    far_spec = pl.BlockSpec(memory_space=pltpu.HBM)
    shape = (ROWS, width + 2 * HD)
    return pl.pallas_call(
        project_own_kernel,
        grid_spec=pltpu.PrefetchScalarGridSpec(
            num_scalar_prefetch=1,
            grid=(1,),
            in_specs=[far_spec] * 2
            + [
                whole((2, ROWS, 2 * HD)), whole((1, width)), whole((ROWS, HD)), whole((ROWS, HD)),
            ],
            out_specs=whole(shape),
            scratch_shapes=[
                pltpu.VMEM((ROWS, features), jnp.bfloat16),
                pltpu.VMEM((2, features, COLUMNS), jnp.bfloat16),
                pltpu.VMEM((2, ROWS, COLUMNS), jnp.float32),
                pltpu.SemaphoreType.DMA,
                pltpu.SemaphoreType.DMA((2, 16)),
            ],
        ),
        out_shape=jax.ShapeDtypeStruct(shape, jnp.bfloat16),
        compiler_params=pltpu.CompilerParams(vmem_limit_bytes=40 << 20),
        cost_estimate=cost(width, features),
        name="project_own",
    )(place, *far([compact, own_q]), kv, bias, cosine, sine)


def attend_kernel(
    info_ref, text_ref, part0, part1, part2, part3, out_ref, merged_ref, run_ref, mask_ref
):
    parts = (part0, part1, part2, part3)
    step = pl.program_id(0)
    block = out_ref.shape[0]
    width = part0.shape[1]
    mine = info_ref[11]
    run_start = info_ref[8]
    run_end = info_ref[9]
    used = info_ref[10]
    first_unit = (run_start + UNIT - 1) // UNIT
    lag = first_unit * UNIT - run_start

    @pl.when(step == 0)
    def _():
        merged_ref[0:WINDOW, :] = jnp.zeros((WINDOW, width), jnp.bfloat16)
        run_ref[0:128, :] = jnp.zeros((128, width), jnp.bfloat16)
        run_ref[128 + 7 * TR:, :] = jnp.zeros((run_ref.shape[0] - 128 - 7 * TR, width), jnp.bfloat16)

        def tile_step(tile, carry):
            for piece in range(16):
                level, delta = piece // 4, piece % 4
                member = (mine + delta) % 4
                source = pl.multiple_of(tile * 64 + level * UNIT, UNIT)
                target = pl.multiple_of(128 + tile * TR + (4 * level + member) * UNIT, UNIT)
                run_ref[pl.ds(target, UNIT), :] = parts[delta][pl.ds(source, UNIT), :]
            return carry

        lax.fori_loop(0, (run_end - run_start) // TR, tile_step, 0)

        def clear_step(tile, carry):
            target = pl.multiple_of(128 + tile * TR, TR // 2)
            run_ref[pl.ds(target, TR), :] = jnp.zeros((TR, width), jnp.bfloat16)
            return carry

        lax.fori_loop((run_end - run_start) // TR, 7, clear_step, 0)

        def block_step(row, carry):
            for delta in range(4):
                number = row * 4 + (mine + delta) % 4
                begin = number * 128
                for unit in range(8):
                    source = pl.multiple_of(text_ref[number * 8 + unit] * UNIT, UNIT)
                    target = pl.multiple_of(WINDOW + begin + unit * UNIT, UNIT)
                    merged_ref[pl.ds(target, UNIT), :] = parts[delta][pl.ds(source, UNIT), :]

                @pl.when((begin < run_end) & (begin + 128 > run_start))
                def _():
                    origin = pl.multiple_of(128 + UNIT * (8 * number - first_unit), UNIT)
                    window = run_ref[pl.ds(origin, 256), :]
                    place = lax.broadcasted_iota(jnp.int32, (128, 256), 0)
                    taken = lax.broadcasted_iota(jnp.int32, (128, 256), 1)
                    pick = jnp.where(taken == place + lag, 1.0, 0.0).astype(jnp.bfloat16)
                    moved = jnp.dot(pick, window, preferred_element_type=jnp.float32)
                    here = pl.ds(pl.multiple_of(WINDOW + begin, 128), 128)
                    old = merged_ref[here, :].astype(jnp.float32)
                    position = begin + lax.broadcasted_iota(jnp.int32, old.shape, 0)
                    covered = (position >= run_start) & (position < run_end)
                    merged_ref[here, :] = jnp.where(covered, moved, old).astype(jnp.bfloat16)
            return carry

        lax.fori_loop(0, 4, block_step, 0)

    base = pl.multiple_of(step * block, block)
    first_doc = jnp.int32(0)
    for doc in range(1, 8):
        first_doc = jnp.where(base >= info_ref[doc], info_ref[doc], first_doc)
    reach = (base - first_doc + 127) // 128

    def attend_span(span):
        position = base + lax.broadcasted_iota(jnp.int32, (block, 1), 0)
        doc_start = jnp.zeros((block, 1), jnp.int32)
        for doc in range(1, 8):
            doc_start = jnp.where(position >= info_ref[doc], info_ref[doc], doc_start)
        other = base + block - span + lax.broadcasted_iota(jnp.int32, (block, span), 1)
        allowed = (other >= doc_start) & (other <= position) & (other < used)
        mask_ref[:, :span] = jnp.where(allowed, 0.0, NEGATIVE)
        queries = pl.ds(pl.multiple_of(WINDOW + base, block), block)
        window = pl.ds(pl.multiple_of(WINDOW + base + block - span, 128), span)
        keys = merged_ref[window, 4 * HD:5 * HD]
        values = merged_ref[window, 5 * HD:6 * HD]
        factor = HD ** (-0.5) * math.log2(math.e)
        for head in range(4):
            lanes = slice(head * HD, (head + 1) * HD)
            scores = lax.dot_general(
                merged_ref[queries, lanes], keys, (((1,), (1,)), ((), ())),
                preferred_element_type=jnp.float32,
            ) + mask_ref[:, :span]
            peak = jnp.max(scores, axis=-1, keepdims=True)
            exponent = jnp.exp2((scores - peak) * factor)
            inverse = 1.0 / jnp.sum(exponent, axis=-1, keepdims=True)
            probs = (exponent * inverse).astype(jnp.bfloat16)
            mixed = jnp.dot(probs, values, preferred_element_type=jnp.float32)
            out_ref[:, lanes] = jnp.where(position < used, mixed, 0.0).astype(jnp.bfloat16)

    for extra in (1, 2, 3, 4):
        within = reach <= 1 if extra == 1 else reach == extra

        @pl.when(within & (base < used))
        def _(extra=extra):
            attend_span(block + 128 * extra)

    @pl.when(base >= used)
    def _():
        out_ref[...] = jnp.zeros(out_ref.shape, jnp.bfloat16)


def attend(info, text_index, parts):
    block = 128
    shape = parts[0].shape
    width = shape[1]
    return pl.pallas_call(
        attend_kernel,
        grid_spec=pltpu.PrefetchScalarGridSpec(
            num_scalar_prefetch=2,
            grid=(LENGTH // block,),
            in_specs=[pl.BlockSpec(shape, lambda i, a, b: (0, 0))] * 4,
            out_specs=pl.BlockSpec((block, 4 * HD), lambda i, a, b: (i, 0)),
            scratch_shapes=[
                pltpu.VMEM((WINDOW + LENGTH, width), jnp.bfloat16),
                pltpu.VMEM((128 + 7 * TR + 384, width), jnp.bfloat16),
                pltpu.VMEM((block, block + WINDOW), jnp.float32),
            ],
        ),
        out_shape=jax.ShapeDtypeStruct((LENGTH, 4 * HD), jnp.bfloat16),
        compiler_params=pltpu.CompilerParams(vmem_limit_bytes=48 << 20),
        name="attend",
    )(info, text_index, *parts)


def tables(tile_group, tile_offset, seq_len, doc_ids, group, z, y, quarters):
    mine = tile_group == group
    present = jnp.any(mine.reshape(8, 4), axis=1)
    count = jnp.sum(mine.astype(jnp.int32))
    run_start = jnp.where(count > 0, jnp.min(jnp.where(mine, tile_offset, LENGTH)), 0)
    run_end = run_start + TR * count
    low_unit = (run_start + UNIT - 1) // UNIT
    high_unit = run_end // UNIT
    eight = jnp.arange(8, dtype=jnp.int32)
    rank = jnp.sum((present[None, :] & (eight[None, :] < eight[:, None])).astype(jnp.int32), axis=1)
    order = jnp.arange(32, dtype=jnp.int32)
    four = jnp.arange(4, dtype=jnp.int32)
    unit_of = 8 * (4 * (order[None, :] // 8) + four[:, None]) + order[None, :] % 8
    before = jnp.sum((unit_of < low_unit).astype(jnp.int32), axis=1)
    hidden = jnp.sum((unit_of < high_unit).astype(jnp.int32), axis=1) - before
    held = (unit_of < low_unit) | (unit_of >= high_unit)
    compact = 4 * count + order[None, :] - jnp.where(unit_of >= high_unit, hidden[:, None], 0)
    compact = jnp.where(held, compact, -1)
    text_index = jnp.maximum(compact, 0).reshape(4, 4, 8).transpose(1, 0, 2).reshape(-1)
    my_before = lax.dynamic_index_in_dim(before, y, 0, keepdims=False)
    my_hidden = lax.dynamic_index_in_dim(hidden, y, 0, keepdims=False)
    member = (z + four) % 4
    my_compact = lax.dynamic_index_in_dim(compact, y, 0, keepdims=False).reshape(4, 8)
    text_place = jnp.take(my_compact, member, axis=0).reshape(-1)
    image_place = jnp.where(eight[None, :] < count, 4 * eight[None, :] + member[:, None], -1)
    image_place = image_place.reshape(-1)
    total = 4 * count + 32 - my_hidden
    place = jnp.concatenate([text_place, image_place, total[None], y[None] % 2, quarters])
    place = place.astype(jnp.int32)
    is_slot = present[None, :] & (rank[None, :] == eight[:7, None])
    slots = jnp.sum(jnp.where(is_slot, eight[None, :], 0), axis=1).astype(jnp.int32)
    number = jnp.arange(ROWS, dtype=jnp.int32) // UNIT
    inner = jnp.arange(ROWS, dtype=jnp.int32) % UNIT
    image_at = run_start + TR * (number // 4) + UNIT * (4 * (number % 4) + y)
    text_number = number - 4 * count
    text_number = jnp.clip(text_number + jnp.where(text_number >= my_before, my_hidden, 0), 0, 31)
    text_at = 128 * (4 * (text_number // 8) + y) + UNIT * (text_number % 8)
    position = jnp.where(number < 4 * count, image_at, text_at) + inner
    starts = jnp.sum((doc_ids[0][None, :] < eight[:, None]).astype(jnp.int32), axis=1)
    doc_start = jnp.max(
        jnp.where(starts[None, :] <= position[:, None], starts[None, :], 0), axis=1
    )
    in_doc = position - doc_start
    info = jnp.concatenate([starts, run_start[None], run_end[None], seq_len, y[None]])
    return place, slots, text_index, info.astype(jnp.int32), in_doc


def one_device(
    text_rows, image_rows, tile_group, tile_offset, seq_len, doc_ids, norm_gain,
    q_weight, k_weight, v_weight, q_bias, k_bias, v_bias,
):
    x = lax.axis_index("x")
    core = lax.axis_index("c")
    group = x * 2 + core
    z = lax.axis_index("z")
    y = lax.axis_index("y")
    gain = norm_gain.reshape(1, -1)

    t0 = norm_text(text_rows, gain)
    t3 = shifted(t0, "z", 1)
    t1 = shifted(t0, "z", -1)

    quarter = 2 * core + x % 2
    begin, t0 = lax.optimization_barrier((quarter * 2 * PIECE, t0))
    own_kv = jnp.concatenate([k_weight, v_weight], axis=1)

    def own_part(half):
        first = begin + half * PIECE
        return jnp.concatenate(
            [
                lax.dynamic_slice_in_dim(weight, first, PIECE, 0)
                for weight in (q_weight, own_kv)
            ],
            axis=1,
        )

    low, high = own_part(0), own_part(1)
    direct = {}
    direct[1, 0] = shifted(low, "y", -1)
    direct[3, 1] = shifted(high, "y", 1)
    direct[1, 1] = shifted(high, "y", -1)
    direct[3, 0] = shifted(low, "y", 1)
    direct[2, 0] = shifted(direct[1, 0], "y", -1)
    direct[2, 1] = shifted(direct[3, 1], "y", 1)
    across = {key: shifted(value, "x", -1 if key[1] else 1) for key, value in direct.items()}
    pieces = {
        delta: [direct[delta, 0], direct[delta, 1], across[delta, 0], across[delta, 1]]
        for delta in (1, 2, 3)
    }
    pieces = {
        delta: found + [shifted(value, "c", 1) for value in found]
        for delta, found in pieces.items()
    }
    quarters = jnp.stack([quarter ^ 0, quarter ^ 1, quarter ^ 2, quarter ^ 3]) * 2 * PIECE

    place, slots, text_index, info, in_doc = tables(
        tile_group, tile_offset, seq_len, doc_ids, group, z, y, quarters
    )
    row_groups = lax.dynamic_slice_in_dim(tile_group, group * 4, 4)
    matches = row_groups[None, :] == jnp.arange(8, dtype=jnp.int32)[:, None]
    chosen = jnp.sum(jnp.where(matches, jnp.arange(4, dtype=jnp.int32)[None, :], 0), axis=1)
    image_rows, t0 = lax.optimization_barrier((image_rows, t0))
    outgoing = norm_image(image_rows, gain, chosen.astype(jnp.int32))
    arrived = lax.all_to_all(outgoing, ("x", "c"), split_axis=0, concat_axis=0, tiled=True)
    i0 = pick_slots(arrived, slots)
    i3 = shifted(i0, "z", 1)
    i1 = shifted(i0, "z", -1)
    t2a = shifted(t3[:64], "z", 1)
    t2b = shifted(t1[64:], "z", -1)
    i2a = shifted(i3[:4], "z", 1)
    i2b = shifted(i1[4:], "z", -1)

    bias = jnp.concatenate([q_bias, k_bias, v_bias])
    biases = [bias, shifted(bias, "y", -1), shifted(bias, "y", 2), shifted(bias, "y", 1)]
    q_biases = [value[None, :4 * HD] for value in biases]
    kv_bias = jnp.concatenate([value[None, 4 * HD:] for value in biases], axis=1)
    frequency = THETA ** (-(jnp.arange(HD // 2, dtype=jnp.float32) * 2.0) / HD)
    angles = in_doc.astype(jnp.float32)[:, None] * frequency[None, :]
    cosine = jnp.concatenate([jnp.cos(angles), jnp.cos(angles)], axis=-1)
    sine = jnp.concatenate([-jnp.sin(angles), jnp.sin(angles)], axis=-1)

    out2, kv, compact = project_first(
        place, (t0, t1, t2a, t2b, t3), (i0, i1, i2a, i2b, i3), (q_weight, own_kv),
        pieces, kv_bias, q_biases[2], cosine, sine,
    )
    part2 = shifted(out2, "y", 2)
    out1, out3 = project_near(place, compact, pieces, kv, q_biases[1], q_biases[3], cosine, sine)
    part3 = shifted(out1, "y", 1)
    part1 = shifted(out3, "y", -1)
    kv, out1 = lax.optimization_barrier((kv, out1))
    part0 = project_own(place, compact, q_weight, kv, q_biases[0], cosine, sine)
    return attend(info, text_index, (part0, part1, part2, part3))


def solution(mesh):
    fine = Mesh(mesh.devices.reshape(4, 2, 4, 4), ("x", "c", "z", "y"))
    dp, seq = ("x", "c"), ("z", "y")
    return jax.shard_map(
        one_device,
        mesh=fine,
        in_specs=(
            P(dp + seq, None),
            P(dp, seq, None),
            P(),
            P(),
            P(dp),
            P(dp, None),
            P(),
            P(None, seq),
            P(None, seq),
            P(None, seq),
            P(seq),
            P(seq),
            P(seq),
        ),
        out_specs=P(dp, seq),
        check_vma=False,
    )
```

```python
import math

import jax
import jax.numpy as jnp
from jax import lax
from jax.experimental import pallas as pl
from jax.experimental.pallas import tpu as pltpu
from jax.sharding import Mesh, PartitionSpec as P

TR = 256
UNIT = 16
HD = 128
LENGTH = 2048
CAPACITY = 36
ROWS = CAPACITY * UNIT
WINDOW = 512
THETA = 1000000.0
NEGATIVE = -1e30
EPSILON = 1e-06


def shifted(block, axis, step):
    count = lax.axis_size(axis)
    return lax.ppermute(block, axis, [(low, (low + step) % count) for low in range(count)])


def rms_norm(row_block, gain):
    float_rows = row_block.astype(jnp.float32)
    inv_rms = lax.rsqrt(jnp.mean(float_rows * float_rows, axis=-1, keepdims=True) + EPSILON)
    return (float_rows * inv_rms * gain).astype(jnp.bfloat16)


def norm_text_kernel(rows_ref, gain_ref, out_ref):
    out_ref[...] = rms_norm(rows_ref[...], gain_ref[...])


def norm_text(rows, gain, first, count):
    features = rows.shape[1]
    step = 2 * UNIT
    return pl.pallas_call(
        norm_text_kernel,
        grid=(count // step,),
        in_specs=[
            pl.BlockSpec((step, features), lambda i: (first // step + i, 0)),
            pl.BlockSpec((1, features), lambda i: (0, 0)),
        ],
        out_specs=pl.BlockSpec((step, features), lambda i: (i, 0)),
        out_shape=jax.ShapeDtypeStruct((count, features), jnp.bfloat16),
    )(rows, gain)


def norm_image_kernel(chosen_ref, rows_ref, gain_ref, out_ref):
    out_ref[0] = rms_norm(rows_ref[0], gain_ref[...])


def norm_image(pieces, gain, chosen):
    _, piece_rows, features = pieces.shape
    groups = chosen.shape[0]
    return pl.pallas_call(
        norm_image_kernel,
        grid_spec=pltpu.PrefetchScalarGridSpec(
            num_scalar_prefetch=1,
            grid=(groups,),
            in_specs=[
                pl.BlockSpec((1, piece_rows, features), lambda i, chosen: (chosen[i], 0, 0)),
                pl.BlockSpec((1, features), lambda i, chosen: (0, 0)),
            ],
            out_specs=pl.BlockSpec((1, piece_rows, features), lambda i, chosen: (i, 0, 0)),
        ),
        out_shape=jax.ShapeDtypeStruct((groups, piece_rows, features), jnp.bfloat16),
        name="norm_image",
    )(chosen, pieces, gain)


def spread_kernel(chosen_ref, pieces_ref, out_ref, sems):
    def copy(index):
        return pltpu.make_async_copy(
            pieces_ref.at[chosen_ref[index]], out_ref.at[index], sems.at[index]
        )

    for index in range(out_ref.shape[0]):
        copy(index).start()
    for index in range(out_ref.shape[0]):
        copy(index).wait()


def spread(pieces, chosen):
    count = chosen.shape[0]
    far_spec = pl.BlockSpec(memory_space=pltpu.HBM)
    return pl.pallas_call(
        spread_kernel,
        grid_spec=pltpu.PrefetchScalarGridSpec(
            num_scalar_prefetch=1,
            grid=(1,),
            in_specs=[far_spec],
            out_specs=far_spec,
            scratch_shapes=[pltpu.SemaphoreType.DMA((count,))],
        ),
        out_shape=pltpu.HBM((count,) + pieces.shape[1:], jnp.bfloat16),
        name="spread",
    )(chosen, *far([pieces]))


def rotated(values, cosine, sine):
    return values * cosine + pltpu.roll(values, HD // 2, 1) * sine


COLUMNS = 256
PIECE = 1024


def weight_tile(own_q, own_kv, pieces, place_ref, weight_buf, sems):
    def copies(tile, slot):
        found = []
        lane = 0
        for delta, first, count in tile:
            lanes = pl.ds(lane, count)
            lane += count
            if delta == 0:
                source = own_kv if first == 512 else own_q.at[:, pl.ds(first, count)]
                found.append((source, weight_buf.at[slot, :, lanes]))
            else:
                for index, piece in enumerate(pieces[delta]):
                    row = pl.multiple_of(place_ref[66 + index // 2] + index % 2 * PIECE, PIECE)
                    found.append(
                        (
                            piece.at[:, pl.ds(first, count)],
                            weight_buf.at[slot, pl.ds(row, PIECE), lanes],
                        )
                    )
        return [
            pltpu.make_async_copy(source, target, sems.at[slot, index])
            for index, (source, target) in enumerate(found)
        ]

    return copies


def run_tiles(tiles, copies, rows_ref, weight_buf, sum_ref, finish, before):
    slots = weight_buf.shape[0]
    for index in range(min(slots, len(tiles))):
        for copy in copies(tiles[index], index):
            copy.start()
    before()

    def step(number, carry):
        slot = number % slots
        for index, tile in enumerate(tiles):
            @pl.when(number == index)
            def _(index=index, tile=tile):
                for copy in copies(tile, index % slots):
                    copy.wait()

        sum_ref[slot] = jnp.dot(
            rows_ref[...], weight_buf[slot], preferred_element_type=jnp.float32
        )
        for index in range(len(tiles)):
            @pl.when(number == index)
            def _(index=index):
                if index + slots < len(tiles):
                    for copy in copies(tiles[index + slots], index % slots):
                        copy.start()
                finish(index, sum_ref.at[index % slots])

        return carry

    lax.fori_loop(0, len(tiles), step, 0)


def project_first_kernel(*refs):
    place_ref = refs[0]
    sources = refs[1:17]
    own_q, own_kv = refs[17:19]
    pieces = {1: refs[19:27], 2: refs[27:35], 3: refs[35:43]}
    kv_bias_ref, q_bias_ref, cos_ref, sin_ref, out_ref, kv_ref, compact_ref = refs[43:50]
    rows_ref, weight_buf, sum_ref, sems, weight_sems, copy_sem = refs[50:]
    copies = weight_tile(own_q, own_kv, pieces, place_ref, weight_buf, weight_sems)
    width = q_bias_ref.shape[1]
    copy_out = pltpu.make_async_copy(rows_ref, compact_ref, copy_sem)

    def unit_copy(index):
        slot = index % 4
        source = sources[index // 4]
        if index < 32:
            source = source.at[pl.ds(UNIT * slot, UNIT), :]
        else:
            source = source.at[slot]
        row = pl.multiple_of(UNIT * jnp.maximum(place_ref[index], 0), UNIT)
        return pltpu.make_async_copy(source, rows_ref.at[pl.ds(row, UNIT), :], sems.at[index])

    def assemble():
        total = place_ref[64]
        for unit in range(24, CAPACITY):
            @pl.when(unit >= total)
            def _(unit=unit):
                rows_ref[pl.ds(UNIT * unit, UNIT), :] = jnp.zeros(
                    (UNIT, rows_ref.shape[1]), jnp.bfloat16
                )

        used = [index for index in range(64) if index < 32 or index % 8 < 7]
        for index in used:
            @pl.when(place_ref[index] >= 0)
            def _(index=index):
                unit_copy(index).start()
        for index in used:
            @pl.when(place_ref[index] >= 0)
            def _(index=index):
                unit_copy(index).wait()
        copy_out.start()

    def finish(index, product):
        if index == 1:
            odd = place_ref[65] == 1
            halves = [
                sum_ref[delta // 2, :, pl.ds(delta % 2 * HD, HD)]
                + kv_bias_ref[:, pl.ds(delta * HD, HD)]
                for delta in range(4)
            ]
            in_low = lax.broadcasted_iota(jnp.int32, halves[0].shape, 1) < HD // 2
            ends = (
                (jnp.where(odd, halves[3], halves[0]), jnp.where(odd, halves[0], halves[1])),
                (jnp.where(odd, halves[1], halves[2]), jnp.where(odd, halves[2], halves[3])),
            )
            for head, (low, high) in enumerate(ends):
                key = jnp.where(in_low, low, pltpu.roll(high, HD // 2, 1))
                value = jnp.where(in_low, pltpu.roll(low, HD // 2, 1), high)
                kv_ref[head, :, :HD] = rotated(key, cos_ref[...], sin_ref[...]).astype(
                    jnp.bfloat16
                )
                kv_ref[head, :, HD:] = value.astype(jnp.bfloat16)
            out_ref[:, width:] = kv_ref[1]
        if index >= 2:
            store_heads(out_ref, index - 2, product, q_bias_ref, cos_ref, sin_ref)

    tiles = [
        [(0, 512, HD), (1, 512, HD)], [(2, 512, HD), (3, 512, HD)],
        [(2, 0, COLUMNS)], [(2, COLUMNS, COLUMNS)],
    ]
    run_tiles(tiles, copies, rows_ref, weight_buf, sum_ref, finish, assemble)
    copy_out.wait()


def store_heads(out_ref, part, product, bias_ref, cos_ref, sin_ref):
    for head in range(COLUMNS // HD):
        lanes = slice(part * COLUMNS + head * HD, part * COLUMNS + (head + 1) * HD)
        values = product[:, head * HD:(head + 1) * HD] + bias_ref[:, lanes]
        out_ref[:, lanes] = rotated(values, cos_ref[...], sin_ref[...]).astype(jnp.bfloat16)


def cost(width, features):
    return pl.CostEstimate(
        flops=2 * ROWS * features * width,
        transcendentals=0,
        bytes_accessed=2 * features * (width + ROWS),
    )


def far(values):
    return [pltpu.with_memory_space_constraint(value, pltpu.HBM) for value in values]


def whole(shape):
    return pl.BlockSpec(shape, lambda i, place: (0,) * len(shape))


def project_first(place, texts, images, own, pieces, kv_bias, q_bias, cosine, sine):
    width = q_bias.shape[1]
    features = texts[0].shape[1]
    far_spec = pl.BlockSpec(memory_space=pltpu.HBM)
    flat = [piece for delta in (1, 2, 3) for piece in pieces[delta]]
    return pl.pallas_call(
        project_first_kernel,
        grid_spec=pltpu.PrefetchScalarGridSpec(
            num_scalar_prefetch=1,
            grid=(1,),
            in_specs=[far_spec] * (18 + len(flat))
            + [whole((1, width)), whole((1, width)), whole((ROWS, HD)), whole((ROWS, HD))],
            out_specs=(whole((ROWS, width + 2 * HD)), whole((2, ROWS, 2 * HD)), far_spec),
            scratch_shapes=[
                pltpu.VMEM((ROWS, features), jnp.bfloat16),
                pltpu.VMEM((2, features, COLUMNS), jnp.bfloat16),
                pltpu.VMEM((2, ROWS, COLUMNS), jnp.float32),
                pltpu.SemaphoreType.DMA((64,)),
                pltpu.SemaphoreType.DMA((2, 16)),
                pltpu.SemaphoreType.DMA,
            ],
        ),
        out_shape=(
            jax.ShapeDtypeStruct((ROWS, width + 2 * HD), jnp.bfloat16),
            jax.ShapeDtypeStruct((2, ROWS, 2 * HD), jnp.bfloat16),
            pltpu.HBM((ROWS, features), jnp.bfloat16),
        ),
        compiler_params=pltpu.CompilerParams(vmem_limit_bytes=40 << 20),
        cost_estimate=cost(2 * width, features),
        name="project_first",
    )(place, *far([*texts, *images, *own, *flat]), kv_bias, q_bias, cosine, sine)


def project_near_kernel(*refs):
    place_ref, compact_ref = refs[:2]
    pieces = {1: refs[2:10], 3: refs[10:18]}
    kv_ref, bias1_ref, bias3_ref, cos_ref, sin_ref, out1_ref, out3_ref = refs[18:25]
    rows_ref, weight_buf, sum_ref, row_sem, weight_sems = refs[25:]
    copies = weight_tile(None, None, pieces, place_ref, weight_buf, weight_sems)
    copy_in = pltpu.make_async_copy(compact_ref, rows_ref, row_sem)
    copy_in.start()
    width = bias1_ref.shape[1]
    odd = place_ref[65]
    out1_ref[:, width:] = kv_ref[odd]
    out3_ref[:, width:] = kv_ref[1 - odd]

    def finish(index, product):
        out_ref, bias_ref = ((out1_ref, bias1_ref), (out3_ref, bias3_ref))[index // 2]
        store_heads(out_ref, index % 2, product, bias_ref, cos_ref, sin_ref)

    tiles = [[(delta, first, COLUMNS)] for delta in (1, 3) for first in (0, COLUMNS)]
    run_tiles(tiles, copies, rows_ref, weight_buf, sum_ref, finish, copy_in.wait)


def project_near(place, compact, pieces, kv, bias1, bias3, cosine, sine):
    width = bias1.shape[1]
    features = compact.shape[1]
    far_spec = pl.BlockSpec(memory_space=pltpu.HBM)
    flat = [piece for delta in (1, 3) for piece in pieces[delta]]
    shape = (ROWS, width + 2 * HD)
    return pl.pallas_call(
        project_near_kernel,
        grid_spec=pltpu.PrefetchScalarGridSpec(
            num_scalar_prefetch=1,
            grid=(1,),
            in_specs=[far_spec] * (1 + len(flat))
            + [
                whole((2, ROWS, 2 * HD)), whole((1, width)), whole((1, width)),
                whole((ROWS, HD)), whole((ROWS, HD)),
            ],
            out_specs=(whole(shape), whole(shape)),
            scratch_shapes=[
                pltpu.VMEM((ROWS, features), jnp.bfloat16),
                pltpu.VMEM((2, features, COLUMNS), jnp.bfloat16),
                pltpu.VMEM((2, ROWS, COLUMNS), jnp.float32),
                pltpu.SemaphoreType.DMA,
                pltpu.SemaphoreType.DMA((2, 16)),
            ],
        ),
        out_shape=(jax.ShapeDtypeStruct(shape, jnp.bfloat16),) * 2,
        compiler_params=pltpu.CompilerParams(vmem_limit_bytes=40 << 20),
        cost_estimate=cost(2 * width, features),
        name="project_near",
    )(place, *far([compact, *flat]), kv, bias1, bias3, cosine, sine)


def project_own_kernel(
    place_ref, compact_ref, own_q, kv_ref, bias_ref, cos_ref, sin_ref, out_ref,
    rows_ref, weight_buf, sum_ref, row_sem, weight_sems,
):
    copies = weight_tile(own_q, None, {}, place_ref, weight_buf, weight_sems)
    copy_in = pltpu.make_async_copy(compact_ref, rows_ref, row_sem)
    copy_in.start()
    out_ref[:, bias_ref.shape[1]:] = kv_ref[0]

    def finish(index, product):
        store_heads(out_ref, index, product, bias_ref, cos_ref, sin_ref)

    tiles = [[(0, 0, COLUMNS)], [(0, COLUMNS, COLUMNS)]]
    run_tiles(tiles, copies, rows_ref, weight_buf, sum_ref, finish, copy_in.wait)


def project_own(place, compact, own_q, kv, bias, cosine, sine):
    width = bias.shape[1]
    features = compact.shape[1]
    far_spec = pl.BlockSpec(memory_space=pltpu.HBM)
    shape = (ROWS, width + 2 * HD)
    return pl.pallas_call(
        project_own_kernel,
        grid_spec=pltpu.PrefetchScalarGridSpec(
            num_scalar_prefetch=1,
            grid=(1,),
            in_specs=[far_spec] * 2
            + [
                whole((2, ROWS, 2 * HD)), whole((1, width)), whole((ROWS, HD)), whole((ROWS, HD)),
            ],
            out_specs=whole(shape),
            scratch_shapes=[
                pltpu.VMEM((ROWS, features), jnp.bfloat16),
                pltpu.VMEM((2, features, COLUMNS), jnp.bfloat16),
                pltpu.VMEM((2, ROWS, COLUMNS), jnp.float32),
                pltpu.SemaphoreType.DMA,
                pltpu.SemaphoreType.DMA((2, 16)),
            ],
        ),
        out_shape=jax.ShapeDtypeStruct(shape, jnp.bfloat16),
        compiler_params=pltpu.CompilerParams(vmem_limit_bytes=40 << 20),
        cost_estimate=cost(width, features),
        name="project_own",
    )(place, *far([compact, own_q]), kv, bias, cosine, sine)


def attend_kernel(
    info_ref, text_ref, part0, part1, part2, part3, out_ref, merged_ref, run_ref, mask_ref
):
    parts = (part0, part1, part2, part3)
    step = pl.program_id(0)
    block = out_ref.shape[0]
    width = part0.shape[1]
    mine = info_ref[11]
    run_start = info_ref[8]
    run_end = info_ref[9]
    used = info_ref[10]
    first_unit = (run_start + UNIT - 1) // UNIT
    lag = first_unit * UNIT - run_start

    @pl.when(step == 0)
    def _():
        merged_ref[0:WINDOW, :] = jnp.zeros((WINDOW, width), jnp.bfloat16)
        run_ref[0:128, :] = jnp.zeros((128, width), jnp.bfloat16)
        run_ref[128 + 7 * TR:, :] = jnp.zeros((run_ref.shape[0] - 128 - 7 * TR, width), jnp.bfloat16)

        def tile_step(tile, carry):
            for piece in range(16):
                level, delta = piece // 4, piece % 4
                member = (mine + delta) % 4
                source = pl.multiple_of(tile * 64 + level * UNIT, UNIT)
                target = pl.multiple_of(128 + tile * TR + (4 * level + member) * UNIT, UNIT)
                run_ref[pl.ds(target, UNIT), :] = parts[delta][pl.ds(source, UNIT), :]
            return carry

        lax.fori_loop(0, (run_end - run_start) // TR, tile_step, 0)

        def clear_step(tile, carry):
            target = pl.multiple_of(128 + tile * TR, TR // 2)
            run_ref[pl.ds(target, TR), :] = jnp.zeros((TR, width), jnp.bfloat16)
            return carry

        lax.fori_loop((run_end - run_start) // TR, 7, clear_step, 0)

        def block_step(row, carry):
            for delta in range(4):
                number = row * 4 + (mine + delta) % 4
                begin = number * 128
                for unit in range(8):
                    source = pl.multiple_of(text_ref[number * 8 + unit] * UNIT, UNIT)
                    target = pl.multiple_of(WINDOW + begin + unit * UNIT, UNIT)
                    merged_ref[pl.ds(target, UNIT), :] = parts[delta][pl.ds(source, UNIT), :]

                @pl.when((begin < run_end) & (begin + 128 > run_start))
                def _():
                    origin = pl.multiple_of(128 + UNIT * (8 * number - first_unit), UNIT)
                    window = run_ref[pl.ds(origin, 256), :]
                    place = lax.broadcasted_iota(jnp.int32, (128, 256), 0)
                    taken = lax.broadcasted_iota(jnp.int32, (128, 256), 1)
                    pick = jnp.where(taken == place + lag, 1.0, 0.0).astype(jnp.bfloat16)
                    moved = jnp.dot(pick, window, preferred_element_type=jnp.float32)
                    here = pl.ds(pl.multiple_of(WINDOW + begin, 128), 128)
                    old = merged_ref[here, :].astype(jnp.float32)
                    position = begin + lax.broadcasted_iota(jnp.int32, old.shape, 0)
                    covered = (position >= run_start) & (position < run_end)
                    merged_ref[here, :] = jnp.where(covered, moved, old).astype(jnp.bfloat16)
            return carry

        lax.fori_loop(0, 4, block_step, 0)

    base = pl.multiple_of(step * block, block)
    first_doc = jnp.int32(0)
    for doc in range(1, 8):
        first_doc = jnp.where(base >= info_ref[doc], info_ref[doc], first_doc)
    reach = (base - first_doc + 127) // 128

    def attend_span(span):
        position = base + lax.broadcasted_iota(jnp.int32, (block, 1), 0)
        doc_start = jnp.zeros((block, 1), jnp.int32)
        for doc in range(1, 8):
            doc_start = jnp.where(position >= info_ref[doc], info_ref[doc], doc_start)
        other = base + block - span + lax.broadcasted_iota(jnp.int32, (block, span), 1)
        allowed = (other >= doc_start) & (other <= position) & (other < used)
        mask_ref[:, :span] = jnp.where(allowed, 0.0, NEGATIVE)
        queries = pl.ds(pl.multiple_of(WINDOW + base, block), block)
        window = pl.ds(pl.multiple_of(WINDOW + base + block - span, 128), span)
        keys = merged_ref[window, 4 * HD:5 * HD]
        values = merged_ref[window, 5 * HD:6 * HD]
        factor = HD ** (-0.5) * math.log2(math.e)
        heads = [merged_ref[queries, head * HD:(head + 1) * HD] for head in range(4)]
        scores = lax.dot_general(
            jnp.concatenate(heads, axis=0), keys, (((1,), (1,)), ((), ())),
            preferred_element_type=jnp.float32,
        )
        scores = scores.reshape(4, block, span) + mask_ref[:, :span][None]
        peak = jnp.max(scores, axis=-1, keepdims=True)
        exponent = jnp.exp2((scores - peak) * factor)
        inverse = 1.0 / jnp.sum(exponent, axis=-1, keepdims=True)
        probs = (exponent * inverse).astype(jnp.bfloat16).reshape(4 * block, span)
        mixed = jnp.dot(probs, values, preferred_element_type=jnp.float32)
        for head in range(4):
            rows = mixed[head * block:(head + 1) * block]
            out_ref[:, head * HD:(head + 1) * HD] = jnp.where(position < used, rows, 0.0).astype(
                jnp.bfloat16
            )

    for extra in (1, 2, 3, 4):
        within = reach <= 1 if extra == 1 else reach == extra

        @pl.when(within & (base < used))
        def _(extra=extra):
            attend_span(block + 128 * extra)

    @pl.when(base >= used)
    def _():
        out_ref[...] = jnp.zeros(out_ref.shape, jnp.bfloat16)


def attend(info, text_index, parts):
    block = 128
    shape = parts[0].shape
    width = shape[1]
    return pl.pallas_call(
        attend_kernel,
        grid_spec=pltpu.PrefetchScalarGridSpec(
            num_scalar_prefetch=2,
            grid=(LENGTH // block,),
            in_specs=[pl.BlockSpec(shape, lambda i, a, b: (0, 0))] * 4,
            out_specs=pl.BlockSpec((block, 4 * HD), lambda i, a, b: (i, 0)),
            scratch_shapes=[
                pltpu.VMEM((WINDOW + LENGTH, width), jnp.bfloat16),
                pltpu.VMEM((128 + 7 * TR + 384, width), jnp.bfloat16),
                pltpu.VMEM((block, block + WINDOW), jnp.float32),
            ],
        ),
        out_shape=jax.ShapeDtypeStruct((LENGTH, 4 * HD), jnp.bfloat16),
        compiler_params=pltpu.CompilerParams(vmem_limit_bytes=48 << 20),
        name="attend",
    )(info, text_index, *parts)


def tables(tile_group, tile_offset, seq_len, doc_ids, group, z, y, quarters):
    mine = tile_group == group
    present = jnp.any(mine.reshape(8, 4), axis=1)
    count = jnp.sum(mine.astype(jnp.int32))
    run_start = jnp.where(count > 0, jnp.min(jnp.where(mine, tile_offset, LENGTH)), 0)
    run_end = run_start + TR * count
    low_unit = (run_start + UNIT - 1) // UNIT
    high_unit = run_end // UNIT
    eight = jnp.arange(8, dtype=jnp.int32)
    rank = jnp.sum((present[None, :] & (eight[None, :] < eight[:, None])).astype(jnp.int32), axis=1)
    order = jnp.arange(32, dtype=jnp.int32)
    four = jnp.arange(4, dtype=jnp.int32)
    unit_of = 8 * (4 * (order[None, :] // 8) + four[:, None]) + order[None, :] % 8
    before = jnp.sum((unit_of < low_unit).astype(jnp.int32), axis=1)
    hidden = jnp.sum((unit_of < high_unit).astype(jnp.int32), axis=1) - before
    held = (unit_of < low_unit) | (unit_of >= high_unit)
    compact = 4 * count + order[None, :] - jnp.where(unit_of >= high_unit, hidden[:, None], 0)
    compact = jnp.where(held, compact, -1)
    text_index = jnp.maximum(compact, 0).reshape(4, 4, 8).transpose(1, 0, 2).reshape(-1)
    my_before = lax.dynamic_index_in_dim(before, y, 0, keepdims=False)
    my_hidden = lax.dynamic_index_in_dim(hidden, y, 0, keepdims=False)
    member = (z + four) % 4
    my_compact = lax.dynamic_index_in_dim(compact, y, 0, keepdims=False).reshape(4, 8)
    text_place = jnp.take(my_compact, member, axis=0).reshape(-1)
    image_place = jnp.where(eight[None, :] < count, 4 * eight[None, :] + member[:, None], -1)
    image_place = image_place.reshape(-1)
    total = 4 * count + 32 - my_hidden
    place = jnp.concatenate([text_place, image_place, total[None], y[None] % 2, quarters])
    place = place.astype(jnp.int32)
    is_slot = present[None, :] & (rank[None, :] == eight[:7, None])
    slots = jnp.sum(jnp.where(is_slot, eight[None, :], 0), axis=1).astype(jnp.int32)
    number = jnp.arange(ROWS, dtype=jnp.int32) // UNIT
    inner = jnp.arange(ROWS, dtype=jnp.int32) % UNIT
    image_at = run_start + TR * (number // 4) + UNIT * (4 * (number % 4) + y)
    text_number = number - 4 * count
    text_number = jnp.clip(text_number + jnp.where(text_number >= my_before, my_hidden, 0), 0, 31)
    text_at = 128 * (4 * (text_number // 8) + y) + UNIT * (text_number % 8)
    position = jnp.where(number < 4 * count, image_at, text_at) + inner
    starts = jnp.sum((doc_ids[0][None, :] < eight[:, None]).astype(jnp.int32), axis=1)
    doc_start = jnp.max(
        jnp.where(starts[None, :] <= position[:, None], starts[None, :], 0), axis=1
    )
    in_doc = position - doc_start
    info = jnp.concatenate([starts, run_start[None], run_end[None], seq_len, y[None]])
    return place, slots, text_index, info.astype(jnp.int32), in_doc


def one_device(
    text_rows, image_rows, tile_group, tile_offset, seq_len, doc_ids, norm_gain,
    q_weight, k_weight, v_weight, q_bias, k_bias, v_bias,
):
    x = lax.axis_index("x")
    core = lax.axis_index("c")
    group = x * 2 + core
    z = lax.axis_index("z")
    y = lax.axis_index("y")
    gain = norm_gain.reshape(1, -1)

    row_groups = lax.dynamic_slice_in_dim(tile_group, group * 4, 4)
    matches = row_groups[None, :] == jnp.arange(8, dtype=jnp.int32)[:, None]
    chosen = jnp.sum(jnp.where(matches, jnp.arange(4, dtype=jnp.int32)[None, :], 0), axis=1)
    outgoing = spread(image_rows, chosen.astype(jnp.int32))
    arrived = lax.all_to_all(outgoing, ("x", "c"), split_axis=0, concat_axis=0, tiled=True)

    outgoing, text_rows = lax.optimization_barrier((outgoing, text_rows))
    t_low = norm_text(text_rows, gain, 0, 64)
    t3_low = shifted(t_low, "z", 1)
    t1_low = shifted(t_low, "z", -1)

    quarter = 2 * core + x % 2
    begin, t_low = lax.optimization_barrier((quarter * 2 * PIECE, t_low))
    own_kv = jnp.concatenate([k_weight, v_weight], axis=1)

    def own_part(half):
        first = begin + half * PIECE
        return jnp.concatenate(
            [
                lax.dynamic_slice_in_dim(weight, first, PIECE, 0)
                for weight in (q_weight, own_kv)
            ],
            axis=1,
        )

    low, high = own_part(0), own_part(1)
    direct = {}
    direct[1, 0] = shifted(low, "y", -1)
    direct[3, 1] = shifted(high, "y", 1)
    direct[1, 1] = shifted(high, "y", -1)
    direct[3, 0] = shifted(low, "y", 1)

    low, high, text_rows = lax.optimization_barrier((low, high, text_rows))
    t_high = norm_text(text_rows, gain, 64, 64)
    t3_high = shifted(t_high, "z", 1)
    t1_high = shifted(t_high, "z", -1)
    t2_low = shifted(t3_low, "z", 1)
    t2_high = shifted(t1_high, "z", -1)

    direct[2, 0] = shifted(direct[1, 0], "y", -1)
    direct[2, 1] = shifted(direct[3, 1], "y", 1)
    across = {key: shifted(value, "x", -1 if key[1] else 1) for key, value in direct.items()}
    pieces = {
        delta: [direct[delta, 0], direct[delta, 1], across[delta, 0], across[delta, 1]]
        for delta in (1, 2, 3)
    }
    pieces = {
        delta: found + [shifted(value, "c", 1) for value in found]
        for delta, found in pieces.items()
    }
    quarters = jnp.stack([quarter ^ 0, quarter ^ 1, quarter ^ 2, quarter ^ 3]) * 2 * PIECE

    place, slots, text_index, info, in_doc = tables(
        tile_group, tile_offset, seq_len, doc_ids, group, z, y, quarters
    )
    i_low = norm_image(arrived, gain, slots[:4])
    i_high = norm_image(arrived, gain, slots[4:])
    i3_low = shifted(i_low, "z", 1)
    i1_low = shifted(i_low, "z", -1)
    i3_high = shifted(i_high, "z", 1)
    i1_high = shifted(i_high, "z", -1)
    i2_low = shifted(i3_low, "z", 1)
    i2_high = shifted(i1_high, "z", -1)

    bias = jnp.concatenate([q_bias, k_bias, v_bias])
    bias, i_high = lax.optimization_barrier((bias, i_high))
    biases = [
        bias, shifted(bias, "y", -1), shifted(bias, "y", 2),
        shifted(bias, "y", 1),
    ]
    q_biases = [value[None, :4 * HD] for value in biases]
    kv_bias = jnp.concatenate([value[None, 4 * HD:] for value in biases], axis=1)
    frequency = THETA ** (-(jnp.arange(HD // 2, dtype=jnp.float32) * 2.0) / HD)
    angles = in_doc.astype(jnp.float32)[:, None] * frequency[None, :]
    cosine = jnp.concatenate([jnp.cos(angles), jnp.cos(angles)], axis=-1)
    sine = jnp.concatenate([-jnp.sin(angles), jnp.sin(angles)], axis=-1)

    texts = (t_low, t_high, t1_low, t1_high, t2_low, t2_high, t3_low, t3_high)
    images = (i_low, i_high, i1_low, i1_high, i2_low, i2_high, i3_low, i3_high)
    out2, kv, compact = project_first(
        place, texts, images, (q_weight, own_kv), pieces, kv_bias, q_biases[2], cosine, sine
    )
    part2 = shifted(out2, "y", 2)
    out1, out3 = project_near(place, compact, pieces, kv, q_biases[1], q_biases[3], cosine, sine)
    part3 = shifted(out1, "y", 1)
    part1 = shifted(out3, "y", -1)
    kv, out1 = lax.optimization_barrier((kv, out1))
    part0 = project_own(place, compact, q_weight, kv, q_biases[0], cosine, sine)
    return attend(info, text_index, (part0, part1, part2, part3))


def solution(mesh):
    fine = Mesh(mesh.devices.reshape(4, 2, 4, 4), ("x", "c", "z", "y"))
    dp, seq = ("x", "c"), ("z", "y")
    return jax.shard_map(
        one_device,
        mesh=fine,
        in_specs=(
            P(dp + seq, None),
            P(dp, seq, None),
            P(),
            P(),
            P(dp),
            P(dp, None),
            P(),
            P(None, seq),
            P(None, seq),
            P(None, seq),
            P(seq),
            P(seq),
            P(seq),
        ),
        out_specs=P(dp, seq),
        check_vma=False,
    )
```

```python
import math

import jax
import jax.numpy as jnp
from jax import lax
from jax.experimental import pallas as pl
from jax.experimental.pallas import tpu as pltpu
from jax.sharding import Mesh, PartitionSpec as P

TR = 256
UNIT = 16
HD = 128
LENGTH = 2048
CAPACITY = 36
ROWS = CAPACITY * UNIT
WINDOW = 512
THETA = 1000000.0
NEGATIVE = -1e30
EPSILON = 1e-06


def shifted(block, axis, step):
    count = lax.axis_size(axis)
    return lax.ppermute(block, axis, [(low, (low + step) % count) for low in range(count)])


def rms_norm(row_block, gain):
    float_rows = row_block.astype(jnp.float32)
    inv_rms = lax.rsqrt(jnp.mean(float_rows * float_rows, axis=-1, keepdims=True) + EPSILON)
    return (float_rows * inv_rms * gain).astype(jnp.bfloat16)


def norm_text_kernel(rows_ref, gain_ref, out_ref):
    out_ref[...] = rms_norm(rows_ref[...], gain_ref[...])


def norm_text(rows, gain, first, count):
    features = rows.shape[1]
    step = 2 * UNIT
    return pl.pallas_call(
        norm_text_kernel,
        grid=(count // step,),
        in_specs=[
            pl.BlockSpec((step, features), lambda i: (first // step + i, 0)),
            pl.BlockSpec((1, features), lambda i: (0, 0)),
        ],
        out_specs=pl.BlockSpec((step, features), lambda i: (i, 0)),
        out_shape=jax.ShapeDtypeStruct((count, features), jnp.bfloat16),
    )(rows, gain)


def norm_image_kernel(chosen_ref, rows_ref, gain_ref, out_ref):
    out_ref[0] = rms_norm(rows_ref[0], gain_ref[...])


def norm_image(pieces, gain, chosen):
    _, piece_rows, features = pieces.shape
    groups = chosen.shape[0]
    return pl.pallas_call(
        norm_image_kernel,
        grid_spec=pltpu.PrefetchScalarGridSpec(
            num_scalar_prefetch=1,
            grid=(groups,),
            in_specs=[
                pl.BlockSpec((1, piece_rows, features), lambda i, chosen: (chosen[i], 0, 0)),
                pl.BlockSpec((1, features), lambda i, chosen: (0, 0)),
            ],
            out_specs=pl.BlockSpec((1, piece_rows, features), lambda i, chosen: (i, 0, 0)),
        ),
        out_shape=jax.ShapeDtypeStruct((groups, piece_rows, features), jnp.bfloat16),
        name="norm_image",
    )(chosen, pieces, gain)


def spread_kernel(chosen_ref, pieces_ref, out_ref, held_ref, in_sem, sems):
    copy_in = pltpu.make_async_copy(pieces_ref, held_ref, in_sem)
    copy_in.start()
    copy_in.wait()

    def copy(index):
        return pltpu.make_async_copy(
            held_ref.at[chosen_ref[index]], out_ref.at[index], sems.at[index]
        )

    for index in range(out_ref.shape[0]):
        copy(index).start()
    for index in range(out_ref.shape[0]):
        copy(index).wait()


def spread(pieces, chosen):
    count = chosen.shape[0]
    far_spec = pl.BlockSpec(memory_space=pltpu.HBM)
    return pl.pallas_call(
        spread_kernel,
        grid_spec=pltpu.PrefetchScalarGridSpec(
            num_scalar_prefetch=1,
            grid=(1,),
            in_specs=[far_spec],
            out_specs=far_spec,
            scratch_shapes=[
                pltpu.VMEM(pieces.shape, jnp.bfloat16),
                pltpu.SemaphoreType.DMA,
                pltpu.SemaphoreType.DMA((count,)),
            ],
        ),
        out_shape=pltpu.HBM((count,) + pieces.shape[1:], jnp.bfloat16),
        name="spread",
    )(chosen, *far([pieces]))


def rotated(values, cosine, sine):
    return values * cosine + pltpu.roll(values, HD // 2, 1) * sine


COLUMNS = 256
PIECE = 1024


def weight_tile(own_q, own_kv, pieces, place_ref, weight_buf, sems):
    def copies(tile, slot):
        found = []
        lane = 0
        for delta, first, count in tile:
            lanes = pl.ds(lane, count)
            lane += count
            if delta == 0:
                source = own_kv if first == 512 else own_q.at[:, pl.ds(first, count)]
                found.append((source, weight_buf.at[slot, :, lanes]))
            else:
                for index, piece in enumerate(pieces[delta]):
                    row = pl.multiple_of(place_ref[66 + index // 2] + index % 2 * PIECE, PIECE)
                    found.append(
                        (
                            piece.at[:, pl.ds(first, count)],
                            weight_buf.at[slot, pl.ds(row, PIECE), lanes],
                        )
                    )
        return [
            pltpu.make_async_copy(source, target, sems.at[slot, index])
            for index, (source, target) in enumerate(found)
        ]

    return copies


def run_tiles(tiles, copies, rows_ref, weight_buf, sum_ref, finish, before):
    slots = weight_buf.shape[0]
    for copy in copies(tiles[0], 0):
        copy.start()
    before()
    for index in range(1, min(slots, len(tiles))):
        for copy in copies(tiles[index], index):
            copy.start()

    def step(number, carry):
        slot = number % slots
        for index, tile in enumerate(tiles):
            @pl.when(number == index)
            def _(index=index, tile=tile):
                for copy in copies(tile, index % slots):
                    copy.wait()

        half = rows_ref.shape[1] // 2

        def half_step(part, carry):
            inner = pl.ds(pl.multiple_of(part * half, half), half)
            product = jnp.dot(
                rows_ref[:, inner], weight_buf[slot, inner, :], preferred_element_type=jnp.float32
            )

            @pl.when(part == 0)
            def _():
                sum_ref[slot] = product

            @pl.when(part == 1)
            def _():
                sum_ref[slot] += product

            return carry

        lax.fori_loop(0, 2, half_step, 0)
        for index in range(len(tiles)):
            @pl.when(number == index)
            def _(index=index):
                if index + slots < len(tiles):
                    for copy in copies(tiles[index + slots], index % slots):
                        copy.start()
                finish(index, sum_ref.at[index % slots])

        return carry

    lax.fori_loop(0, len(tiles), step, 0)


def project_kv_kernel(*refs):
    place_ref = refs[0]
    sources = refs[1:17]
    own_kv = refs[17]
    pieces = {1: refs[18:26], 2: refs[26:34], 3: refs[34:42]}
    bias_ref, cos_ref, sin_ref = refs[42:45]
    outs, compact_ref = refs[45:49], refs[49]
    rows_ref, weight_buf, sum_ref, sems, weight_sems, copy_sem = refs[50:]
    copies = weight_tile(None, own_kv, pieces, place_ref, weight_buf, weight_sems)
    copy_out = pltpu.make_async_copy(rows_ref, compact_ref, copy_sem)

    def unit_copy(index):
        slot = index % 4
        source = sources[index // 4]
        if index < 32:
            source = source.at[pl.ds(UNIT * slot, UNIT), :]
        else:
            source = source.at[slot]
        row = pl.multiple_of(UNIT * jnp.maximum(place_ref[index], 0), UNIT)
        return pltpu.make_async_copy(source, rows_ref.at[pl.ds(row, UNIT), :], sems.at[index])

    def assemble():
        total = place_ref[64]
        for unit in range(24, CAPACITY):
            @pl.when(unit >= total)
            def _(unit=unit):
                rows_ref[pl.ds(UNIT * unit, UNIT), :] = jnp.zeros(
                    (UNIT, rows_ref.shape[1]), jnp.bfloat16
                )

        used = [index for index in range(64) if index < 32 or index % 8 < 7]
        for index in used:
            @pl.when(place_ref[index] >= 0)
            def _(index=index):
                unit_copy(index).start()
        for index in used:
            @pl.when(place_ref[index] >= 0)
            def _(index=index):
                unit_copy(index).wait()
        copy_out.start()

    def finish(index, product):
        if index == 0:
            return
        odd = place_ref[65] == 1
        halves = [
            sum_ref[delta // 2, :, pl.ds(delta % 2 * HD, HD)] + bias_ref[:, pl.ds(delta * HD, HD)]
            for delta in range(4)
        ]
        in_low = lax.broadcasted_iota(jnp.int32, halves[0].shape, 1) < HD // 2
        ends = (
            (jnp.where(odd, halves[3], halves[0]), jnp.where(odd, halves[0], halves[1])),
            (jnp.where(odd, halves[1], halves[2]), jnp.where(odd, halves[2], halves[3])),
        )
        near, away = [], []
        for group, (low, high) in zip((near, away), ends):
            key = jnp.where(in_low, low, pltpu.roll(high, HD // 2, 1))
            value = jnp.where(in_low, pltpu.roll(low, HD // 2, 1), high)
            group += [rotated(key, cos_ref[...], sin_ref[...]), value]
        for part in range(2):
            lanes = slice(part * HD, (part + 1) * HD)
            outs[0][:, lanes] = near[part].astype(jnp.bfloat16)
            outs[1][:, lanes] = jnp.where(odd, away[part], near[part]).astype(jnp.bfloat16)
            outs[2][:, lanes] = away[part].astype(jnp.bfloat16)
            outs[3][:, lanes] = jnp.where(odd, near[part], away[part]).astype(jnp.bfloat16)

    tiles = [[(0, 512, HD), (1, 512, HD)], [(2, 512, HD), (3, 512, HD)]]
    run_tiles(tiles, copies, rows_ref, weight_buf, sum_ref, finish, assemble)
    copy_out.wait()


def store_heads(out_ref, part, product, bias_ref, cos_ref, sin_ref):
    for head in range(COLUMNS // HD):
        lanes = slice(part * COLUMNS + head * HD, part * COLUMNS + (head + 1) * HD)
        values = product[:, head * HD:(head + 1) * HD] + bias_ref[:, lanes]
        out_ref[:, lanes] = rotated(values, cos_ref[...], sin_ref[...]).astype(jnp.bfloat16)


def cost(width, features):
    return pl.CostEstimate(
        flops=2 * ROWS * features * width,
        transcendentals=0,
        bytes_accessed=2 * features * (width + ROWS),
    )


def far(values):
    return [pltpu.with_memory_space_constraint(value, pltpu.HBM) for value in values]


def whole(shape):
    return pl.BlockSpec(shape, lambda i, place: (0,) * len(shape))


def project_kv(place, texts, images, own_kv, pieces, bias, cosine, sine):
    features = texts[0].shape[1]
    far_spec = pl.BlockSpec(memory_space=pltpu.HBM)
    flat = [piece for delta in (1, 2, 3) for piece in pieces[delta]]
    shape = (ROWS, 2 * HD)
    return pl.pallas_call(
        project_kv_kernel,
        grid_spec=pltpu.PrefetchScalarGridSpec(
            num_scalar_prefetch=1,
            grid=(1,),
            in_specs=[far_spec] * (17 + len(flat))
            + [whole(bias.shape), whole((ROWS, HD)), whole((ROWS, HD))],
            out_specs=(whole(shape),) * 4 + (far_spec,),
            scratch_shapes=[
                pltpu.VMEM((ROWS, features), jnp.bfloat16),
                pltpu.VMEM((2, features, COLUMNS), jnp.bfloat16),
                pltpu.VMEM((2, ROWS, COLUMNS), jnp.float32),
                pltpu.SemaphoreType.DMA((64,)),
                pltpu.SemaphoreType.DMA((2, 16)),
                pltpu.SemaphoreType.DMA,
            ],
        ),
        out_shape=(jax.ShapeDtypeStruct(shape, jnp.bfloat16),) * 4
        + (pltpu.HBM((ROWS, features), jnp.bfloat16),),
        compiler_params=pltpu.CompilerParams(vmem_limit_bytes=40 << 20),
        cost_estimate=cost(2 * COLUMNS, features),
        name="project_kv",
    )(place, *far([*texts, *images, own_kv, *flat]), bias, cosine, sine)


def project_q(place, compact, own_q, pieces, biases, cosine, sine):
    deltas = list(biases)
    width = biases[deltas[0]].shape[1]
    features = compact.shape[1]
    far_spec = pl.BlockSpec(memory_space=pltpu.HBM)
    weights = [own_q] if deltas == [0] else [p for delta in deltas for p in pieces[delta]]
    shape = (ROWS, width)

    def kernel(*refs):
        place_ref, compact_ref = refs[:2]
        weight_refs, refs = refs[2:2 + len(weights)], refs[2 + len(weights):]
        bias_refs, refs = refs[:len(deltas)], refs[len(deltas):]
        cos_ref, sin_ref = refs[:2]
        outs, refs = refs[2:2 + len(deltas)], refs[2 + len(deltas):]
        rows_ref, weight_buf, sum_ref, row_sem, weight_sems = refs
        found = {delta: weight_refs[8 * i:8 * i + 8] for i, delta in enumerate(deltas)}
        copies = weight_tile(weight_refs[0], None, found, place_ref, weight_buf, weight_sems)
        copy_in = pltpu.make_async_copy(compact_ref, rows_ref, row_sem)
        copy_in.start()

        def finish(index, product):
            store_heads(
                outs[index // 2], index % 2, product, bias_refs[index // 2], cos_ref, sin_ref
            )

        tiles = [[(delta, first, COLUMNS)] for delta in deltas for first in (0, COLUMNS)]
        run_tiles(tiles, copies, rows_ref, weight_buf, sum_ref, finish, copy_in.wait)

    return pl.pallas_call(
        kernel,
        grid_spec=pltpu.PrefetchScalarGridSpec(
            num_scalar_prefetch=1,
            grid=(1,),
            in_specs=[far_spec] * (1 + len(weights))
            + [whole((1, width))] * len(deltas)
            + [whole((ROWS, HD)), whole((ROWS, HD))],
            out_specs=(whole(shape),) * len(deltas),
            scratch_shapes=[
                pltpu.VMEM((ROWS, features), jnp.bfloat16),
                pltpu.VMEM((2, features, COLUMNS), jnp.bfloat16),
                pltpu.VMEM((2, ROWS, COLUMNS), jnp.float32),
                pltpu.SemaphoreType.DMA,
                pltpu.SemaphoreType.DMA((2, 16)),
            ],
        ),
        out_shape=(jax.ShapeDtypeStruct(shape, jnp.bfloat16),) * len(deltas),
        compiler_params=pltpu.CompilerParams(vmem_limit_bytes=40 << 20),
        cost_estimate=cost(width * len(deltas), features),
        name="project_q",
    )(place, *far([compact, *weights]), *biases.values(), cosine, sine)


def attend_kernel(
    info_ref, text_ref, q0, q1, q2, q3, kv0, kv1, kv2, kv3, out_ref, merged_ref, run_ref, mask_ref
):
    parts = ((q0, kv0), (q1, kv1), (q2, kv2), (q3, kv3))
    q_width = q0.shape[1]
    step = pl.program_id(0)
    block = out_ref.shape[0]
    width = merged_ref.shape[1]
    mine = info_ref[11]
    run_start = info_ref[8]
    run_end = info_ref[9]
    used = info_ref[10]
    first_unit = (run_start + UNIT - 1) // UNIT
    lag = first_unit * UNIT - run_start

    @pl.when(step == 0)
    def _():
        merged_ref[0:WINDOW, :] = jnp.zeros((WINDOW, width), jnp.bfloat16)
        run_ref[0:128, :] = jnp.zeros((128, width), jnp.bfloat16)
        run_ref[128 + 7 * TR:, :] = jnp.zeros((run_ref.shape[0] - 128 - 7 * TR, width), jnp.bfloat16)

        def tile_step(tile, carry):
            for piece in range(16):
                level, delta = piece // 4, piece % 4
                member = (mine + delta) % 4
                source = pl.multiple_of(tile * 64 + level * UNIT, UNIT)
                target = pl.multiple_of(128 + tile * TR + (4 * level + member) * UNIT, UNIT)
                query, pair = parts[delta]
                run_ref[pl.ds(target, UNIT), :q_width] = query[pl.ds(source, UNIT), :]
                run_ref[pl.ds(target, UNIT), q_width:] = pair[pl.ds(source, UNIT), :]
            return carry

        lax.fori_loop(0, (run_end - run_start) // TR, tile_step, 0)

        def clear_step(tile, carry):
            target = pl.multiple_of(128 + tile * TR, TR // 2)
            run_ref[pl.ds(target, TR), :] = jnp.zeros((TR, width), jnp.bfloat16)
            return carry

        lax.fori_loop((run_end - run_start) // TR, 7, clear_step, 0)

        def block_step(row, carry):
            for delta in range(4):
                number = row * 4 + (mine + delta) % 4
                begin = number * 128
                for unit in range(8):
                    source = pl.multiple_of(text_ref[number * 8 + unit] * UNIT, UNIT)
                    target = pl.multiple_of(WINDOW + begin + unit * UNIT, UNIT)
                    query, pair = parts[delta]
                    merged_ref[pl.ds(target, UNIT), :q_width] = query[pl.ds(source, UNIT), :]
                    merged_ref[pl.ds(target, UNIT), q_width:] = pair[pl.ds(source, UNIT), :]

                @pl.when((begin < run_end) & (begin + 128 > run_start))
                def _():
                    origin = pl.multiple_of(128 + UNIT * (8 * number - first_unit), UNIT)
                    window = run_ref[pl.ds(origin, 256), :]
                    place = lax.broadcasted_iota(jnp.int32, (128, 256), 0)
                    taken = lax.broadcasted_iota(jnp.int32, (128, 256), 1)
                    pick = jnp.where(taken == place + lag, 1.0, 0.0).astype(jnp.bfloat16)
                    moved = jnp.dot(pick, window, preferred_element_type=jnp.float32)
                    here = pl.ds(pl.multiple_of(WINDOW + begin, 128), 128)
                    old = merged_ref[here, :].astype(jnp.float32)
                    position = begin + lax.broadcasted_iota(jnp.int32, old.shape, 0)
                    covered = (position >= run_start) & (position < run_end)
                    merged_ref[here, :] = jnp.where(covered, moved, old).astype(jnp.bfloat16)
            return carry

        lax.fori_loop(0, 4, block_step, 0)

    base = pl.multiple_of(step * block, block)
    first_doc = jnp.int32(0)
    for doc in range(1, 8):
        first_doc = jnp.where(base >= info_ref[doc], info_ref[doc], first_doc)
    reach = (base - first_doc + 127) // 128

    def attend_span(span):
        position = base + lax.broadcasted_iota(jnp.int32, (block, 1), 0)
        doc_start = jnp.zeros((block, 1), jnp.int32)
        for doc in range(1, 8):
            doc_start = jnp.where(position >= info_ref[doc], info_ref[doc], doc_start)
        other = base + block - span + lax.broadcasted_iota(jnp.int32, (block, span), 1)
        allowed = (other >= doc_start) & (other <= position) & (other < used)
        mask_ref[:, :span] = jnp.where(allowed, 0.0, NEGATIVE)
        queries = pl.ds(pl.multiple_of(WINDOW + base, block), block)
        window = pl.ds(pl.multiple_of(WINDOW + base + block - span, 128), span)
        keys = merged_ref[window, 4 * HD:5 * HD]
        values = merged_ref[window, 5 * HD:6 * HD]
        factor = HD ** (-0.5) * math.log2(math.e)
        heads = [merged_ref[queries, head * HD:(head + 1) * HD] for head in range(4)]
        scores = lax.dot_general(
            jnp.concatenate(heads, axis=0), keys, (((1,), (1,)), ((), ())),
            preferred_element_type=jnp.float32,
        )
        scores = scores.reshape(4, block, span) + mask_ref[:, :span][None]
        peak = jnp.max(scores, axis=-1, keepdims=True)
        exponent = jnp.exp2((scores - peak) * factor)
        inverse = 1.0 / jnp.sum(exponent, axis=-1, keepdims=True)
        probs = (exponent * inverse).astype(jnp.bfloat16).reshape(4 * block, span)
        mixed = jnp.dot(probs, values, preferred_element_type=jnp.float32)
        for head in range(4):
            rows = mixed[head * block:(head + 1) * block]
            out_ref[:, head * HD:(head + 1) * HD] = jnp.where(position < used, rows, 0.0).astype(
                jnp.bfloat16
            )

    for extra in (1, 2, 3, 4):
        within = reach <= 1 if extra == 1 else reach == extra

        @pl.when(within & (base < used))
        def _(extra=extra):
            attend_span(block + 128 * extra)

    @pl.when(base >= used)
    def _():
        out_ref[...] = jnp.zeros(out_ref.shape, jnp.bfloat16)


def attend(info, text_index, parts):
    block = 128
    width = parts[0].shape[1] + parts[4].shape[1]
    return pl.pallas_call(
        attend_kernel,
        grid_spec=pltpu.PrefetchScalarGridSpec(
            num_scalar_prefetch=2,
            grid=(LENGTH // block,),
            in_specs=[pl.BlockSpec(part.shape, lambda i, a, b: (0, 0)) for part in parts],
            out_specs=pl.BlockSpec((block, 4 * HD), lambda i, a, b: (i, 0)),
            scratch_shapes=[
                pltpu.VMEM((WINDOW + LENGTH, width), jnp.bfloat16),
                pltpu.VMEM((128 + 7 * TR + 384, width), jnp.bfloat16),
                pltpu.VMEM((block, block + WINDOW), jnp.float32),
            ],
        ),
        out_shape=jax.ShapeDtypeStruct((LENGTH, 4 * HD), jnp.bfloat16),
        compiler_params=pltpu.CompilerParams(vmem_limit_bytes=48 << 20),
        name="attend",
    )(info, text_index, *parts)


def tables(tile_group, tile_offset, seq_len, doc_ids, group, z, y, quarters):
    mine = tile_group == group
    present = jnp.any(mine.reshape(8, 4), axis=1)
    count = jnp.sum(mine.astype(jnp.int32))
    run_start = jnp.where(count > 0, jnp.min(jnp.where(mine, tile_offset, LENGTH)), 0)
    run_end = run_start + TR * count
    low_unit = (run_start + UNIT - 1) // UNIT
    high_unit = run_end // UNIT
    eight = jnp.arange(8, dtype=jnp.int32)
    rank = jnp.sum((present[None, :] & (eight[None, :] < eight[:, None])).astype(jnp.int32), axis=1)
    order = jnp.arange(32, dtype=jnp.int32)
    four = jnp.arange(4, dtype=jnp.int32)
    unit_of = 8 * (4 * (order[None, :] // 8) + four[:, None]) + order[None, :] % 8
    before = jnp.sum((unit_of < low_unit).astype(jnp.int32), axis=1)
    hidden = jnp.sum((unit_of < high_unit).astype(jnp.int32), axis=1) - before
    held = (unit_of < low_unit) | (unit_of >= high_unit)
    compact = 4 * count + order[None, :] - jnp.where(unit_of >= high_unit, hidden[:, None], 0)
    compact = jnp.where(held, compact, -1)
    text_index = jnp.maximum(compact, 0).reshape(4, 4, 8).transpose(1, 0, 2).reshape(-1)
    my_before = lax.dynamic_index_in_dim(before, y, 0, keepdims=False)
    my_hidden = lax.dynamic_index_in_dim(hidden, y, 0, keepdims=False)
    member = (z + four) % 4
    my_compact = lax.dynamic_index_in_dim(compact, y, 0, keepdims=False).reshape(4, 8)
    text_place = jnp.take(my_compact, member, axis=0).reshape(-1)
    image_place = jnp.where(eight[None, :] < count, 4 * eight[None, :] + member[:, None], -1)
    image_place = image_place.reshape(-1)
    total = 4 * count + 32 - my_hidden
    place = jnp.concatenate([text_place, image_place, total[None], y[None] % 2, quarters])
    place = place.astype(jnp.int32)
    is_slot = present[None, :] & (rank[None, :] == eight[:7, None])
    slots = jnp.sum(jnp.where(is_slot, eight[None, :], 0), axis=1).astype(jnp.int32)
    number = jnp.arange(ROWS, dtype=jnp.int32) // UNIT
    inner = jnp.arange(ROWS, dtype=jnp.int32) % UNIT
    image_at = run_start + TR * (number // 4) + UNIT * (4 * (number % 4) + y)
    text_number = number - 4 * count
    text_number = jnp.clip(text_number + jnp.where(text_number >= my_before, my_hidden, 0), 0, 31)
    text_at = 128 * (4 * (text_number // 8) + y) + UNIT * (text_number % 8)
    position = jnp.where(number < 4 * count, image_at, text_at) + inner
    starts = jnp.sum((doc_ids[0][None, :] < eight[:, None]).astype(jnp.int32), axis=1)
    doc_start = jnp.max(
        jnp.where(starts[None, :] <= position[:, None], starts[None, :], 0), axis=1
    )
    in_doc = position - doc_start
    info = jnp.concatenate([starts, run_start[None], run_end[None], seq_len, y[None]])
    return place, slots, text_index, info.astype(jnp.int32), in_doc


def one_device(
    text_rows, image_rows, tile_group, tile_offset, seq_len, doc_ids, norm_gain,
    q_weight, k_weight, v_weight, q_bias, k_bias, v_bias,
):
    x = lax.axis_index("x")
    core = lax.axis_index("c")
    group = x * 2 + core
    z = lax.axis_index("z")
    y = lax.axis_index("y")
    gain = norm_gain.reshape(1, -1)

    row_groups = lax.dynamic_slice_in_dim(tile_group, group * 4, 4)
    matches = row_groups[None, :] == jnp.arange(8, dtype=jnp.int32)[:, None]
    chosen = jnp.sum(jnp.where(matches, jnp.arange(4, dtype=jnp.int32)[None, :], 0), axis=1)
    outgoing = spread(image_rows, chosen.astype(jnp.int32))
    arrived = lax.all_to_all(outgoing, ("x", "c"), split_axis=0, concat_axis=0, tiled=True)

    outgoing, text_rows = lax.optimization_barrier((outgoing, text_rows))
    t_low = norm_text(text_rows, gain, 0, 64)
    t3_low = shifted(t_low, "z", 1)
    t1_low = shifted(t_low, "z", -1)

    quarter = 2 * core + x % 2
    begin, t_low = lax.optimization_barrier((quarter * 2 * PIECE, t_low))
    own_kv = jnp.concatenate([k_weight, v_weight], axis=1)

    def own_part(half):
        first = begin + half * PIECE
        return jnp.concatenate(
            [
                lax.dynamic_slice_in_dim(weight, first, PIECE, 0)
                for weight in (q_weight, own_kv)
            ],
            axis=1,
        )

    low, high = own_part(0), own_part(1)
    direct = {}
    direct[1, 0] = shifted(low, "y", -1)
    direct[3, 1] = shifted(high, "y", 1)
    direct[1, 1] = shifted(high, "y", -1)
    direct[3, 0] = shifted(low, "y", 1)

    low, high, text_rows = lax.optimization_barrier((low, high, text_rows))
    t_high = norm_text(text_rows, gain, 64, 64)
    t3_high = shifted(t_high, "z", 1)
    t1_high = shifted(t_high, "z", -1)
    t2_low = shifted(t3_low, "z", 1)
    t2_high = shifted(t1_high, "z", -1)

    direct[2, 0] = shifted(direct[1, 0], "y", -1)
    direct[2, 1] = shifted(direct[3, 1], "y", 1)
    across = {key: shifted(value, "x", -1 if key[1] else 1) for key, value in direct.items()}
    pieces = {
        delta: [direct[delta, 0], direct[delta, 1], across[delta, 0], across[delta, 1]]
        for delta in (1, 2, 3)
    }
    pieces = {
        delta: found + [shifted(value, "c", 1) for value in found]
        for delta, found in pieces.items()
    }
    quarters = jnp.stack([quarter ^ 0, quarter ^ 1, quarter ^ 2, quarter ^ 3]) * 2 * PIECE

    place, slots, text_index, info, in_doc = tables(
        tile_group, tile_offset, seq_len, doc_ids, group, z, y, quarters
    )
    i_low = norm_image(arrived, gain, slots[:4])
    i_high = norm_image(arrived, gain, slots[4:])
    i3_low = shifted(i_low, "z", 1)
    i1_low = shifted(i_low, "z", -1)
    i3_high = shifted(i_high, "z", 1)
    i1_high = shifted(i_high, "z", -1)
    i2_low = shifted(i3_low, "z", 1)
    i2_high = shifted(i1_high, "z", -1)

    bias = jnp.concatenate([q_bias, k_bias, v_bias])
    bias, i_high = lax.optimization_barrier((bias, i_high))
    biases = [
        bias, shifted(bias, "y", -1), shifted(bias, "y", 2),
        shifted(bias, "y", 1),
    ]
    q_biases = [value[None, :4 * HD] for value in biases]
    kv_bias = jnp.concatenate([value[None, 4 * HD:] for value in biases], axis=1)
    frequency = THETA ** (-(jnp.arange(HD // 2, dtype=jnp.float32) * 2.0) / HD)
    angles = in_doc.astype(jnp.float32)[:, None] * frequency[None, :]
    cosine = jnp.concatenate([jnp.cos(angles), jnp.cos(angles)], axis=-1)
    sine = jnp.concatenate([-jnp.sin(angles), jnp.sin(angles)], axis=-1)

    texts = (t_low, t_high, t1_low, t1_high, t2_low, t2_high, t3_low, t3_high)
    images = (i_low, i_high, i1_low, i1_high, i2_low, i2_high, i3_low, i3_high)
    *pairs, compact = project_kv(place, texts, images, own_kv, pieces, kv_bias, cosine, sine)
    queries = {}
    after = compact
    for deltas in ((2,), (1, 3), (0,)):
        found = project_q(
            place, after, q_weight, pieces,
            {delta: q_biases[delta] for delta in deltas}, cosine, sine,
        )
        after, *found = lax.optimization_barrier((after, *found))
        queries.update(zip(deltas, found))
    parts = []
    for values in (queries, pairs):
        parts.append(values[0])
        parts += [shifted(values[4 - delta], "y", -delta) for delta in (1, 2, 3)]
    return attend(info, text_index, parts)


def solution(mesh):
    fine = Mesh(mesh.devices.reshape(4, 2, 4, 4), ("x", "c", "z", "y"))
    dp, seq = ("x", "c"), ("z", "y")
    return jax.shard_map(
        one_device,
        mesh=fine,
        in_specs=(
            P(dp + seq, None),
            P(dp, seq, None),
            P(),
            P(),
            P(dp),
            P(dp, None),
            P(),
            P(None, seq),
            P(None, seq),
            P(None, seq),
            P(seq),
            P(seq),
            P(seq),
        ),
        out_specs=P(dp, seq),
        check_vma=False,
    )
```

```python
import math

import jax
import jax.numpy as jnp
from jax import lax
from jax.experimental import pallas as pl
from jax.experimental.pallas import tpu as pltpu
from jax.sharding import Mesh, PartitionSpec as P

TR = 256
UNIT = 16
HD = 128
LENGTH = 2048
CAPACITY = 36
ROWS = CAPACITY * UNIT
WINDOW = 512
THETA = 1000000.0
NEGATIVE = -1e30
EPSILON = 1e-06


def shifted(block, axis, step):
    count = lax.axis_size(axis)
    return lax.ppermute(block, axis, [(low, (low + step) % count) for low in range(count)])


def rms_norm(row_block, gain):
    float_rows = row_block.astype(jnp.float32)
    inv_rms = lax.rsqrt(jnp.mean(float_rows * float_rows, axis=-1, keepdims=True) + EPSILON)
    return (float_rows * inv_rms * gain).astype(jnp.bfloat16)


def norm_text_kernel(rows_ref, gain_ref, out_ref):
    out_ref[...] = rms_norm(rows_ref[...], gain_ref[...])


def norm_text(rows, gain, first, count):
    features = rows.shape[1]
    step = 2 * UNIT
    return pl.pallas_call(
        norm_text_kernel,
        grid=(count // step,),
        in_specs=[
            pl.BlockSpec((step, features), lambda i: (first // step + i, 0)),
            pl.BlockSpec((1, features), lambda i: (0, 0)),
        ],
        out_specs=pl.BlockSpec((step, features), lambda i: (i, 0)),
        out_shape=jax.ShapeDtypeStruct((count, features), jnp.bfloat16),
    )(rows, gain)


def norm_image_kernel(chosen_ref, rows_ref, gain_ref, out_ref):
    out_ref[0] = rms_norm(rows_ref[0], gain_ref[...])


def norm_image(pieces, gain, chosen):
    _, piece_rows, features = pieces.shape
    groups = chosen.shape[0]
    return pl.pallas_call(
        norm_image_kernel,
        grid_spec=pltpu.PrefetchScalarGridSpec(
            num_scalar_prefetch=1,
            grid=(groups,),
            in_specs=[
                pl.BlockSpec((1, piece_rows, features), lambda i, chosen: (chosen[i], 0, 0)),
                pl.BlockSpec((1, features), lambda i, chosen: (0, 0)),
            ],
            out_specs=pl.BlockSpec((1, piece_rows, features), lambda i, chosen: (i, 0, 0)),
        ),
        out_shape=jax.ShapeDtypeStruct((groups, piece_rows, features), jnp.bfloat16),
        name="norm_image",
    )(chosen, pieces, gain)


def spread_kernel(chosen_ref, pieces_ref, out_ref, held_ref, in_sem, sems):
    copy_in = pltpu.make_async_copy(pieces_ref, held_ref, in_sem)
    copy_in.start()
    copy_in.wait()

    def copy(index):
        return pltpu.make_async_copy(
            held_ref.at[chosen_ref[index]], out_ref.at[index], sems.at[index]
        )

    for index in range(out_ref.shape[0]):
        copy(index).start()
    for index in range(out_ref.shape[0]):
        copy(index).wait()


def spread(pieces, chosen):
    count = chosen.shape[0]
    far_spec = pl.BlockSpec(memory_space=pltpu.HBM)
    return pl.pallas_call(
        spread_kernel,
        grid_spec=pltpu.PrefetchScalarGridSpec(
            num_scalar_prefetch=1,
            grid=(1,),
            in_specs=[far_spec],
            out_specs=far_spec,
            scratch_shapes=[
                pltpu.VMEM(pieces.shape, jnp.bfloat16),
                pltpu.SemaphoreType.DMA,
                pltpu.SemaphoreType.DMA((count,)),
            ],
        ),
        out_shape=pltpu.HBM((count,) + pieces.shape[1:], jnp.bfloat16),
        name="spread",
    )(chosen, *far([pieces]))


def rotated(values, cosine, sine):
    return values * cosine + pltpu.roll(values, HD // 2, 1) * sine


COLUMNS = 256
PIECE = 1024


def weight_tile(own_q, own_kv, pieces, place_ref, weight_buf, sems):
    def copies(tile, slot):
        found = []
        lane = 0
        for delta, first, count in tile:
            lanes = pl.ds(lane, count)
            lane += count
            if delta == 0 and first == 512:
                found.append((own_kv, weight_buf.at[slot, :, lanes]))
            elif delta == 0:
                for index in range(8):
                    rows = pl.ds(index * PIECE, PIECE)
                    source = own_q.at[rows, pl.ds(first, count)]
                    found.append((source, weight_buf.at[slot, rows, lanes]))
            else:
                for index, piece in enumerate(pieces[delta]):
                    row = pl.multiple_of(place_ref[66 + index // 2] + index % 2 * PIECE, PIECE)
                    found.append(
                        (
                            piece.at[:, pl.ds(first, count)],
                            weight_buf.at[slot, pl.ds(row, PIECE), lanes],
                        )
                    )
        return [
            pltpu.make_async_copy(source, target, sems.at[slot, index])
            for index, (source, target) in enumerate(found)
        ]

    return copies


def run_tiles(tiles, copies, rows_ref, weight_buf, sum_ref, finish, before):
    slots = weight_buf.shape[0]
    for copy in copies(tiles[0], 0):
        copy.start()
    before()
    for index in range(1, min(slots, len(tiles))):
        for copy in copies(tiles[index], index):
            copy.start()

    def step(number, carry):
        slot = number % slots
        for index, tile in enumerate(tiles):
            @pl.when(number == index)
            def _(index=index, tile=tile):
                for copy in copies(tile, index % slots):
                    copy.wait()

        sum_ref[slot] = jnp.dot(
            rows_ref[...], weight_buf[slot], preferred_element_type=jnp.float32
        )
        for index in range(len(tiles)):
            @pl.when(number == index)
            def _(index=index):
                if index + slots < len(tiles):
                    for copy in copies(tiles[index + slots], index % slots):
                        copy.start()
                finish(index, sum_ref.at[index % slots])

        return carry

    lax.fori_loop(0, len(tiles), step, 0)


def project_kv_kernel(*refs):
    place_ref = refs[0]
    sources = refs[1:17]
    own_kv = refs[17]
    pieces = {1: refs[18:26], 2: refs[26:34], 3: refs[34:42]}
    bias_ref, q_bias_ref, cos_ref, sin_ref = refs[42:46]
    outs, out_ref, compact_ref = refs[46:50], refs[50], refs[51]
    rows_ref, weight_buf, sum_ref, sems, weight_sems, copy_sem = refs[52:]
    copies = weight_tile(None, own_kv, pieces, place_ref, weight_buf, weight_sems)
    copy_out = pltpu.make_async_copy(rows_ref, compact_ref, copy_sem)

    def unit_copy(index):
        slot = index % 4
        source = sources[index // 4]
        if index < 32:
            source = source.at[pl.ds(UNIT * slot, UNIT), :]
        else:
            source = source.at[slot]
        row = pl.multiple_of(UNIT * jnp.maximum(place_ref[index], 0), UNIT)
        return pltpu.make_async_copy(source, rows_ref.at[pl.ds(row, UNIT), :], sems.at[index])

    def assemble():
        total = place_ref[64]
        for unit in range(24, CAPACITY):
            @pl.when(unit >= total)
            def _(unit=unit):
                rows_ref[pl.ds(UNIT * unit, UNIT), :] = jnp.zeros(
                    (UNIT, rows_ref.shape[1]), jnp.bfloat16
                )

        used = [index for index in range(64) if index < 32 or index % 8 < 7]
        for index in used:
            @pl.when(place_ref[index] >= 0)
            def _(index=index):
                unit_copy(index).start()
        for index in used:
            @pl.when(place_ref[index] >= 0)
            def _(index=index):
                unit_copy(index).wait()
        copy_out.start()

    def finish(index, product):
        if index >= 2:
            store_heads(out_ref, index - 2, product, q_bias_ref, cos_ref, sin_ref)
        if index != 1:
            return
        odd = place_ref[65] == 1
        halves = [
            sum_ref[delta // 2, :, pl.ds(delta % 2 * HD, HD)] + bias_ref[:, pl.ds(delta * HD, HD)]
            for delta in range(4)
        ]
        in_low = lax.broadcasted_iota(jnp.int32, halves[0].shape, 1) < HD // 2
        ends = (
            (jnp.where(odd, halves[3], halves[0]), jnp.where(odd, halves[0], halves[1])),
            (jnp.where(odd, halves[1], halves[2]), jnp.where(odd, halves[2], halves[3])),
        )
        near, away = [], []
        for group, (low, high) in zip((near, away), ends):
            key = jnp.where(in_low, low, pltpu.roll(high, HD // 2, 1))
            value = jnp.where(in_low, pltpu.roll(low, HD // 2, 1), high)
            group += [rotated(key, cos_ref[...], sin_ref[...]), value]
        for part in range(2):
            lanes = slice(part * HD, (part + 1) * HD)
            outs[0][:, lanes] = near[part].astype(jnp.bfloat16)
            outs[1][:, lanes] = jnp.where(odd, away[part], near[part]).astype(jnp.bfloat16)
            outs[2][:, lanes] = away[part].astype(jnp.bfloat16)
            outs[3][:, lanes] = jnp.where(odd, near[part], away[part]).astype(jnp.bfloat16)

    tiles = [
        [(0, 512, HD), (1, 512, HD)], [(2, 512, HD), (3, 512, HD)],
        [(2, 0, COLUMNS)], [(2, COLUMNS, COLUMNS)],
    ]
    run_tiles(tiles, copies, rows_ref, weight_buf, sum_ref, finish, assemble)
    copy_out.wait()


def store_heads(out_ref, part, product, bias_ref, cos_ref, sin_ref):
    for head in range(COLUMNS // HD):
        lanes = slice(part * COLUMNS + head * HD, part * COLUMNS + (head + 1) * HD)
        values = product[:, head * HD:(head + 1) * HD] + bias_ref[:, lanes]
        out_ref[:, lanes] = rotated(values, cos_ref[...], sin_ref[...]).astype(jnp.bfloat16)


def cost(width, features):
    return pl.CostEstimate(
        flops=2 * ROWS * features * width,
        transcendentals=0,
        bytes_accessed=2 * features * (width + ROWS),
    )


def far(values):
    return [pltpu.with_memory_space_constraint(value, pltpu.HBM) for value in values]


def whole(shape):
    return pl.BlockSpec(shape, lambda i, place: (0,) * len(shape))


def project_kv(place, texts, images, own_kv, pieces, bias, q_bias, cosine, sine):
    query_shape = (ROWS, q_bias.shape[1])
    features = texts[0].shape[1]
    far_spec = pl.BlockSpec(memory_space=pltpu.HBM)
    flat = [piece for delta in (1, 2, 3) for piece in pieces[delta]]
    shape = (ROWS, 2 * HD)
    return pl.pallas_call(
        project_kv_kernel,
        grid_spec=pltpu.PrefetchScalarGridSpec(
            num_scalar_prefetch=1,
            grid=(1,),
            in_specs=[far_spec] * (17 + len(flat))
            + [whole(bias.shape), whole(q_bias.shape), whole((ROWS, HD)), whole((ROWS, HD))],
            out_specs=(whole(shape),) * 4 + (whole(query_shape), far_spec),
            scratch_shapes=[
                pltpu.VMEM((ROWS, features), jnp.bfloat16),
                pltpu.VMEM((2, features, COLUMNS), jnp.bfloat16),
                pltpu.VMEM((2, ROWS, COLUMNS), jnp.float32),
                pltpu.SemaphoreType.DMA((64,)),
                pltpu.SemaphoreType.DMA((2, 16)),
                pltpu.SemaphoreType.DMA,
            ],
        ),
        out_shape=(jax.ShapeDtypeStruct(shape, jnp.bfloat16),) * 4
        + (
            jax.ShapeDtypeStruct(query_shape, jnp.bfloat16),
            pltpu.HBM((ROWS, features), jnp.bfloat16),
        ),
        compiler_params=pltpu.CompilerParams(vmem_limit_bytes=40 << 20),
        cost_estimate=cost(4 * COLUMNS, features),
        name="project_kv",
    )(place, *far([*texts, *images, own_kv, *flat]), bias, q_bias, cosine, sine)


def project_q(place, compact, own_q, pieces, biases, cosine, sine):
    deltas = list(biases)
    width = biases[deltas[0]].shape[1]
    features = compact.shape[1]
    far_spec = pl.BlockSpec(memory_space=pltpu.HBM)
    weights = [own_q] if deltas == [0] else [p for delta in deltas for p in pieces[delta]]
    shape = (ROWS, width)

    def kernel(*refs):
        place_ref, compact_ref = refs[:2]
        weight_refs, refs = refs[2:2 + len(weights)], refs[2 + len(weights):]
        bias_refs, refs = refs[:len(deltas)], refs[len(deltas):]
        cos_ref, sin_ref = refs[:2]
        outs, refs = refs[2:2 + len(deltas)], refs[2 + len(deltas):]
        rows_ref, weight_buf, sum_ref, row_sem, weight_sems = refs
        found = {delta: weight_refs[8 * i:8 * i + 8] for i, delta in enumerate(deltas)}
        copies = weight_tile(weight_refs[0], None, found, place_ref, weight_buf, weight_sems)
        share = ROWS // 6
        copies_in = [
            pltpu.make_async_copy(
                compact_ref.at[pl.ds(part * share, share), :],
                rows_ref.at[pl.ds(part * share, share), :],
                row_sem.at[part],
            )
            for part in range(6)
        ]
        for copy in copies_in:
            copy.start()

        def rows_here():
            for copy in copies_in:
                copy.wait()

        def finish(index, product):
            store_heads(
                outs[index // 2], index % 2, product, bias_refs[index // 2], cos_ref, sin_ref
            )

        tiles = [[(delta, first, COLUMNS)] for delta in deltas for first in (0, COLUMNS)]
        run_tiles(tiles, copies, rows_ref, weight_buf, sum_ref, finish, rows_here)

    return pl.pallas_call(
        kernel,
        grid_spec=pltpu.PrefetchScalarGridSpec(
            num_scalar_prefetch=1,
            grid=(1,),
            in_specs=[far_spec] * (1 + len(weights))
            + [whole((1, width))] * len(deltas)
            + [whole((ROWS, HD)), whole((ROWS, HD))],
            out_specs=(whole(shape),) * len(deltas),
            scratch_shapes=[
                pltpu.VMEM((ROWS, features), jnp.bfloat16),
                pltpu.VMEM((2, features, COLUMNS), jnp.bfloat16),
                pltpu.VMEM((2, ROWS, COLUMNS), jnp.float32),
                pltpu.SemaphoreType.DMA((6,)),
                pltpu.SemaphoreType.DMA((2, 16)),
            ],
        ),
        out_shape=(jax.ShapeDtypeStruct(shape, jnp.bfloat16),) * len(deltas),
        compiler_params=pltpu.CompilerParams(vmem_limit_bytes=40 << 20),
        cost_estimate=cost(width * len(deltas), features),
        name="project_q",
    )(place, *far([compact, *weights]), *biases.values(), cosine, sine)


def attend_kernel(
    info_ref, text_ref, q0, q1, q2, q3, kv0, kv1, kv2, kv3, out_ref, merged_ref, run_ref, mask_ref
):
    parts = ((q0, kv0), (q1, kv1), (q2, kv2), (q3, kv3))
    q_width = q0.shape[1]
    step = pl.program_id(0)
    block = out_ref.shape[0]
    width = merged_ref.shape[1]
    mine = info_ref[11]
    run_start = info_ref[8]
    run_end = info_ref[9]
    used = info_ref[10]
    first_unit = (run_start + UNIT - 1) // UNIT
    lag = first_unit * UNIT - run_start

    @pl.when(step == 0)
    def _():
        merged_ref[0:WINDOW, :] = jnp.zeros((WINDOW, width), jnp.bfloat16)
        run_ref[0:128, :] = jnp.zeros((128, width), jnp.bfloat16)
        run_ref[128 + 7 * TR:, :] = jnp.zeros((run_ref.shape[0] - 128 - 7 * TR, width), jnp.bfloat16)

        def tile_step(tile, carry):
            for piece in range(16):
                level, delta = piece // 4, piece % 4
                member = (mine + delta) % 4
                source = pl.multiple_of(tile * 64 + level * UNIT, UNIT)
                target = pl.multiple_of(128 + tile * TR + (4 * level + member) * UNIT, UNIT)
                query, pair = parts[delta]
                run_ref[pl.ds(target, UNIT), :q_width] = query[pl.ds(source, UNIT), :]
                run_ref[pl.ds(target, UNIT), q_width:] = pair[pl.ds(source, UNIT), :]
            return carry

        lax.fori_loop(0, (run_end - run_start) // TR, tile_step, 0)

        def clear_step(tile, carry):
            target = pl.multiple_of(128 + tile * TR, TR // 2)
            run_ref[pl.ds(target, TR), :] = jnp.zeros((TR, width), jnp.bfloat16)
            return carry

        lax.fori_loop((run_end - run_start) // TR, 7, clear_step, 0)

        def block_step(row, carry):
            for delta in range(4):
                number = row * 4 + (mine + delta) % 4
                begin = number * 128
                for unit in range(8):
                    source = pl.multiple_of(text_ref[number * 8 + unit] * UNIT, UNIT)
                    target = pl.multiple_of(WINDOW + begin + unit * UNIT, UNIT)
                    query, pair = parts[delta]
                    merged_ref[pl.ds(target, UNIT), :q_width] = query[pl.ds(source, UNIT), :]
                    merged_ref[pl.ds(target, UNIT), q_width:] = pair[pl.ds(source, UNIT), :]

                @pl.when((begin < run_end) & (begin + 128 > run_start))
                def _():
                    origin = pl.multiple_of(128 + UNIT * (8 * number - first_unit), UNIT)
                    window = run_ref[pl.ds(origin, 256), :]
                    place = lax.broadcasted_iota(jnp.int32, (128, 256), 0)
                    taken = lax.broadcasted_iota(jnp.int32, (128, 256), 1)
                    pick = jnp.where(taken == place + lag, 1.0, 0.0).astype(jnp.bfloat16)
                    moved = jnp.dot(pick, window, preferred_element_type=jnp.float32)
                    here = pl.ds(pl.multiple_of(WINDOW + begin, 128), 128)
                    old = merged_ref[here, :].astype(jnp.float32)
                    position = begin + lax.broadcasted_iota(jnp.int32, old.shape, 0)
                    covered = (position >= run_start) & (position < run_end)
                    merged_ref[here, :] = jnp.where(covered, moved, old).astype(jnp.bfloat16)
            return carry

        lax.fori_loop(0, 4, block_step, 0)

    base = pl.multiple_of(step * block, block)
    first_doc = jnp.int32(0)
    for doc in range(1, 8):
        first_doc = jnp.where(base >= info_ref[doc], info_ref[doc], first_doc)
    reach = (base - first_doc + 127) // 128

    def attend_span(span):
        position = base + lax.broadcasted_iota(jnp.int32, (block, 1), 0)
        doc_start = jnp.zeros((block, 1), jnp.int32)
        for doc in range(1, 8):
            doc_start = jnp.where(position >= info_ref[doc], info_ref[doc], doc_start)
        other = base + block - span + lax.broadcasted_iota(jnp.int32, (block, span), 1)
        allowed = (other >= doc_start) & (other <= position) & (other < used)
        mask_ref[:, :span] = jnp.where(allowed, 0.0, NEGATIVE)
        queries = pl.ds(pl.multiple_of(WINDOW + base, block), block)
        window = pl.ds(pl.multiple_of(WINDOW + base + block - span, 128), span)
        keys = merged_ref[window, 4 * HD:5 * HD]
        values = merged_ref[window, 5 * HD:6 * HD]
        factor = HD ** (-0.5) * math.log2(math.e)
        heads = [merged_ref[queries, head * HD:(head + 1) * HD] for head in range(4)]
        scores = lax.dot_general(
            jnp.concatenate(heads, axis=0), keys, (((1,), (1,)), ((), ())),
            preferred_element_type=jnp.float32,
        )
        scores = scores.reshape(4, block, span) + mask_ref[:, :span][None]
        peak = jnp.max(scores, axis=-1, keepdims=True)
        exponent = jnp.exp2((scores - peak) * factor)
        inverse = 1.0 / jnp.sum(exponent, axis=-1, keepdims=True)
        probs = (exponent * inverse).astype(jnp.bfloat16).reshape(4 * block, span)
        mixed = jnp.dot(probs, values, preferred_element_type=jnp.float32)
        for head in range(4):
            rows = mixed[head * block:(head + 1) * block]
            out_ref[:, head * HD:(head + 1) * HD] = jnp.where(position < used, rows, 0.0).astype(
                jnp.bfloat16
            )

    for extra in (1, 2, 3, 4):
        within = reach <= 1 if extra == 1 else reach == extra

        @pl.when(within & (base < used))
        def _(extra=extra):
            attend_span(block + 128 * extra)

    @pl.when(base >= used)
    def _():
        out_ref[...] = jnp.zeros(out_ref.shape, jnp.bfloat16)


def attend(info, text_index, parts):
    block = 128
    width = parts[0].shape[1] + parts[4].shape[1]
    return pl.pallas_call(
        attend_kernel,
        grid_spec=pltpu.PrefetchScalarGridSpec(
            num_scalar_prefetch=2,
            grid=(LENGTH // block,),
            in_specs=[pl.BlockSpec(part.shape, lambda i, a, b: (0, 0)) for part in parts],
            out_specs=pl.BlockSpec((block, 4 * HD), lambda i, a, b: (i, 0)),
            scratch_shapes=[
                pltpu.VMEM((WINDOW + LENGTH, width), jnp.bfloat16),
                pltpu.VMEM((128 + 7 * TR + 384, width), jnp.bfloat16),
                pltpu.VMEM((block, block + WINDOW), jnp.float32),
            ],
        ),
        out_shape=jax.ShapeDtypeStruct((LENGTH, 4 * HD), jnp.bfloat16),
        compiler_params=pltpu.CompilerParams(vmem_limit_bytes=48 << 20),
        name="attend",
    )(info, text_index, *parts)


def tables(tile_group, tile_offset, seq_len, doc_ids, group, z, y, quarters):
    mine = tile_group == group
    present = jnp.any(mine.reshape(8, 4), axis=1)
    count = jnp.sum(mine.astype(jnp.int32))
    run_start = jnp.where(count > 0, jnp.min(jnp.where(mine, tile_offset, LENGTH)), 0)
    run_end = run_start + TR * count
    low_unit = (run_start + UNIT - 1) // UNIT
    high_unit = run_end // UNIT
    eight = jnp.arange(8, dtype=jnp.int32)
    rank = jnp.sum((present[None, :] & (eight[None, :] < eight[:, None])).astype(jnp.int32), axis=1)
    order = jnp.arange(32, dtype=jnp.int32)
    four = jnp.arange(4, dtype=jnp.int32)
    unit_of = 8 * (4 * (order[None, :] // 8) + four[:, None]) + order[None, :] % 8
    before = jnp.sum((unit_of < low_unit).astype(jnp.int32), axis=1)
    hidden = jnp.sum((unit_of < high_unit).astype(jnp.int32), axis=1) - before
    held = (unit_of < low_unit) | (unit_of >= high_unit)
    compact = 4 * count + order[None, :] - jnp.where(unit_of >= high_unit, hidden[:, None], 0)
    compact = jnp.where(held, compact, -1)
    text_index = jnp.maximum(compact, 0).reshape(4, 4, 8).transpose(1, 0, 2).reshape(-1)
    my_before = lax.dynamic_index_in_dim(before, y, 0, keepdims=False)
    my_hidden = lax.dynamic_index_in_dim(hidden, y, 0, keepdims=False)
    member = (z + four) % 4
    my_compact = lax.dynamic_index_in_dim(compact, y, 0, keepdims=False).reshape(4, 8)
    text_place = jnp.take(my_compact, member, axis=0).reshape(-1)
    image_place = jnp.where(eight[None, :] < count, 4 * eight[None, :] + member[:, None], -1)
    image_place = image_place.reshape(-1)
    total = 4 * count + 32 - my_hidden
    place = jnp.concatenate([text_place, image_place, total[None], y[None] % 2, quarters])
    place = place.astype(jnp.int32)
    is_slot = present[None, :] & (rank[None, :] == eight[:7, None])
    slots = jnp.sum(jnp.where(is_slot, eight[None, :], 0), axis=1).astype(jnp.int32)
    number = jnp.arange(ROWS, dtype=jnp.int32) // UNIT
    inner = jnp.arange(ROWS, dtype=jnp.int32) % UNIT
    image_at = run_start + TR * (number // 4) + UNIT * (4 * (number % 4) + y)
    text_number = number - 4 * count
    text_number = jnp.clip(text_number + jnp.where(text_number >= my_before, my_hidden, 0), 0, 31)
    text_at = 128 * (4 * (text_number // 8) + y) + UNIT * (text_number % 8)
    position = jnp.where(number < 4 * count, image_at, text_at) + inner
    starts = jnp.sum((doc_ids[0][None, :] < eight[:, None]).astype(jnp.int32), axis=1)
    doc_start = jnp.max(
        jnp.where(starts[None, :] <= position[:, None], starts[None, :], 0), axis=1
    )
    in_doc = position - doc_start
    info = jnp.concatenate([starts, run_start[None], run_end[None], seq_len, y[None]])
    return place, slots, text_index, info.astype(jnp.int32), in_doc


def one_device(
    text_rows, image_rows, tile_group, tile_offset, seq_len, doc_ids, norm_gain,
    q_weight, k_weight, v_weight, q_bias, k_bias, v_bias,
):
    x = lax.axis_index("x")
    core = lax.axis_index("c")
    group = x * 2 + core
    z = lax.axis_index("z")
    y = lax.axis_index("y")
    gain = norm_gain.reshape(1, -1)

    quarter = 2 * core + x % 2
    own_kv = jnp.concatenate([k_weight, v_weight], axis=1)

    def own_part(half):
        first = quarter * 2 * PIECE + half * PIECE
        return jnp.concatenate(
            [
                lax.dynamic_slice_in_dim(weight, first, PIECE, 0)
                for weight in (q_weight, own_kv)
            ],
            axis=1,
        )

    low, high = own_part(0), own_part(1)
    direct = {}
    direct[1, 0] = shifted(low, "y", -1)
    direct[3, 1] = shifted(high, "y", 1)
    direct[1, 1] = shifted(high, "y", -1)
    direct[3, 0] = shifted(low, "y", 1)

    low, high, text_rows = lax.optimization_barrier((low, high, text_rows))
    t_low = norm_text(text_rows, gain, 0, 64)
    t3_low = shifted(t_low, "z", 1)
    t1_low = shifted(t_low, "z", -1)

    row_groups = lax.dynamic_slice_in_dim(tile_group, group * 4, 4)
    matches = row_groups[None, :] == jnp.arange(8, dtype=jnp.int32)[:, None]
    chosen = jnp.sum(jnp.where(matches, jnp.arange(4, dtype=jnp.int32)[None, :], 0), axis=1)
    image_rows, t_low = lax.optimization_barrier((image_rows, t_low))
    outgoing = spread(image_rows, chosen.astype(jnp.int32))
    arrived = lax.all_to_all(outgoing, ("x", "c"), split_axis=0, concat_axis=0, tiled=True)

    outgoing, text_rows = lax.optimization_barrier((outgoing, text_rows))
    t_high = norm_text(text_rows, gain, 64, 64)
    t3_high = shifted(t_high, "z", 1)
    t1_high = shifted(t_high, "z", -1)
    t2_low = shifted(t3_low, "z", 1)
    t2_high = shifted(t1_high, "z", -1)

    direct[2, 0] = shifted(direct[1, 0], "y", -1)
    direct[2, 1] = shifted(direct[3, 1], "y", 1)
    across = {key: shifted(value, "x", -1 if key[1] else 1) for key, value in direct.items()}
    pieces = {
        delta: [direct[delta, 0], direct[delta, 1], across[delta, 0], across[delta, 1]]
        for delta in (1, 2, 3)
    }
    pieces = {
        delta: found + [shifted(value, "c", 1) for value in found]
        for delta, found in pieces.items()
    }
    quarters = jnp.stack([quarter ^ 0, quarter ^ 1, quarter ^ 2, quarter ^ 3]) * 2 * PIECE

    doc_ids, direct[2, 0] = lax.optimization_barrier((doc_ids, direct[2, 0]))
    place, slots, text_index, info, in_doc = tables(
        tile_group, tile_offset, seq_len, doc_ids, group, z, y, quarters
    )
    i_low = norm_image(arrived, gain, slots[:4])
    i_high = norm_image(arrived, gain, slots[4:])
    i3_low = shifted(i_low, "z", 1)
    i1_low = shifted(i_low, "z", -1)
    i3_high = shifted(i_high, "z", 1)
    i1_high = shifted(i_high, "z", -1)
    i2_low = shifted(i3_low, "z", 1)
    i2_high = shifted(i1_high, "z", -1)

    bias = jnp.concatenate([q_bias, k_bias, v_bias])
    bias, i_high = lax.optimization_barrier((bias, i_high))
    biases = [
        bias, shifted(bias, "y", -1), shifted(bias, "y", 2),
        shifted(bias, "y", 1),
    ]
    q_biases = [value[None, :4 * HD] for value in biases]
    kv_bias = jnp.concatenate([value[None, 4 * HD:] for value in biases], axis=1)
    frequency = THETA ** (-(jnp.arange(HD // 2, dtype=jnp.float32) * 2.0) / HD)
    angles = in_doc.astype(jnp.float32)[:, None] * frequency[None, :]
    cosine = jnp.concatenate([jnp.cos(angles), jnp.cos(angles)], axis=-1)
    sine = jnp.concatenate([-jnp.sin(angles), jnp.sin(angles)], axis=-1)

    texts = (t_low, t_high, t1_low, t1_high, t2_low, t2_high, t3_low, t3_high)
    images = (i_low, i_high, i1_low, i1_high, i2_low, i2_high, i3_low, i3_high)
    *pairs, far_query, compact = project_kv(
        place, texts, images, own_kv, pieces, kv_bias, q_biases[2], cosine, sine
    )
    queries = {2: far_query}
    after = compact
    for deltas in ((1, 3), (0,)):
        found = project_q(
            place, after, q_weight, pieces,
            {delta: q_biases[delta] for delta in deltas}, cosine, sine,
        )
        after, *found = lax.optimization_barrier((after, *found))
        queries.update(zip(deltas, found))
    parts = []
    for values in (queries, pairs):
        parts.append(values[0])
        parts += [shifted(values[4 - delta], "y", -delta) for delta in (1, 2, 3)]
    return attend(info, text_index, parts)


def solution(mesh):
    fine = Mesh(mesh.devices.reshape(4, 2, 4, 4), ("x", "c", "z", "y"))
    dp, seq = ("x", "c"), ("z", "y")
    return jax.shard_map(
        one_device,
        mesh=fine,
        in_specs=(
            P(dp + seq, None),
            P(dp, seq, None),
            P(),
            P(),
            P(dp),
            P(dp, None),
            P(),
            P(None, seq),
            P(None, seq),
            P(None, seq),
            P(seq),
            P(seq),
            P(seq),
        ),
        out_specs=P(dp, seq),
        check_vma=False,
    )
```

```python
import math

import jax
import jax.numpy as jnp
from jax import lax
from jax.experimental import pallas as pl
from jax.experimental.pallas import tpu as pltpu
from jax.sharding import Mesh, PartitionSpec as P

TR = 256
UNIT = 16
HD = 128
LENGTH = 2048
CAPACITY = 36
ROWS = CAPACITY * UNIT
WINDOW = 512
THETA = 1000000.0
NEGATIVE = -1e30
EPSILON = 1e-06


def shifted(block, axis, step):
    count = lax.axis_size(axis)
    return lax.ppermute(block, axis, [(low, (low + step) % count) for low in range(count)])


def rms_norm(row_block, gain):
    float_rows = row_block.astype(jnp.float32)
    inv_rms = lax.rsqrt(jnp.mean(float_rows * float_rows, axis=-1, keepdims=True) + EPSILON)
    return (float_rows * inv_rms * gain).astype(jnp.bfloat16)


def norm_text_kernel(rows_ref, gain_ref, out_ref):
    out_ref[...] = rms_norm(rows_ref[...], gain_ref[...])


def norm_text(rows, gain, first, count):
    features = rows.shape[1]
    step = 2 * UNIT
    return pl.pallas_call(
        norm_text_kernel,
        grid=(count // step,),
        in_specs=[
            pl.BlockSpec((step, features), lambda i: (first // step + i, 0)),
            pl.BlockSpec((1, features), lambda i: (0, 0)),
        ],
        out_specs=pl.BlockSpec((step, features), lambda i: (i, 0)),
        out_shape=jax.ShapeDtypeStruct((count, features), jnp.bfloat16),
    )(rows, gain)


def norm_image_kernel(chosen_ref, rows_ref, gain_ref, out_ref):
    out_ref[0] = rms_norm(rows_ref[0], gain_ref[...])


def norm_image(pieces, gain, chosen):
    _, piece_rows, features = pieces.shape
    groups = chosen.shape[0]
    return pl.pallas_call(
        norm_image_kernel,
        grid_spec=pltpu.PrefetchScalarGridSpec(
            num_scalar_prefetch=1,
            grid=(groups,),
            in_specs=[
                pl.BlockSpec((1, piece_rows, features), lambda i, chosen: (chosen[i], 0, 0)),
                pl.BlockSpec((1, features), lambda i, chosen: (0, 0)),
            ],
            out_specs=pl.BlockSpec((1, piece_rows, features), lambda i, chosen: (i, 0, 0)),
        ),
        out_shape=jax.ShapeDtypeStruct((groups, piece_rows, features), jnp.bfloat16),
        name="norm_image",
    )(chosen, pieces, gain)


def spread_kernel(chosen_ref, pieces_ref, out_ref, held_ref, in_sem, sems):
    copy_in = pltpu.make_async_copy(pieces_ref, held_ref, in_sem)
    copy_in.start()
    copy_in.wait()

    def copy(index):
        return pltpu.make_async_copy(
            held_ref.at[chosen_ref[index]], out_ref.at[index], sems.at[index]
        )

    for index in range(out_ref.shape[0]):
        copy(index).start()
    for index in range(out_ref.shape[0]):
        copy(index).wait()


def spread(pieces, chosen):
    count = chosen.shape[0]
    far_spec = pl.BlockSpec(memory_space=pltpu.HBM)
    return pl.pallas_call(
        spread_kernel,
        grid_spec=pltpu.PrefetchScalarGridSpec(
            num_scalar_prefetch=1,
            grid=(1,),
            in_specs=[far_spec],
            out_specs=far_spec,
            scratch_shapes=[
                pltpu.VMEM(pieces.shape, jnp.bfloat16),
                pltpu.SemaphoreType.DMA,
                pltpu.SemaphoreType.DMA((count,)),
            ],
        ),
        out_shape=pltpu.HBM((count,) + pieces.shape[1:], jnp.bfloat16),
        name="spread",
    )(chosen, *far([pieces]))


def rotated(values, cosine, sine):
    return values * cosine + pltpu.roll(values, HD // 2, 1) * sine


COLUMNS = 256
PIECE = 1024


def weight_tile(own_q, own_kv, pieces, place_ref, weight_buf, sems):
    def copies(tile, slot):
        found = []
        lane = 0
        for delta, first, count in tile:
            lanes = pl.ds(lane, count)
            lane += count
            if delta == 0 and first == 512:
                found.append((own_kv, weight_buf.at[slot, :, lanes]))
            elif delta == 0:
                for index in range(8):
                    rows = pl.ds(index * PIECE, PIECE)
                    source = own_q.at[rows, pl.ds(first, count)]
                    found.append((source, weight_buf.at[slot, rows, lanes]))
            else:
                for index, piece in enumerate(pieces[delta]):
                    row = pl.multiple_of(place_ref[66 + index // 2] + index % 2 * PIECE, PIECE)
                    found.append(
                        (
                            piece.at[:, pl.ds(first, count)],
                            weight_buf.at[slot, pl.ds(row, PIECE), lanes],
                        )
                    )
        return [
            pltpu.make_async_copy(source, target, sems.at[slot, index])
            for index, (source, target) in enumerate(found)
        ]

    return copies


def run_tiles(tiles, copies, rows_ref, weight_buf, sum_ref, finish, before):
    slots = weight_buf.shape[0]
    for copy in copies(tiles[0], 0):
        copy.start()
    before()
    for index in range(1, min(slots, len(tiles))):
        for copy in copies(tiles[index], index):
            copy.start()

    def step(number, carry):
        slot = number % slots
        for index, tile in enumerate(tiles):
            @pl.when(number == index)
            def _(index=index, tile=tile):
                for copy in copies(tile, index % slots):
                    copy.wait()

        sum_ref[slot] = jnp.dot(
            rows_ref[...], weight_buf[slot], preferred_element_type=jnp.float32
        )
        for index in range(len(tiles)):
            @pl.when(number == index)
            def _(index=index):
                if index + slots < len(tiles):
                    for copy in copies(tiles[index + slots], index % slots):
                        copy.start()
                finish(index, sum_ref.at[index % slots])

        return carry

    lax.fori_loop(0, len(tiles), step, 0)


def project_kv_kernel(*refs):
    place_ref = refs[0]
    sources = refs[1:17]
    own_kv = refs[17]
    pieces = {1: refs[18:26], 2: refs[26:34], 3: refs[34:42]}
    bias_ref, q_bias_ref, cos_ref, sin_ref = refs[42:46]
    outs, out_ref, compact_ref = refs[46:50], refs[50], refs[51]
    rows_ref, weight_buf, sum_ref, sems, weight_sems, copy_sem = refs[52:]
    copies = weight_tile(None, own_kv, pieces, place_ref, weight_buf, weight_sems)
    copy_out = pltpu.make_async_copy(rows_ref, compact_ref, copy_sem)

    def unit_copy(index):
        slot = index % 4
        source = sources[index // 4]
        if index < 32:
            source = source.at[pl.ds(UNIT * slot, UNIT), :]
        else:
            source = source.at[slot]
        row = pl.multiple_of(UNIT * jnp.maximum(place_ref[index], 0), UNIT)
        return pltpu.make_async_copy(source, rows_ref.at[pl.ds(row, UNIT), :], sems.at[index])

    def assemble():
        total = place_ref[64]
        for unit in range(24, CAPACITY):
            @pl.when(unit >= total)
            def _(unit=unit):
                rows_ref[pl.ds(UNIT * unit, UNIT), :] = jnp.zeros(
                    (UNIT, rows_ref.shape[1]), jnp.bfloat16
                )

        used = [index for index in range(64) if index < 32 or index % 8 < 7]
        for index in used:
            @pl.when(place_ref[index] >= 0)
            def _(index=index):
                unit_copy(index).start()
        for index in used:
            @pl.when(place_ref[index] >= 0)
            def _(index=index):
                unit_copy(index).wait()
        copy_out.start()

    def finish(index, product):
        if index >= 2:
            store_heads(out_ref, index - 2, product, q_bias_ref, cos_ref, sin_ref)
        if index != 1:
            return
        odd = place_ref[65] == 1
        halves = [
            sum_ref[delta // 2, :, pl.ds(delta % 2 * HD, HD)] + bias_ref[:, pl.ds(delta * HD, HD)]
            for delta in range(4)
        ]
        in_low = lax.broadcasted_iota(jnp.int32, halves[0].shape, 1) < HD // 2
        ends = (
            (jnp.where(odd, halves[3], halves[0]), jnp.where(odd, halves[0], halves[1])),
            (jnp.where(odd, halves[1], halves[2]), jnp.where(odd, halves[2], halves[3])),
        )
        near, away = [], []
        for group, (low, high) in zip((near, away), ends):
            key = jnp.where(in_low, low, pltpu.roll(high, HD // 2, 1))
            value = jnp.where(in_low, pltpu.roll(low, HD // 2, 1), high)
            group += [rotated(key, cos_ref[...], sin_ref[...]), value]
        for part in range(2):
            lanes = slice(part * HD, (part + 1) * HD)
            outs[0][:, lanes] = near[part].astype(jnp.bfloat16)
            outs[1][:, lanes] = jnp.where(odd, away[part], near[part]).astype(jnp.bfloat16)
            outs[2][:, lanes] = away[part].astype(jnp.bfloat16)
            outs[3][:, lanes] = jnp.where(odd, near[part], away[part]).astype(jnp.bfloat16)

    tiles = [
        [(0, 512, HD), (1, 512, HD)], [(2, 512, HD), (3, 512, HD)],
        [(2, 0, COLUMNS)], [(2, COLUMNS, COLUMNS)],
    ]
    run_tiles(tiles, copies, rows_ref, weight_buf, sum_ref, finish, assemble)
    copy_out.wait()


def store_heads(out_ref, part, product, bias_ref, cos_ref, sin_ref):
    for head in range(COLUMNS // HD):
        lanes = slice(part * COLUMNS + head * HD, part * COLUMNS + (head + 1) * HD)
        values = product[:, head * HD:(head + 1) * HD] + bias_ref[:, lanes]
        out_ref[:, lanes] = rotated(values, cos_ref[...], sin_ref[...]).astype(jnp.bfloat16)


def cost(width, features):
    return pl.CostEstimate(
        flops=2 * ROWS * features * width,
        transcendentals=0,
        bytes_accessed=2 * features * (width + ROWS),
    )


def far(values):
    return [pltpu.with_memory_space_constraint(value, pltpu.HBM) for value in values]


def whole(shape):
    return pl.BlockSpec(shape, lambda i, place: (0,) * len(shape))


def project_kv(place, texts, images, own_kv, pieces, bias, q_bias, cosine, sine):
    query_shape = (ROWS, q_bias.shape[1])
    features = texts[0].shape[1]
    far_spec = pl.BlockSpec(memory_space=pltpu.HBM)
    flat = [piece for delta in (1, 2, 3) for piece in pieces[delta]]
    shape = (ROWS, 2 * HD)
    return pl.pallas_call(
        project_kv_kernel,
        grid_spec=pltpu.PrefetchScalarGridSpec(
            num_scalar_prefetch=1,
            grid=(1,),
            in_specs=[far_spec] * (17 + len(flat))
            + [whole(bias.shape), whole(q_bias.shape), whole((ROWS, HD)), whole((ROWS, HD))],
            out_specs=(whole(shape),) * 4 + (whole(query_shape), far_spec),
            scratch_shapes=[
                pltpu.VMEM((ROWS, features), jnp.bfloat16),
                pltpu.VMEM((2, features, COLUMNS), jnp.bfloat16),
                pltpu.VMEM((2, ROWS, COLUMNS), jnp.float32),
                pltpu.SemaphoreType.DMA((64,)),
                pltpu.SemaphoreType.DMA((2, 16)),
                pltpu.SemaphoreType.DMA,
            ],
        ),
        out_shape=(jax.ShapeDtypeStruct(shape, jnp.bfloat16),) * 4
        + (
            jax.ShapeDtypeStruct(query_shape, jnp.bfloat16),
            pltpu.HBM((ROWS, features), jnp.bfloat16),
        ),
        compiler_params=pltpu.CompilerParams(vmem_limit_bytes=40 << 20),
        cost_estimate=cost(4 * COLUMNS, features),
        name="project_kv",
    )(place, *far([*texts, *images, own_kv, *flat]), bias, q_bias, cosine, sine)


def project_q(place, compact, own_q, pieces, biases, cosine, sine):
    deltas = list(biases)
    width = biases[deltas[0]].shape[1]
    features = compact.shape[1]
    far_spec = pl.BlockSpec(memory_space=pltpu.HBM)
    weights = [own_q] if deltas == [0] else [p for delta in deltas for p in pieces[delta]]
    shape = (ROWS, width)

    def kernel(*refs):
        place_ref, compact_ref = refs[:2]
        weight_refs, refs = refs[2:2 + len(weights)], refs[2 + len(weights):]
        bias_refs, refs = refs[:len(deltas)], refs[len(deltas):]
        cos_ref, sin_ref = refs[:2]
        outs, refs = refs[2:2 + len(deltas)], refs[2 + len(deltas):]
        rows_ref, weight_buf, sum_ref, row_sem, weight_sems = refs
        found = {delta: weight_refs[8 * i:8 * i + 8] for i, delta in enumerate(deltas)}
        copies = weight_tile(weight_refs[0], None, found, place_ref, weight_buf, weight_sems)
        share = ROWS // 6
        copies_in = [
            pltpu.make_async_copy(
                compact_ref.at[pl.ds(part * share, share), :],
                rows_ref.at[pl.ds(part * share, share), :],
                row_sem.at[part],
            )
            for part in range(6)
        ]
        for copy in copies_in:
            copy.start()

        def rows_here():
            for copy in copies_in:
                copy.wait()

        def finish(index, product):
            store_heads(
                outs[index // 2], index % 2, product, bias_refs[index // 2], cos_ref, sin_ref
            )

        tiles = [[(delta, first, COLUMNS)] for delta in deltas for first in (0, COLUMNS)]
        run_tiles(tiles, copies, rows_ref, weight_buf, sum_ref, finish, rows_here)

    return pl.pallas_call(
        kernel,
        grid_spec=pltpu.PrefetchScalarGridSpec(
            num_scalar_prefetch=1,
            grid=(1,),
            in_specs=[far_spec] * (1 + len(weights))
            + [whole((1, width))] * len(deltas)
            + [whole((ROWS, HD)), whole((ROWS, HD))],
            out_specs=(whole(shape),) * len(deltas),
            scratch_shapes=[
                pltpu.VMEM((ROWS, features), jnp.bfloat16),
                pltpu.VMEM((2, features, COLUMNS), jnp.bfloat16),
                pltpu.VMEM((2, ROWS, COLUMNS), jnp.float32),
                pltpu.SemaphoreType.DMA((6,)),
                pltpu.SemaphoreType.DMA((2, 16)),
            ],
        ),
        out_shape=(jax.ShapeDtypeStruct(shape, jnp.bfloat16),) * len(deltas),
        compiler_params=pltpu.CompilerParams(vmem_limit_bytes=40 << 20),
        cost_estimate=cost(width * len(deltas), features),
        name="project_q",
    )(place, *far([compact, *weights]), *biases.values(), cosine, sine)


def attend_kernel(
    info_ref, text_ref, q0, q1, q2, q3, kv0, kv1, kv2, kv3, out_ref, merged_ref, run_ref, mask_ref
):
    parts = ((q0, kv0), (q1, kv1), (q2, kv2), (q3, kv3))
    q_width = q0.shape[1]
    step = pl.program_id(0)
    block = out_ref.shape[0]
    width = merged_ref.shape[1]
    mine = info_ref[11]
    run_start = info_ref[8]
    run_end = info_ref[9]
    used = info_ref[10]
    first_unit = (run_start + UNIT - 1) // UNIT
    lag = first_unit * UNIT - run_start

    @pl.when(step == 0)
    def _():
        merged_ref[0:WINDOW, :] = jnp.zeros((WINDOW, width), jnp.bfloat16)
        run_ref[0:128, :] = jnp.zeros((128, width), jnp.bfloat16)
        run_ref[128 + 7 * TR:, :] = jnp.zeros((run_ref.shape[0] - 128 - 7 * TR, width), jnp.bfloat16)

        def tile_step(tile, carry):
            for piece in range(16):
                level, delta = piece // 4, piece % 4
                member = (mine + delta) % 4
                source = pl.multiple_of(tile * 64 + level * UNIT, UNIT)
                target = pl.multiple_of(128 + tile * TR + (4 * level + member) * UNIT, UNIT)
                query, pair = parts[delta]
                run_ref[pl.ds(target, UNIT), :q_width] = query[pl.ds(source, UNIT), :]
                run_ref[pl.ds(target, UNIT), q_width:] = pair[pl.ds(source, UNIT), :]
            return carry

        lax.fori_loop(0, (run_end - run_start) // TR, tile_step, 0)

        def clear_step(tile, carry):
            target = pl.multiple_of(128 + tile * TR, TR // 2)
            run_ref[pl.ds(target, TR), :] = jnp.zeros((TR, width), jnp.bfloat16)
            return carry

        lax.fori_loop((run_end - run_start) // TR, 7, clear_step, 0)

        def block_step(row, carry):
            for delta in range(4):
                number = row * 4 + (mine + delta) % 4
                begin = number * 128
                for unit in range(8):
                    source = pl.multiple_of(text_ref[number * 8 + unit] * UNIT, UNIT)
                    target = pl.multiple_of(WINDOW + begin + unit * UNIT, UNIT)
                    query, pair = parts[delta]
                    merged_ref[pl.ds(target, UNIT), :q_width] = query[pl.ds(source, UNIT), :]
                    merged_ref[pl.ds(target, UNIT), q_width:] = pair[pl.ds(source, UNIT), :]

                @pl.when((begin < run_end) & (begin + 128 > run_start))
                def _():
                    origin = pl.multiple_of(128 + UNIT * (8 * number - first_unit), UNIT)
                    window = run_ref[pl.ds(origin, 256), :]
                    place = lax.broadcasted_iota(jnp.int32, (128, 256), 0)
                    taken = lax.broadcasted_iota(jnp.int32, (128, 256), 1)
                    pick = jnp.where(taken == place + lag, 1.0, 0.0).astype(jnp.bfloat16)
                    moved = jnp.dot(pick, window, preferred_element_type=jnp.float32)
                    here = pl.ds(pl.multiple_of(WINDOW + begin, 128), 128)
                    old = merged_ref[here, :].astype(jnp.float32)
                    position = begin + lax.broadcasted_iota(jnp.int32, old.shape, 0)
                    covered = (position >= run_start) & (position < run_end)
                    merged_ref[here, :] = jnp.where(covered, moved, old).astype(jnp.bfloat16)
            return carry

        lax.fori_loop(0, 4, block_step, 0)

    base = pl.multiple_of(step * block, block)
    first_doc = jnp.int32(0)
    for doc in range(1, 8):
        first_doc = jnp.where(base >= info_ref[doc], info_ref[doc], first_doc)
    reach = (base - first_doc + 127) // 128

    def attend_span(span):
        position = base + lax.broadcasted_iota(jnp.int32, (block, 1), 0)
        doc_start = jnp.zeros((block, 1), jnp.int32)
        for doc in range(1, 8):
            doc_start = jnp.where(position >= info_ref[doc], info_ref[doc], doc_start)
        other = base + block - span + lax.broadcasted_iota(jnp.int32, (block, span), 1)
        allowed = (other >= doc_start) & (other <= position) & (other < used)
        mask_ref[:, :span] = jnp.where(allowed, 0.0, NEGATIVE)
        queries = pl.ds(pl.multiple_of(WINDOW + base, block), block)
        window = pl.ds(pl.multiple_of(WINDOW + base + block - span, 128), span)
        keys = merged_ref[window, 4 * HD:5 * HD]
        values = merged_ref[window, 5 * HD:6 * HD]
        factor = HD ** (-0.5) * math.log2(math.e)
        heads = [merged_ref[queries, head * HD:(head + 1) * HD] for head in range(4)]
        scores = lax.dot_general(
            jnp.concatenate(heads, axis=0), keys, (((1,), (1,)), ((), ())),
            preferred_element_type=jnp.float32,
        )
        scores = scores.reshape(4, block, span) + mask_ref[:, :span][None]
        peak = jnp.max(scores, axis=-1, keepdims=True)
        exponent = jnp.exp2((scores - peak) * factor)
        inverse = 1.0 / jnp.sum(exponent, axis=-1, keepdims=True)
        probs = (exponent * inverse).astype(jnp.bfloat16).reshape(4 * block, span)
        mixed = jnp.dot(probs, values, preferred_element_type=jnp.float32)
        for head in range(4):
            rows = mixed[head * block:(head + 1) * block]
            out_ref[:, head * HD:(head + 1) * HD] = jnp.where(position < used, rows, 0.0).astype(
                jnp.bfloat16
            )

    for extra in (1, 2, 3, 4):
        within = reach <= 1 if extra == 1 else reach == extra

        @pl.when(within & (base < used))
        def _(extra=extra):
            attend_span(block + 128 * extra)

    @pl.when(base >= used)
    def _():
        out_ref[...] = jnp.zeros(out_ref.shape, jnp.bfloat16)


def attend(info, text_index, parts):
    block = 128
    width = parts[0].shape[1] + parts[4].shape[1]
    return pl.pallas_call(
        attend_kernel,
        grid_spec=pltpu.PrefetchScalarGridSpec(
            num_scalar_prefetch=2,
            grid=(LENGTH // block,),
            in_specs=[pl.BlockSpec(part.shape, lambda i, a, b: (0, 0)) for part in parts],
            out_specs=pl.BlockSpec((block, 4 * HD), lambda i, a, b: (i, 0)),
            scratch_shapes=[
                pltpu.VMEM((WINDOW + LENGTH, width), jnp.bfloat16),
                pltpu.VMEM((128 + 7 * TR + 384, width), jnp.bfloat16),
                pltpu.VMEM((block, block + WINDOW), jnp.float32),
            ],
        ),
        out_shape=jax.ShapeDtypeStruct((LENGTH, 4 * HD), jnp.bfloat16),
        compiler_params=pltpu.CompilerParams(vmem_limit_bytes=48 << 20),
        name="attend",
    )(info, text_index, *parts)


def tables(tile_group, tile_offset, seq_len, doc_ids, group, z, y, quarters):
    mine = tile_group == group
    present = jnp.any(mine.reshape(8, 4), axis=1)
    count = jnp.sum(mine.astype(jnp.int32))
    run_start = jnp.where(count > 0, jnp.min(jnp.where(mine, tile_offset, LENGTH)), 0)
    run_end = run_start + TR * count
    low_unit = (run_start + UNIT - 1) // UNIT
    high_unit = run_end // UNIT
    eight = jnp.arange(8, dtype=jnp.int32)
    rank = jnp.sum((present[None, :] & (eight[None, :] < eight[:, None])).astype(jnp.int32), axis=1)
    order = jnp.arange(32, dtype=jnp.int32)
    four = jnp.arange(4, dtype=jnp.int32)
    unit_of = 8 * (4 * (order[None, :] // 8) + four[:, None]) + order[None, :] % 8
    before = jnp.sum((unit_of < low_unit).astype(jnp.int32), axis=1)
    hidden = jnp.sum((unit_of < high_unit).astype(jnp.int32), axis=1) - before
    held = (unit_of < low_unit) | (unit_of >= high_unit)
    compact = 4 * count + order[None, :] - jnp.where(unit_of >= high_unit, hidden[:, None], 0)
    compact = jnp.where(held, compact, -1)
    text_index = jnp.maximum(compact, 0).reshape(4, 4, 8).transpose(1, 0, 2).reshape(-1)
    my_before = lax.dynamic_index_in_dim(before, y, 0, keepdims=False)
    my_hidden = lax.dynamic_index_in_dim(hidden, y, 0, keepdims=False)
    member = (z + four) % 4
    my_compact = lax.dynamic_index_in_dim(compact, y, 0, keepdims=False).reshape(4, 8)
    text_place = jnp.take(my_compact, member, axis=0).reshape(-1)
    image_place = jnp.where(eight[None, :] < count, 4 * eight[None, :] + member[:, None], -1)
    image_place = image_place.reshape(-1)
    total = 4 * count + 32 - my_hidden
    place = jnp.concatenate([text_place, image_place, total[None], y[None] % 2, quarters])
    place = place.astype(jnp.int32)
    is_slot = present[None, :] & (rank[None, :] == eight[:7, None])
    slots = jnp.sum(jnp.where(is_slot, eight[None, :], 0), axis=1).astype(jnp.int32)
    number = jnp.arange(ROWS, dtype=jnp.int32) // UNIT
    inner = jnp.arange(ROWS, dtype=jnp.int32) % UNIT
    image_at = run_start + TR * (number // 4) + UNIT * (4 * (number % 4) + y)
    text_number = number - 4 * count
    text_number = jnp.clip(text_number + jnp.where(text_number >= my_before, my_hidden, 0), 0, 31)
    text_at = 128 * (4 * (text_number // 8) + y) + UNIT * (text_number % 8)
    position = jnp.where(number < 4 * count, image_at, text_at) + inner
    starts = jnp.sum((doc_ids[0][None, :] < eight[:, None]).astype(jnp.int32), axis=1)
    doc_start = jnp.max(
        jnp.where(starts[None, :] <= position[:, None], starts[None, :], 0), axis=1
    )
    in_doc = position - doc_start
    info = jnp.concatenate([starts, run_start[None], run_end[None], seq_len, y[None]])
    return place, slots, text_index, info.astype(jnp.int32), in_doc


def one_device(
    text_rows, image_rows, tile_group, tile_offset, seq_len, doc_ids, norm_gain,
    q_weight, k_weight, v_weight, q_bias, k_bias, v_bias,
):
    x = lax.axis_index("x")
    core = lax.axis_index("c")
    group = x * 2 + core
    z = lax.axis_index("z")
    y = lax.axis_index("y")
    gain = norm_gain.reshape(1, -1)

    t_low = norm_text(text_rows, gain, 0, 64)
    t3_low = shifted(t_low, "z", 1)
    t1_low = shifted(t_low, "z", -1)

    quarter = 2 * core + x % 2
    begin, t_low = lax.optimization_barrier((quarter * 2 * PIECE, t_low))
    own_kv = jnp.concatenate([k_weight, v_weight], axis=1)

    def own_part(half):
        first = begin + half * PIECE
        return jnp.concatenate(
            [
                lax.dynamic_slice_in_dim(weight, first, PIECE, 0)
                for weight in (q_weight, own_kv)
            ],
            axis=1,
        )

    low, high = own_part(0), own_part(1)
    direct = {}
    direct[1, 0] = shifted(low, "y", -1)
    direct[3, 1] = shifted(high, "y", 1)
    direct[1, 1] = shifted(high, "y", -1)
    direct[3, 0] = shifted(low, "y", 1)

    low, high, text_rows = lax.optimization_barrier((low, high, text_rows))
    t_high = norm_text(text_rows, gain, 64, 64)
    t3_high = shifted(t_high, "z", 1)
    t1_high = shifted(t_high, "z", -1)

    row_groups = lax.dynamic_slice_in_dim(tile_group, group * 4, 4)
    matches = row_groups[None, :] == jnp.arange(8, dtype=jnp.int32)[:, None]
    chosen = jnp.sum(jnp.where(matches, jnp.arange(4, dtype=jnp.int32)[None, :], 0), axis=1)
    image_rows, t_high = lax.optimization_barrier((image_rows, t_high))
    outgoing = spread(image_rows, chosen.astype(jnp.int32))
    arrived = lax.all_to_all(outgoing, ("x", "c"), split_axis=0, concat_axis=0, tiled=True)

    t2_low = shifted(t3_low, "z", 1)
    t2_high = shifted(t1_high, "z", -1)

    direct[2, 0] = shifted(direct[1, 0], "y", -1)
    direct[2, 1] = shifted(direct[3, 1], "y", 1)
    across = {
        key: shifted(value, "x", -1 if key[1] else 1)
        for key, value in direct.items()
        if key[0] != 2
    }
    across[2, 0] = shifted(across[1, 0], "y", -1)
    across[2, 1] = shifted(across[3, 1], "y", 1)
    pieces = {
        delta: [direct[delta, 0], direct[delta, 1], across[delta, 0], across[delta, 1]]
        for delta in (1, 2, 3)
    }
    pieces = {
        delta: found
        + [shifted(value, "c", 1) for value in found]
        for delta, found in pieces.items()
    }
    quarters = jnp.stack([quarter ^ 0, quarter ^ 1, quarter ^ 2, quarter ^ 3]) * 2 * PIECE

    doc_ids, direct[2, 0] = lax.optimization_barrier((doc_ids, direct[2, 0]))
    place, slots, text_index, info, in_doc = tables(
        tile_group, tile_offset, seq_len, doc_ids, group, z, y, quarters
    )
    i_low = norm_image(arrived, gain, slots[:4])
    i_high = norm_image(arrived, gain, slots[4:])
    i3_low = shifted(i_low, "z", 1)
    i1_low = shifted(i_low, "z", -1)
    i3_high = shifted(i_high, "z", 1)
    i1_high = shifted(i_high, "z", -1)
    i2_low = shifted(i3_low, "z", 1)
    i2_high = shifted(i1_high, "z", -1)

    bias = jnp.concatenate([q_bias, k_bias, v_bias])
    bias, t_high = lax.optimization_barrier((bias, t_high))
    biases = [
        bias, shifted(bias, "y", -1), shifted(bias, "y", 2),
        shifted(bias, "y", 1),
    ]
    q_biases = [value[None, :4 * HD] for value in biases]
    kv_bias = jnp.concatenate([value[None, 4 * HD:] for value in biases], axis=1)
    frequency = THETA ** (-(jnp.arange(HD // 2, dtype=jnp.float32) * 2.0) / HD)
    angles = in_doc.astype(jnp.float32)[:, None] * frequency[None, :]
    cosine = jnp.concatenate([jnp.cos(angles), jnp.cos(angles)], axis=-1)
    sine = jnp.concatenate([-jnp.sin(angles), jnp.sin(angles)], axis=-1)

    place, text_index, info = lax.optimization_barrier((place, text_index, info))
    texts = (t_low, t_high, t1_low, t1_high, t2_low, t2_high, t3_low, t3_high)
    images = (i_low, i_high, i1_low, i1_high, i2_low, i2_high, i3_low, i3_high)
    *pairs, far_query, compact = project_kv(
        place, texts, images, own_kv, pieces, kv_bias, q_biases[2], cosine, sine
    )
    queries = {2: far_query}
    after = compact
    for deltas in ((1, 3), (0,)):
        found = project_q(
            place, after, q_weight, pieces,
            {delta: q_biases[delta] for delta in deltas}, cosine, sine,
        )
        after, *found = lax.optimization_barrier((after, *found))
        queries.update(zip(deltas, found))
    parts = []
    for values in (queries, pairs):
        parts.append(values[0])
        parts += [shifted(values[4 - delta], "y", -delta) for delta in (1, 2, 3)]
    return attend(info, text_index, parts)


def solution(mesh):
    fine = Mesh(mesh.devices.reshape(4, 2, 4, 4), ("x", "c", "z", "y"))
    dp, seq = ("x", "c"), ("z", "y")
    return jax.shard_map(
        one_device,
        mesh=fine,
        in_specs=(
            P(dp + seq, None),
            P(dp, seq, None),
            P(),
            P(),
            P(dp),
            P(dp, None),
            P(),
            P(None, seq),
            P(None, seq),
            P(None, seq),
            P(seq),
            P(seq),
            P(seq),
        ),
        out_specs=P(dp, seq),
        check_vma=False,
    )
```

```python
import math

import jax
import jax.numpy as jnp
from jax import lax
from jax.experimental import pallas as pl
from jax.experimental.pallas import tpu as pltpu
from jax.sharding import Mesh, PartitionSpec as P

TR = 256
UNIT = 16
HD = 128
LENGTH = 2048
CAPACITY = 36
ROWS = CAPACITY * UNIT
WINDOW = 512
THETA = 1000000.0
NEGATIVE = -1e30
EPSILON = 1e-06


def shifted(block, axis, step):
    count = lax.axis_size(axis)
    return lax.ppermute(block, axis, [(low, (low + step) % count) for low in range(count)])


def rms_norm(row_block, gain):
    float_rows = row_block.astype(jnp.float32)
    inv_rms = lax.rsqrt(jnp.mean(float_rows * float_rows, axis=-1, keepdims=True) + EPSILON)
    return (float_rows * inv_rms * gain).astype(jnp.bfloat16)


def norm_text_kernel(rows_ref, gain_ref, out_ref):
    out_ref[...] = rms_norm(rows_ref[...], gain_ref[...])


def norm_text(rows, gain, first, count):
    features = rows.shape[1]
    step = 2 * UNIT
    return pl.pallas_call(
        norm_text_kernel,
        grid=(count // step,),
        in_specs=[
            pl.BlockSpec((step, features), lambda i: (first // step + i, 0)),
            pl.BlockSpec((1, features), lambda i: (0, 0)),
        ],
        out_specs=pl.BlockSpec((step, features), lambda i: (i, 0)),
        out_shape=jax.ShapeDtypeStruct((count, features), jnp.bfloat16),
    )(rows, gain)


def norm_image_kernel(chosen_ref, rows_ref, gain_ref, out_ref):
    out_ref[0] = rms_norm(rows_ref[0], gain_ref[...])


def norm_image(pieces, gain, chosen):
    _, piece_rows, features = pieces.shape
    groups = chosen.shape[0]
    return pl.pallas_call(
        norm_image_kernel,
        grid_spec=pltpu.PrefetchScalarGridSpec(
            num_scalar_prefetch=1,
            grid=(groups,),
            in_specs=[
                pl.BlockSpec((1, piece_rows, features), lambda i, chosen: (chosen[i], 0, 0)),
                pl.BlockSpec((1, features), lambda i, chosen: (0, 0)),
            ],
            out_specs=pl.BlockSpec((1, piece_rows, features), lambda i, chosen: (i, 0, 0)),
        ),
        out_shape=jax.ShapeDtypeStruct((groups, piece_rows, features), jnp.bfloat16),
        name="norm_image",
    )(chosen, pieces, gain)


def spread_kernel(chosen_ref, pieces_ref, out_ref, held_ref, in_sem, sems):
    copy_in = pltpu.make_async_copy(pieces_ref, held_ref, in_sem)
    copy_in.start()
    copy_in.wait()

    def copy(index):
        return pltpu.make_async_copy(
            held_ref.at[chosen_ref[index]], out_ref.at[index], sems.at[index]
        )

    for index in range(out_ref.shape[0]):
        copy(index).start()
    for index in range(out_ref.shape[0]):
        copy(index).wait()


def spread(pieces, chosen):
    count = chosen.shape[0]
    far_spec = pl.BlockSpec(memory_space=pltpu.HBM)
    return pl.pallas_call(
        spread_kernel,
        grid_spec=pltpu.PrefetchScalarGridSpec(
            num_scalar_prefetch=1,
            grid=(1,),
            in_specs=[far_spec],
            out_specs=far_spec,
            scratch_shapes=[
                pltpu.VMEM(pieces.shape, jnp.bfloat16),
                pltpu.SemaphoreType.DMA,
                pltpu.SemaphoreType.DMA((count,)),
            ],
        ),
        out_shape=pltpu.HBM((count,) + pieces.shape[1:], jnp.bfloat16),
        name="spread",
    )(chosen, *far([pieces]))


def rotated(values, cosine, sine):
    return values * cosine + pltpu.roll(values, HD // 2, 1) * sine


COLUMNS = 256
PIECE = 1024


def weight_tile(own_q, own_kv, pieces, place_ref, weight_buf, sems):
    def copies(tile, slot):
        found = []
        lane = 0
        for delta, first, count in tile:
            lanes = pl.ds(lane, count)
            lane += count
            if delta == 0 and first == 512:
                found.append((own_kv, weight_buf.at[slot, :, lanes]))
            elif delta == 0:
                for index in range(8):
                    rows = pl.ds(index * PIECE, PIECE)
                    source = own_q.at[rows, pl.ds(first, count)]
                    found.append((source, weight_buf.at[slot, rows, lanes]))
            else:
                for index, piece in enumerate(pieces[delta]):
                    row = pl.multiple_of(place_ref[66 + index // 2] + index % 2 * PIECE, PIECE)
                    found.append(
                        (
                            piece.at[:, pl.ds(first, count)],
                            weight_buf.at[slot, pl.ds(row, PIECE), lanes],
                        )
                    )
        return [
            pltpu.make_async_copy(source, target, sems.at[slot, index])
            for index, (source, target) in enumerate(found)
        ]

    return copies


def run_tiles(tiles, copies, rows_ref, weight_buf, sum_ref, finish, before):
    slots = weight_buf.shape[0]
    for copy in copies(tiles[0], 0):
        copy.start()
    before()
    for index in range(1, min(slots, len(tiles))):
        for copy in copies(tiles[index], index):
            copy.start()

    def step(number, carry):
        slot = number % slots
        for index, tile in enumerate(tiles):
            @pl.when(number == index)
            def _(index=index, tile=tile):
                for copy in copies(tile, index % slots):
                    copy.wait()

        sum_ref[slot] = jnp.dot(
            rows_ref[...], weight_buf[slot], preferred_element_type=jnp.float32
        )
        for index in range(len(tiles)):
            @pl.when(number == index)
            def _(index=index):
                if index + slots < len(tiles):
                    for copy in copies(tiles[index + slots], index % slots):
                        copy.start()
                finish(index, sum_ref.at[index % slots])

        return carry

    lax.fori_loop(0, len(tiles), step, 0)


def project_kv_kernel(*refs):
    place_ref = refs[0]
    sources = refs[1:17]
    own_kv = refs[17]
    pieces = {1: refs[18:26], 2: refs[26:34], 3: refs[34:42]}
    bias_ref, q_bias_ref, cos_ref, sin_ref = refs[42:46]
    outs, out_ref, compact_ref = refs[46:50], refs[50], refs[51]
    rows_ref, weight_buf, sum_ref, sems, weight_sems, copy_sem = refs[52:]
    copies = weight_tile(None, own_kv, pieces, place_ref, weight_buf, weight_sems)
    copy_out = pltpu.make_async_copy(rows_ref, compact_ref, copy_sem)

    def unit_copy(index):
        slot = index % 4
        source = sources[index // 4]
        if index < 32:
            source = source.at[pl.ds(UNIT * slot, UNIT), :]
        else:
            source = source.at[slot]
        row = pl.multiple_of(UNIT * jnp.maximum(place_ref[index], 0), UNIT)
        return pltpu.make_async_copy(source, rows_ref.at[pl.ds(row, UNIT), :], sems.at[index])

    def assemble():
        total = place_ref[64]
        for unit in range(24, CAPACITY):
            @pl.when(unit >= total)
            def _(unit=unit):
                rows_ref[pl.ds(UNIT * unit, UNIT), :] = jnp.zeros(
                    (UNIT, rows_ref.shape[1]), jnp.bfloat16
                )

        used = [index for index in range(64) if index < 32 or index % 8 < 7]
        for index in used:
            @pl.when(place_ref[index] >= 0)
            def _(index=index):
                unit_copy(index).start()
        for index in used:
            @pl.when(place_ref[index] >= 0)
            def _(index=index):
                unit_copy(index).wait()
        copy_out.start()

    def finish(index, product):
        if index >= 2:
            store_heads(out_ref, index - 2, product, q_bias_ref, cos_ref, sin_ref)
        if index != 1:
            return
        odd = place_ref[65] == 1
        halves = [
            sum_ref[delta // 2, :, pl.ds(delta % 2 * HD, HD)] + bias_ref[:, pl.ds(delta * HD, HD)]
            for delta in range(4)
        ]
        in_low = lax.broadcasted_iota(jnp.int32, halves[0].shape, 1) < HD // 2
        ends = (
            (jnp.where(odd, halves[3], halves[0]), jnp.where(odd, halves[0], halves[1])),
            (jnp.where(odd, halves[1], halves[2]), jnp.where(odd, halves[2], halves[3])),
        )
        near, away = [], []
        for group, (low, high) in zip((near, away), ends):
            key = jnp.where(in_low, low, pltpu.roll(high, HD // 2, 1))
            value = jnp.where(in_low, pltpu.roll(low, HD // 2, 1), high)
            group += [rotated(key, cos_ref[...], sin_ref[...]), value]
        for part in range(2):
            lanes = slice(part * HD, (part + 1) * HD)
            outs[0][:, lanes] = near[part].astype(jnp.bfloat16)
            outs[1][:, lanes] = jnp.where(odd, away[part], near[part]).astype(jnp.bfloat16)
            outs[2][:, lanes] = away[part].astype(jnp.bfloat16)
            outs[3][:, lanes] = jnp.where(odd, near[part], away[part]).astype(jnp.bfloat16)

    tiles = [
        [(0, 512, HD), (1, 512, HD)], [(2, 512, HD), (3, 512, HD)],
        [(2, 0, COLUMNS)], [(2, COLUMNS, COLUMNS)],
    ]
    run_tiles(tiles, copies, rows_ref, weight_buf, sum_ref, finish, assemble)
    copy_out.wait()


def store_heads(out_ref, part, product, bias_ref, cos_ref, sin_ref):
    for head in range(COLUMNS // HD):
        lanes = slice(part * COLUMNS + head * HD, part * COLUMNS + (head + 1) * HD)
        values = product[:, head * HD:(head + 1) * HD] + bias_ref[:, lanes]
        out_ref[:, lanes] = rotated(values, cos_ref[...], sin_ref[...]).astype(jnp.bfloat16)


def cost(width, features):
    return pl.CostEstimate(
        flops=2 * ROWS * features * width,
        transcendentals=0,
        bytes_accessed=2 * features * (width + ROWS),
    )


def far(values):
    return [pltpu.with_memory_space_constraint(value, pltpu.HBM) for value in values]


def whole(shape):
    return pl.BlockSpec(shape, lambda i, place: (0,) * len(shape))


def project_kv(place, texts, images, own_kv, pieces, bias, q_bias, cosine, sine):
    query_shape = (ROWS, q_bias.shape[1])
    features = texts[0].shape[1]
    far_spec = pl.BlockSpec(memory_space=pltpu.HBM)
    flat = [piece for delta in (1, 2, 3) for piece in pieces[delta]]
    shape = (ROWS, 2 * HD)
    return pl.pallas_call(
        project_kv_kernel,
        grid_spec=pltpu.PrefetchScalarGridSpec(
            num_scalar_prefetch=1,
            grid=(1,),
            in_specs=[far_spec] * (17 + len(flat))
            + [whole(bias.shape), whole(q_bias.shape), whole((ROWS, HD)), whole((ROWS, HD))],
            out_specs=(whole(shape),) * 4 + (whole(query_shape), far_spec),
            scratch_shapes=[
                pltpu.VMEM((ROWS, features), jnp.bfloat16),
                pltpu.VMEM((2, features, COLUMNS), jnp.bfloat16),
                pltpu.VMEM((2, ROWS, COLUMNS), jnp.float32),
                pltpu.SemaphoreType.DMA((64,)),
                pltpu.SemaphoreType.DMA((2, 16)),
                pltpu.SemaphoreType.DMA,
            ],
        ),
        out_shape=(jax.ShapeDtypeStruct(shape, jnp.bfloat16),) * 4
        + (
            jax.ShapeDtypeStruct(query_shape, jnp.bfloat16),
            pltpu.HBM((ROWS, features), jnp.bfloat16),
        ),
        compiler_params=pltpu.CompilerParams(vmem_limit_bytes=40 << 20),
        cost_estimate=cost(4 * COLUMNS, features),
        name="project_kv",
    )(place, *far([*texts, *images, own_kv, *flat]), bias, q_bias, cosine, sine)


def project_q(place, compact, own_q, pieces, biases, cosine, sine):
    deltas = list(biases)
    width = biases[deltas[0]].shape[1]
    features = compact.shape[1]
    far_spec = pl.BlockSpec(memory_space=pltpu.HBM)
    weights = [own_q] if deltas == [0] else [p for delta in deltas for p in pieces[delta]]
    shape = (ROWS, width)

    def kernel(*refs):
        place_ref, compact_ref = refs[:2]
        weight_refs, refs = refs[2:2 + len(weights)], refs[2 + len(weights):]
        bias_refs, refs = refs[:len(deltas)], refs[len(deltas):]
        cos_ref, sin_ref = refs[:2]
        outs, refs = refs[2:2 + len(deltas)], refs[2 + len(deltas):]
        rows_ref, weight_buf, sum_ref, row_sem, weight_sems = refs
        found = {delta: weight_refs[8 * i:8 * i + 8] for i, delta in enumerate(deltas)}
        copies = weight_tile(weight_refs[0], None, found, place_ref, weight_buf, weight_sems)
        share = ROWS // 6
        copies_in = [
            pltpu.make_async_copy(
                compact_ref.at[pl.ds(part * share, share), :],
                rows_ref.at[pl.ds(part * share, share), :],
                row_sem.at[part],
            )
            for part in range(6)
        ]
        for copy in copies_in:
            copy.start()

        def rows_here():
            for copy in copies_in:
                copy.wait()

        def finish(index, product):
            store_heads(
                outs[index // 2], index % 2, product, bias_refs[index // 2], cos_ref, sin_ref
            )

        tiles = [[(delta, first, COLUMNS)] for delta in deltas for first in (0, COLUMNS)]
        run_tiles(tiles, copies, rows_ref, weight_buf, sum_ref, finish, rows_here)

    return pl.pallas_call(
        kernel,
        grid_spec=pltpu.PrefetchScalarGridSpec(
            num_scalar_prefetch=1,
            grid=(1,),
            in_specs=[far_spec] * (1 + len(weights))
            + [whole((1, width))] * len(deltas)
            + [whole((ROWS, HD)), whole((ROWS, HD))],
            out_specs=(whole(shape),) * len(deltas),
            scratch_shapes=[
                pltpu.VMEM((ROWS, features), jnp.bfloat16),
                pltpu.VMEM((2, features, COLUMNS), jnp.bfloat16),
                pltpu.VMEM((2, ROWS, COLUMNS), jnp.float32),
                pltpu.SemaphoreType.DMA((6,)),
                pltpu.SemaphoreType.DMA((2, 16)),
            ],
        ),
        out_shape=(jax.ShapeDtypeStruct(shape, jnp.bfloat16),) * len(deltas),
        compiler_params=pltpu.CompilerParams(vmem_limit_bytes=40 << 20),
        cost_estimate=cost(width * len(deltas), features),
        name="project_q",
    )(place, *far([compact, *weights]), *biases.values(), cosine, sine)


def attend_kernel(
    info_ref, text_ref, q0, q1, q2, q3, kv0, kv1, kv2, kv3, out_ref, merged_ref, run_ref, mask_ref
):
    parts = ((q0, kv0), (q1, kv1), (q2, kv2), (q3, kv3))
    q_width = q0.shape[1]
    step = pl.program_id(0)
    block = out_ref.shape[0]
    width = merged_ref.shape[1]
    mine = info_ref[11]
    run_start = info_ref[8]
    run_end = info_ref[9]
    used = info_ref[10]
    first_unit = (run_start + UNIT - 1) // UNIT
    lag = first_unit * UNIT - run_start

    @pl.when(step == 0)
    def _():
        merged_ref[0:WINDOW, :] = jnp.zeros((WINDOW, width), jnp.bfloat16)
        run_ref[0:128, :] = jnp.zeros((128, width), jnp.bfloat16)
        run_ref[128 + 7 * TR:, :] = jnp.zeros((run_ref.shape[0] - 128 - 7 * TR, width), jnp.bfloat16)

        def tile_step(tile, carry):
            for piece in range(16):
                level, delta = piece // 4, piece % 4
                member = (mine + delta) % 4
                source = pl.multiple_of(tile * 64 + level * UNIT, UNIT)
                target = pl.multiple_of(128 + tile * TR + (4 * level + member) * UNIT, UNIT)
                query, pair = parts[delta]
                run_ref[pl.ds(target, UNIT), :q_width] = query[pl.ds(source, UNIT), :]
                run_ref[pl.ds(target, UNIT), q_width:] = pair[pl.ds(source, UNIT), :]
            return carry

        lax.fori_loop(0, (run_end - run_start) // TR, tile_step, 0)

        def clear_step(tile, carry):
            target = pl.multiple_of(128 + tile * TR, TR // 2)
            run_ref[pl.ds(target, TR), :] = jnp.zeros((TR, width), jnp.bfloat16)
            return carry

        lax.fori_loop((run_end - run_start) // TR, 7, clear_step, 0)

        def block_step(row, carry):
            for delta in range(4):
                number = row * 4 + (mine + delta) % 4
                begin = number * 128

                @pl.when((begin < run_start) | (begin + 128 > run_end))
                def _(delta=delta, number=number, begin=begin):
                    for unit in range(8):
                        source = pl.multiple_of(text_ref[number * 8 + unit] * UNIT, UNIT)
                        target = pl.multiple_of(WINDOW + begin + unit * UNIT, UNIT)
                        query, pair = parts[delta]
                        merged_ref[pl.ds(target, UNIT), :q_width] = query[pl.ds(source, UNIT), :]
                        merged_ref[pl.ds(target, UNIT), q_width:] = pair[pl.ds(source, UNIT), :]

                @pl.when((begin < run_end) & (begin + 128 > run_start))
                def _():
                    origin = pl.multiple_of(128 + UNIT * (8 * number - first_unit), UNIT)
                    window = run_ref[pl.ds(origin, 256), :]
                    place = lax.broadcasted_iota(jnp.int32, (128, 256), 0)
                    taken = lax.broadcasted_iota(jnp.int32, (128, 256), 1)
                    pick = jnp.where(taken == place + lag, 1.0, 0.0).astype(jnp.bfloat16)
                    moved = jnp.dot(pick, window, preferred_element_type=jnp.float32)
                    here = pl.ds(pl.multiple_of(WINDOW + begin, 128), 128)
                    old = merged_ref[here, :].astype(jnp.float32)
                    position = begin + lax.broadcasted_iota(jnp.int32, old.shape, 0)
                    covered = (position >= run_start) & (position < run_end)
                    merged_ref[here, :] = jnp.where(covered, moved, old).astype(jnp.bfloat16)
            return carry

        lax.fori_loop(0, 4, block_step, 0)

    base = pl.multiple_of(step * block, block)
    first_doc = jnp.int32(0)
    for doc in range(1, 8):
        first_doc = jnp.where(base >= info_ref[doc], info_ref[doc], first_doc)
    reach = (base - first_doc + 127) // 128

    def attend_span(span):
        position = base + lax.broadcasted_iota(jnp.int32, (block, 1), 0)
        doc_start = jnp.zeros((block, 1), jnp.int32)
        for doc in range(1, 8):
            doc_start = jnp.where(position >= info_ref[doc], info_ref[doc], doc_start)
        other = base + block - span + lax.broadcasted_iota(jnp.int32, (block, span), 1)
        allowed = (other >= doc_start) & (other <= position) & (other < used)
        mask_ref[:, :span] = jnp.where(allowed, 0.0, NEGATIVE)
        queries = pl.ds(pl.multiple_of(WINDOW + base, block), block)
        window = pl.ds(pl.multiple_of(WINDOW + base + block - span, 128), span)
        keys = merged_ref[window, 4 * HD:5 * HD]
        values = merged_ref[window, 5 * HD:6 * HD]
        factor = HD ** (-0.5) * math.log2(math.e)
        heads = [merged_ref[queries, head * HD:(head + 1) * HD] for head in range(4)]
        scores = lax.dot_general(
            jnp.concatenate(heads, axis=0), keys, (((1,), (1,)), ((), ())),
            preferred_element_type=jnp.float32,
        )
        scores = scores.reshape(4, block, span) + mask_ref[:, :span][None]
        peak = jnp.max(scores, axis=-1, keepdims=True)
        exponent = jnp.exp2((scores - peak) * factor)
        inverse = 1.0 / jnp.sum(exponent, axis=-1, keepdims=True)
        probs = (exponent * inverse).astype(jnp.bfloat16).reshape(4 * block, span)
        mixed = jnp.dot(probs, values, preferred_element_type=jnp.float32)
        for head in range(4):
            rows = mixed[head * block:(head + 1) * block]
            out_ref[:, head * HD:(head + 1) * HD] = jnp.where(position < used, rows, 0.0).astype(
                jnp.bfloat16
            )

    for extra in (1, 2, 3, 4):
        within = reach <= 1 if extra == 1 else reach == extra

        @pl.when(within & (base < used))
        def _(extra=extra):
            attend_span(block + 128 * extra)

    @pl.when(base >= used)
    def _():
        out_ref[...] = jnp.zeros(out_ref.shape, jnp.bfloat16)


def attend(info, text_index, parts):
    block = 128
    width = parts[0].shape[1] + parts[4].shape[1]
    return pl.pallas_call(
        attend_kernel,
        grid_spec=pltpu.PrefetchScalarGridSpec(
            num_scalar_prefetch=2,
            grid=(LENGTH // block,),
            in_specs=[pl.BlockSpec(part.shape, lambda i, a, b: (0, 0)) for part in parts],
            out_specs=pl.BlockSpec((block, 4 * HD), lambda i, a, b: (i, 0)),
            scratch_shapes=[
                pltpu.VMEM((WINDOW + LENGTH, width), jnp.bfloat16),
                pltpu.VMEM((128 + 7 * TR + 384, width), jnp.bfloat16),
                pltpu.VMEM((block, block + WINDOW), jnp.float32),
            ],
        ),
        out_shape=jax.ShapeDtypeStruct((LENGTH, 4 * HD), jnp.bfloat16),
        compiler_params=pltpu.CompilerParams(vmem_limit_bytes=48 << 20),
        name="attend",
    )(info, text_index, *parts)


def tables(tile_group, tile_offset, seq_len, doc_ids, group, z, y, quarters):
    mine = tile_group == group
    present = jnp.any(mine.reshape(8, 4), axis=1)
    count = jnp.sum(mine.astype(jnp.int32))
    run_start = jnp.where(count > 0, jnp.min(jnp.where(mine, tile_offset, LENGTH)), 0)
    run_end = run_start + TR * count
    low_unit = (run_start + UNIT - 1) // UNIT
    high_unit = run_end // UNIT
    eight = jnp.arange(8, dtype=jnp.int32)
    rank = jnp.sum((present[None, :] & (eight[None, :] < eight[:, None])).astype(jnp.int32), axis=1)
    order = jnp.arange(32, dtype=jnp.int32)
    four = jnp.arange(4, dtype=jnp.int32)
    unit_of = 8 * (4 * (order[None, :] // 8) + four[:, None]) + order[None, :] % 8
    before = jnp.sum((unit_of < low_unit).astype(jnp.int32), axis=1)
    hidden = jnp.sum((unit_of < high_unit).astype(jnp.int32), axis=1) - before
    held = (unit_of < low_unit) | (unit_of >= high_unit)
    compact = 4 * count + order[None, :] - jnp.where(unit_of >= high_unit, hidden[:, None], 0)
    compact = jnp.where(held, compact, -1)
    text_index = jnp.maximum(compact, 0).reshape(4, 4, 8).transpose(1, 0, 2).reshape(-1)
    my_before = lax.dynamic_index_in_dim(before, y, 0, keepdims=False)
    my_hidden = lax.dynamic_index_in_dim(hidden, y, 0, keepdims=False)
    member = (z + four) % 4
    my_compact = lax.dynamic_index_in_dim(compact, y, 0, keepdims=False).reshape(4, 8)
    text_place = jnp.take(my_compact, member, axis=0).reshape(-1)
    image_place = jnp.where(eight[None, :] < count, 4 * eight[None, :] + member[:, None], -1)
    image_place = image_place.reshape(-1)
    total = 4 * count + 32 - my_hidden
    place = jnp.concatenate([text_place, image_place, total[None], y[None] % 2, quarters])
    place = place.astype(jnp.int32)
    is_slot = present[None, :] & (rank[None, :] == eight[:7, None])
    slots = jnp.sum(jnp.where(is_slot, eight[None, :], 0), axis=1).astype(jnp.int32)
    number = jnp.arange(ROWS, dtype=jnp.int32) // UNIT
    inner = jnp.arange(ROWS, dtype=jnp.int32) % UNIT
    image_at = run_start + TR * (number // 4) + UNIT * (4 * (number % 4) + y)
    text_number = number - 4 * count
    text_number = jnp.clip(text_number + jnp.where(text_number >= my_before, my_hidden, 0), 0, 31)
    text_at = 128 * (4 * (text_number // 8) + y) + UNIT * (text_number % 8)
    position = jnp.where(number < 4 * count, image_at, text_at) + inner
    starts = jnp.sum((doc_ids[0][None, :] < eight[:, None]).astype(jnp.int32), axis=1)
    doc_start = jnp.max(
        jnp.where(starts[None, :] <= position[:, None], starts[None, :], 0), axis=1
    )
    in_doc = position - doc_start
    info = jnp.concatenate([starts, run_start[None], run_end[None], seq_len, y[None]])
    return place, slots, text_index, info.astype(jnp.int32), in_doc


def one_device(
    text_rows, image_rows, tile_group, tile_offset, seq_len, doc_ids, norm_gain,
    q_weight, k_weight, v_weight, q_bias, k_bias, v_bias,
):
    x = lax.axis_index("x")
    core = lax.axis_index("c")
    group = x * 2 + core
    z = lax.axis_index("z")
    y = lax.axis_index("y")
    gain = norm_gain.reshape(1, -1)

    t_low = norm_text(text_rows, gain, 0, 64)
    t3_low = shifted(t_low, "z", 1)
    t1_low = shifted(t_low, "z", -1)

    quarter = 2 * core + x % 2
    begin, t_low = lax.optimization_barrier((quarter * 2 * PIECE, t_low))
    own_kv = jnp.concatenate([k_weight, v_weight], axis=1)

    def own_part(half):
        first = begin + half * PIECE
        return jnp.concatenate(
            [
                lax.dynamic_slice_in_dim(weight, first, PIECE, 0)
                for weight in (q_weight, own_kv)
            ],
            axis=1,
        )

    low, high = own_part(0), own_part(1)
    direct = {}
    direct[1, 0] = shifted(low, "y", -1)
    direct[3, 1] = shifted(high, "y", 1)
    direct[1, 1] = shifted(high, "y", -1)
    direct[3, 0] = shifted(low, "y", 1)

    low, high, text_rows = lax.optimization_barrier((low, high, text_rows))
    t_high = norm_text(text_rows, gain, 64, 64)
    t3_high = shifted(t_high, "z", 1)
    t1_high = shifted(t_high, "z", -1)

    row_groups = lax.dynamic_slice_in_dim(tile_group, group * 4, 4)
    matches = row_groups[None, :] == jnp.arange(8, dtype=jnp.int32)[:, None]
    chosen = jnp.sum(jnp.where(matches, jnp.arange(4, dtype=jnp.int32)[None, :], 0), axis=1)
    image_rows, t_high = lax.optimization_barrier((image_rows, t_high))
    outgoing = spread(image_rows, chosen.astype(jnp.int32))
    arrived = lax.all_to_all(outgoing, ("x", "c"), split_axis=0, concat_axis=0, tiled=True)

    t2_low = shifted(t3_low, "z", 1)
    t2_high = shifted(t1_high, "z", -1)

    direct[2, 0] = shifted(direct[1, 0], "y", -1)
    direct[2, 1] = shifted(direct[3, 1], "y", 1)
    across = {
        key: shifted(value, "x", -1 if key[1] else 1)
        for key, value in direct.items()
        if key[0] != 2
    }
    across[2, 0] = shifted(across[1, 0], "y", -1)
    across[2, 1] = shifted(across[3, 1], "y", 1)
    pieces = {
        delta: [direct[delta, 0], direct[delta, 1], across[delta, 0], across[delta, 1]]
        for delta in (1, 2, 3)
    }
    pieces = {
        delta: found
        + [shifted(value, "c", 1) for value in found]
        for delta, found in pieces.items()
    }
    quarters = jnp.stack([quarter ^ 0, quarter ^ 1, quarter ^ 2, quarter ^ 3]) * 2 * PIECE

    doc_ids, t1_high = lax.optimization_barrier((doc_ids, t1_high))
    place, slots, text_index, info, in_doc = tables(
        tile_group, tile_offset, seq_len, doc_ids, group, z, y, quarters
    )
    frequency = THETA ** (-(jnp.arange(HD // 2, dtype=jnp.float32) * 2.0) / HD)
    angles = in_doc.astype(jnp.float32)[:, None] * frequency[None, :]
    cosine = jnp.concatenate([jnp.cos(angles), jnp.cos(angles)], axis=-1)
    sine = jnp.concatenate([-jnp.sin(angles), jnp.sin(angles)], axis=-1)
    arrived, cosine, sine = lax.optimization_barrier((arrived, cosine, sine))
    i_low = norm_image(arrived, gain, slots[:4])
    i_high = norm_image(arrived, gain, slots[4:])
    i3_low = shifted(i_low, "z", 1)
    i1_low = shifted(i_low, "z", -1)
    i3_high = shifted(i_high, "z", 1)
    i1_high = shifted(i_high, "z", -1)
    i2_low = shifted(i3_low, "z", 1)
    i2_high = shifted(i1_high, "z", -1)

    bias = jnp.concatenate([q_bias, k_bias, v_bias])
    bias, t_high = lax.optimization_barrier((bias, t_high))
    biases = [
        bias, shifted(bias, "y", -1), shifted(bias, "y", 2),
        shifted(bias, "y", 1),
    ]
    q_biases = [value[None, :4 * HD] for value in biases]
    kv_bias = jnp.concatenate([value[None, 4 * HD:] for value in biases], axis=1)
    place, text_index, info = lax.optimization_barrier((place, text_index, info))
    texts = (t_low, t_high, t1_low, t1_high, t2_low, t2_high, t3_low, t3_high)
    images = (i_low, i_high, i1_low, i1_high, i2_low, i2_high, i3_low, i3_high)
    *pairs, far_query, compact = project_kv(
        place, texts, images, own_kv, pieces, kv_bias, q_biases[2], cosine, sine
    )
    queries = {2: far_query}
    after = compact
    for deltas in ((1, 3), (0,)):
        found = project_q(
            place, after, q_weight, pieces,
            {delta: q_biases[delta] for delta in deltas}, cosine, sine,
        )
        after, *found = lax.optimization_barrier((after, *found))
        queries.update(zip(deltas, found))
    parts = []
    for values in (queries, pairs):
        parts.append(values[0])
        parts += [shifted(values[4 - delta], "y", -delta) for delta in (1, 2, 3)]
    return attend(info, text_index, parts)


def solution(mesh):
    fine = Mesh(mesh.devices.reshape(4, 2, 4, 4), ("x", "c", "z", "y"))
    dp, seq = ("x", "c"), ("z", "y")
    return jax.shard_map(
        one_device,
        mesh=fine,
        in_specs=(
            P(dp + seq, None),
            P(dp, seq, None),
            P(),
            P(),
            P(dp),
            P(dp, None),
            P(),
            P(None, seq),
            P(None, seq),
            P(None, seq),
            P(seq),
            P(seq),
            P(seq),
        ),
        out_specs=P(dp, seq),
        check_vma=False,
    )
```
